32 devices in a mesh: grp: 4 (over y, x), shard: 8 (over z, core).
Axes of the slice: x: 2, y: 2, z: 4, core: 2. Of those that a mesh axis runs over, the one named last changes fastest.
Arguments:
- bottom_out: bfloat16 [4096, 128], P(('grp', 'shard')), may hold values from -6 to 6
- lookups: int32 [4096, 1, 4], P(('grp', 'shard')), may hold values from 0 to 62975, as said below
- starts: int32 [4, 32], replicated, may hold values from 0 to 1967
- tables: float32 [1, 62976, 128], P(None, 'shard'), may hold values from -0.3 to 0.3
- top_dense: bfloat16 [128, 1024], replicated, may hold values from -0.5 to 0.5
- top_pairs: float32 [1, 1024], replicated, may hold values from -6 to 6
- cotangent: float32 [4096, 1024], P(('grp', 'shard')), may hold values from -1.5 to 1.5
Outputs:
- activation: bfloat16 [4096, 1024], P(('grp', 'shard'))
- bottom_grad: float32 [4096, 128], P(('grp', 'shard'))
- table_grad: float32 [1, 8, 7872, 128], P(None, 'shard', 'grp')
The draws below stay inside these ranges and needn't reach their ends.
Inputs may be any that keep to these rules, and one draw needn't show every extreme that they name: lookups % 1968 is below 64, and 63 occurs.
All inputs are finite; a program needn't handle non-finite values.
Results may differ from the reference program's by a relative error of at most 0.0023.
Values sent between devices are 32-bit elements; how exact they have to be, the bound alone decides.
No kernel may reach another device: no remote copies, remote signals or barrier semaphores. Data moves between devices by JAX's collectives and lax.ppermute only.
A program may use at most 64 MiB of HBM per device.

```python
import jax
import jax.numpy as jnp
from jax import lax

D = 128
HIDDEN_SIZE = 1024
ROWS_DEV = 7872
NT = 1
BAG = 4
HOT = 64
B_DEV = 128
ROWS = 62976
WIN = 1968
WINDOWS = 32
BATCH = 4096
PAIRS = 1
N_GRP = 4
N_SHARD = 8


def draw_lookups(key, part):
    first_key = jax.random.fold_in(key, 11)
    second_key = jax.random.fold_in(key, 23)
    window = jax.random.randint(first_key, (BATCH, NT, BAG), 0, WINDOWS, dtype=jnp.int32)
    inner = jax.random.randint(second_key, (BATCH, NT, BAG), 0, HOT, dtype=jnp.int32)
    return (window * WIN + inner).astype(jnp.int32)


def touch_ends(values, stream_key, least, top_value):
    spot = [jax.random.randint(jax.random.fold_in(stream_key, axis), (), 0, length) for axis, length in enumerate(values.shape)]
    widest = values.shape.index(max(values.shape))
    next_to = spot[:widest] + [(spot[widest] + 1) % values.shape[widest]] + spot[widest + 1:]
    return values.at[tuple(spot)].set(least).at[tuple(next_to)].set(top_value)


def levels(key, shape, shards, low, largest):
    def one(position, shards_of):
        draws = jax.random.uniform(jax.random.fold_in(jax.random.fold_in(key, 6), position), (shards_of,), jnp.float32, low / len(shards), largest / len(shards))
        return jnp.repeat(jnp.exp(draws), shape[position] // shards_of).reshape((-1,) + (1,) * (len(shape) - position - 1))

    loudness = one(*shards[0])
    for cut in shards[1:]:
        loudness = loudness * one(*cut)
    return loudness


def normal_values(own_key, dims, spread, most, cuts=(), held_as=jnp.bfloat16):
    values = jax.random.normal(own_key, dims, jnp.float32) * spread
    if len(cuts) > 0:
        values = levels(own_key, dims, cuts, -0.22, 0.18) * values
    return jnp.clip(values, min=-most, max=most).astype(held_as)


def setup_inputs(seed: int = 0) -> dict:
    key_list = jax.random.split(jax.random.key(seed), 8)
    return {
        "bottom_out": normal_values(key_list[0], (BATCH, D), 1.0, 6.0, ((0, 32),)),
        "lookups": draw_lookups(jax.random.fold_in(key_list[7], 71), 0),
        "starts": touch_ends(jax.random.randint(key_list[2], (N_GRP, WINDOWS), 0, WIN), jax.random.fold_in(key_list[2], 1), 0, WIN - 1).astype(jnp.int32),
        "tables": normal_values(key_list[3], (NT, ROWS, D), 0.05, 0.3, ((1, 8),), jnp.float32),
        "top_dense": normal_values(key_list[4], (D, HIDDEN_SIZE), D ** -0.5, 0.5),
        "top_pairs": normal_values(key_list[5], (PAIRS, HIDDEN_SIZE), PAIRS ** -0.5, 6.0, (), jnp.float32),
        "cotangent": normal_values(key_list[6], (BATCH, HIDDEN_SIZE), 0.25, 1.5, ((0, 32),), jnp.float32),
    }


def pair_list(number):
    return [(former, latter) for former in range(number) for latter in range(former + 1, number)]


def reference(bottom_out, lookups, starts, tables, top_dense, top_pairs, cotangent):
    group_of = (jnp.arange(BATCH, dtype=jnp.int32) // (B_DEV * N_SHARD)).astype(jnp.int32)
    window = (lookups // WIN).astype(jnp.int32)
    inner = (lookups % WIN).astype(jnp.int32)
    shift = starts[group_of[:, None, None], window]
    rows = (window * WIN + (inner + shift) % WIN).astype(jnp.int32)
    pooled_list = []
    for table_pos in range(NT):
        running = jnp.zeros((BATCH, D), jnp.float32)
        for slot in range(BAG):
            running = running + tables[table_pos][rows[:, table_pos, slot]]
        pooled_list.append(running)
    vectors = [bottom_out.astype(jnp.float32)] + pooled_list
    couples = pair_list(NT + 1)
    pair_dots = jnp.stack([jnp.sum(vectors[former] * vectors[latter], axis=-1) for former, latter in couples], axis=1)
    preact = jnp.dot(bottom_out, top_dense, preferred_element_type=jnp.float32)
    preact = preact + jnp.dot(pair_dots, top_pairs, precision=lax.Precision.HIGHEST)
    sigmoid_pre = jax.nn.sigmoid(preact)
    activation = (preact * sigmoid_pre).astype(jnp.bfloat16)
    pre_grad = cotangent * sigmoid_pre * (1.0 + preact * (1.0 - sigmoid_pre))
    pair_grad = jnp.dot(pre_grad, top_pairs.T, precision=lax.Precision.HIGHEST)
    vec_grads = [jnp.zeros_like(vector) for vector in vectors]
    for place, (former, latter) in enumerate(couples):
        weight_col = pair_grad[:, place:place + 1]
        vec_grads[former] = vec_grads[former] + weight_col * vectors[latter]
        vec_grads[latter] = vec_grads[latter] + weight_col * vectors[former]
    pre_half = pre_grad.astype(jnp.bfloat16)
    bottom_grad = jnp.dot(pre_half, top_dense.T, preferred_element_type=jnp.float32) + vec_grads[0]
    grad_list = []
    for table_pos in range(NT):
        running = jnp.zeros((ROWS, D), jnp.float32)
        for slot in range(BAG):
            running = running.at[rows[:, table_pos, slot]].add(vec_grads[table_pos + 1])
        grad_list.append(running)
    table_grad = jnp.stack(grad_list, axis=0).reshape(NT, N_SHARD, ROWS_DEV, D)
    return activation, bottom_grad, table_grad
```

```python
import math

import jax
import jax.numpy as jnp
from jax import lax
from jax.experimental import pallas as pl
from jax.experimental.pallas import tpu as pltpu
from jax.sharding import PartitionSpec as P

HOT = 64


def pair_list(number):
    return [(former, latter) for former in range(number) for latter in range(former + 1, number)]


def pool_lookups(tables, picked, offset):
    rows_count = picked.shape[0]
    table_count = picked.shape[1]
    bag_count = picked.shape[2]
    rows_block = math.gcd(rows_count, 512)
    bag_block = math.gcd(bag_count, 8)
    bag_turns = bag_count // bag_block
    span_rows = tables.shape[1]
    table_ids = jnp.arange(table_count, dtype=jnp.int32)[None, :, None]

    def pool_step(turn, running):
        row_turn = turn // bag_turns
        bag_turn = turn % bag_turns
        chosen = lax.dynamic_slice(
            picked,
            (row_turn * rows_block, 0, bag_turn * bag_block),
            (rows_block, table_count, bag_block),
        )
        local = chosen - offset
        inside = (local >= 0) & (local < span_rows)
        fetched = tables[table_ids, jnp.clip(local, 0, span_rows - 1)]
        summed = jnp.sum(jnp.where(inside[..., None], fetched, 0.0), axis=2)
        current = lax.dynamic_slice_in_dim(running, row_turn * rows_block, rows_block, 0)
        return lax.dynamic_update_slice_in_dim(running, current + summed, row_turn * rows_block, 0)

    start_value = jnp.zeros((rows_count, table_count, tables.shape[2]), jnp.float32)
    return lax.fori_loop(0, rows_count // rows_block * bag_turns, pool_step, start_value)


def add_lookups(running_grad, grads, picked, offset, span_rows):
    rows_count = picked.shape[0]
    table_count = picked.shape[1]
    bag_count = picked.shape[2]
    rows_block = math.gcd(rows_count, 512)
    bag_block = math.gcd(bag_count, 8)
    bag_turns = bag_count // bag_block
    table_ids = jnp.arange(table_count, dtype=jnp.int32)[None, :, None]

    def add_step(turn, running):
        row_turn = turn // bag_turns
        bag_turn = turn % bag_turns
        chosen = lax.dynamic_slice(
            picked,
            (row_turn * rows_block, 0, bag_turn * bag_block),
            (rows_block, table_count, bag_block),
        )
        grads_block = lax.dynamic_slice_in_dim(grads, row_turn * rows_block, rows_block, 0)
        local = chosen - offset
        inside = (local >= 0) & (local < span_rows)
        updates = jnp.where(inside[..., None], grads_block[:, :, None, :], 0.0)
        return running.at[table_ids, jnp.clip(local, 0, span_rows - 1)].add(updates)

    return lax.fori_loop(0, rows_count // rows_block * bag_turns, add_step, running_grad)


def by_row_sums(bottom_out, lookups, starts, tables, top_dense, top_pairs, cotangent):
    shard_pos = lax.axis_index("shard")
    grp_pos = lax.axis_index("grp")
    group_count = lax.axis_size("grp")
    span_rows = tables.shape[1]
    table_count = tables.shape[0]
    width = tables.shape[2]
    win_size = span_rows // group_count
    offset = shard_pos * span_rows
    my_starts = lax.dynamic_index_in_dim(starts, grp_pos, 0, keepdims=False)
    window = lookups // win_size
    inner = lookups % win_size
    own_rows = window * win_size + (inner + my_starts[window]) % win_size
    group_idx = lax.all_gather(own_rows, "shard", axis=0, tiled=True)
    picked = group_idx
    pooled = lax.psum_scatter(
        pool_lookups(tables, picked, offset), "shard", scatter_dimension=0, tiled=True
    )
    vectors = [bottom_out.astype(jnp.float32)] + [pooled[:, 0]]
    couples = pair_list(table_count + 1)
    pair_dots = jnp.stack(
        [jnp.sum(vectors[former] * vectors[latter], axis=-1) for former, latter in couples], axis=1
    )
    preact = jnp.dot(bottom_out, top_dense, preferred_element_type=jnp.float32)
    preact = preact + jnp.dot(pair_dots, top_pairs, precision=lax.Precision.HIGHEST)
    sigmoid_pre = jax.nn.sigmoid(preact)
    activation = (preact * sigmoid_pre).astype(jnp.bfloat16)
    pre_grad = cotangent * sigmoid_pre * (1.0 + preact * (1.0 - sigmoid_pre))
    pair_grad = jnp.dot(pre_grad, top_pairs.T, precision=lax.Precision.HIGHEST)
    vec_grads = [jnp.zeros_like(vector) for vector in vectors]
    for place, (former, latter) in enumerate(couples):
        vec_grads[former] = pair_grad * vectors[latter]
        vec_grads[latter] = pair_grad * vectors[former]
    pre_half = pre_grad.astype(jnp.bfloat16)
    bottom_grad = (
        lax.dot_general(
            pre_half, top_dense, (((1,), (1,)), ((), ())), preferred_element_type=jnp.float32
        )
        + vec_grads[0]
    )
    pooled_grad = jnp.stack(vec_grads[1:], axis=1)
    start_grad = jnp.zeros((table_count, span_rows, width), jnp.float32)
    picked = group_idx
    local_grad = add_lookups(
        start_grad,
        lax.all_gather(pooled_grad, "shard", axis=0, tiled=True),
        picked,
        offset,
        span_rows,
    )
    hot_range = jnp.arange(HOT, dtype=jnp.int32)
    owner_range = jnp.arange(group_count, dtype=jnp.int32)
    send_starts = lax.dynamic_slice_in_dim(my_starts, shard_pos * group_count, group_count, 0)
    send_index = (
        owner_range[:, None] * win_size + (send_starts[:, None] + hot_range[None, :]) % win_size
    )
    packed = local_grad[:, send_index]
    received = lax.all_to_all(packed, "grp", split_axis=1, concat_axis=1, tiled=True)
    recv_starts = lax.dynamic_slice_in_dim(starts, shard_pos * group_count + grp_pos, 1, 1)[:, 0]
    places = ((recv_starts[:, None] + hot_range[None, :]) % win_size).reshape(-1)
    flat_rows = received.reshape(table_count, group_count * HOT, width)
    table_grad = jnp.zeros((table_count, win_size, width), jnp.float32).at[:, places].add(flat_rows)
    return (activation, bottom_grad, table_grad[:, None])


def whole(memory=pltpu.VMEM):
    return pl.BlockSpec(memory_space=memory)


def cost(flops, moved):
    return pl.CostEstimate(flops=int(flops), bytes_accessed=int(moved), transcendentals=0)


def two_terms(values):
    high = values.astype(jnp.bfloat16)
    low = (values - high.astype(jnp.float32)).astype(jnp.bfloat16)
    return high, low


def dot_two(counts, values):
    high, low = two_terms(values)
    return jnp.dot(counts, high, preferred_element_type=jnp.float32) + jnp.dot(
        counts, low, preferred_element_type=jnp.float32
    )


def pack_hot(starts, looked, bottom_out, table, group_count):
    span_rows, width = table.shape
    win_size = span_rows // group_count
    samples = bottom_out.shape[0]
    bag = looked.shape[0]
    head = min(HOT + 8, win_size)

    def kernel(starts_ref, looked_ref, bottom_ref, table_ref, hot_ref, sent_ref, places_ref, held, sems):
        grp_pos = lax.axis_index("grp")
        shard_pos = lax.axis_index("shard")
        shifts = []
        copies = []
        for window in range(group_count):
            start = starts_ref[grp_pos, shard_pos * group_count + window]
            aligned = jnp.minimum(start // 8 * 8, win_size - head)
            shifts.append(start - aligned)
            base = window * win_size
            first = pltpu.make_async_copy(
                table_ref.at[pl.ds(pl.multiple_of(base + aligned, 8), head)],
                held.at[window, pl.ds(0, head)],
                sems.at[window, 0],
            )
            second = pltpu.make_async_copy(
                table_ref.at[pl.ds(base, HOT)], held.at[window, pl.ds(head, HOT)], sems.at[window, 1]
            )
            first.start()
            second.start()
            copies += [first, second]
        found = looked_ref[...]
        window_of = jnp.floor((found.astype(jnp.float32) + 0.5) * (1.0 / win_size)).astype(jnp.int32)
        places = (found - window_of * (win_size - HOT)).astype(jnp.float32)
        places = jnp.concatenate([places, jnp.zeros((8 - bag, samples), jnp.float32)], axis=0)
        places_ref[...] = places
        sent_ref[pl.ds(0, samples), :] = bottom_ref[...].astype(jnp.float32)
        sent_ref[pl.ds(samples, 8), :] = places
        for copy in copies:
            copy.wait()
        for window in range(group_count):
            hot_ref[pl.ds(window * HOT, HOT), :] = held[window, pl.ds(shifts[window], HOT), :]

    hot_rows = group_count * HOT
    return pl.pallas_call(
        kernel,
        out_shape=(
            jax.ShapeDtypeStruct((hot_rows, width), jnp.float32),
            jax.ShapeDtypeStruct((samples + 8, width), jnp.float32),
            jax.ShapeDtypeStruct((8, samples), jnp.float32),
        ),
        in_specs=[whole(pltpu.SMEM), whole(), whole(), whole(pl.ANY)],
        out_specs=(whole(), whole(), whole()),
        scratch_shapes=[
            pltpu.VMEM((group_count, head + HOT, width), jnp.float32),
            pltpu.SemaphoreType.DMA((group_count, 2)),
        ],
        cost_estimate=cost(1e6, 1e6),
        name="pack_hot",
    )(starts, looked, bottom_out, table)


def count_rows(places_own, places_other, bottom_out, top_dense, bag, block_rows, steps):
    samples = bottom_out.shape[0]
    hidden = top_dense.shape[1]

    def kernel(own_ref, other_ref, bottom_ref, dense_ref, counts_ref, linear_ref):
        shard_pos = lax.axis_index("shard")
        rows = lax.broadcasted_iota(jnp.int32, (samples, block_rows), 1).astype(jnp.float32)
        for part, ref in enumerate((own_ref, other_ref)):
            padded = jnp.concatenate(
                [ref[...], jnp.zeros((samples - 8, samples), jnp.float32)], axis=0
            )
            columns = padded.T
            for place, step in enumerate(steps):
                base = (jnp.bitwise_xor(shard_pos, step) * block_rows).astype(jnp.float32)
                total = jnp.zeros((samples, block_rows), jnp.float32)
                for slot in range(bag):
                    total += jnp.where(columns[:, slot : slot + 1] - base == rows, 1.0, 0.0)
                counts_ref[
                    pl.ds(part * samples, samples), pl.ds(place * block_rows, block_rows)
                ] = total.astype(jnp.bfloat16)
        linear_ref[...] = jnp.dot(bottom_ref[...], dense_ref[...], preferred_element_type=jnp.float32)

    return pl.pallas_call(
        kernel,
        out_shape=(
            jax.ShapeDtypeStruct((2 * samples, len(steps) * block_rows), jnp.bfloat16),
            jax.ShapeDtypeStruct((samples, hidden), jnp.float32),
        ),
        in_specs=[whole()] * 4,
        out_specs=(whole(), whole()),
        cost_estimate=cost(3e7, 1e6),
        name="count_rows",
    )(places_own, places_other, bottom_out, top_dense)


def pool_hot(counts, blocks):
    block_rows, width = blocks[0].shape
    samples = counts.shape[0] // 2

    def kernel(counts_ref, *refs):
        block_refs = refs[: len(blocks)]
        own_ref, other_ref = refs[len(blocks) :]
        total = jnp.zeros((2 * samples, width), jnp.float32)
        for place, ref in enumerate(block_refs):
            total += dot_two(counts_ref[:, pl.ds(place * block_rows, block_rows)], ref[...])
        own_ref[...] = total[:samples]
        other_ref[...] = total[samples:]

    part = jax.ShapeDtypeStruct((samples, width), jnp.float32)
    return pl.pallas_call(
        kernel,
        out_shape=(part, part),
        in_specs=[whole()] * (1 + len(blocks)),
        out_specs=(whole(), whole()),
        cost_estimate=cost(1e8, 1e6),
        name="pool_hot",
    )(counts, *blocks)


def head_terms(pooled, bottom_ref, linear_ref, pairs_ref, cot_ref):
    dots = jnp.sum(bottom_ref[...].astype(jnp.float32) * pooled, axis=1, keepdims=True)
    preact = linear_ref[...] + dots * pairs_ref[...]
    sig = 1.0 / (1.0 + jnp.exp(-preact))
    pre_grad = cot_ref[...] * sig * (1.0 + preact * (1.0 - sig))
    pair_grad = jnp.sum(pre_grad * pairs_ref[...], axis=1, keepdims=True)
    return preact, sig, pre_grad, pair_grad


def score(part_own, part_other, bottom_out, linear, top_pairs, cotangent):
    samples, width = bottom_out.shape

    def kernel(own_ref, other_ref, bottom_ref, linear_ref, pairs_ref, cot_ref, row_ref, pooled_ref):
        pooled = own_ref[...] + other_ref[...]
        pooled_ref[...] = pooled
        pair_grad = head_terms(pooled, bottom_ref, linear_ref, pairs_ref, cot_ref)[3]
        down = lax.broadcasted_iota(jnp.int32, (samples, samples), 0)
        across = lax.broadcasted_iota(jnp.int32, (samples, samples), 1)
        row_ref[...] = jnp.sum(jnp.where(down == across, pair_grad, 0.0), axis=0, keepdims=True)

    return pl.pallas_call(
        kernel,
        out_shape=(
            jax.ShapeDtypeStruct((1, samples), jnp.float32),
            jax.ShapeDtypeStruct((samples, width), jnp.float32),
        ),
        in_specs=[whole()] * 6,
        out_specs=(whole(), whole()),
        cost_estimate=cost(1e7, 1e6),
        name="score",
    )(part_own, part_other, bottom_out, linear, top_pairs, cotangent)


def finish_dense(pooled, bottom_out, linear, top_pairs, cotangent, top_dense):
    samples, width = bottom_out.shape
    hidden = top_dense.shape[1]

    def kernel(pooled_ref, bottom_ref, linear_ref, pairs_ref, cot_ref, dense_ref, act_ref, grad_ref):
        pooled = pooled_ref[...]
        preact, sig, pre_grad, pair_grad = head_terms(pooled, bottom_ref, linear_ref, pairs_ref, cot_ref)
        act_ref[...] = (preact * sig).astype(jnp.bfloat16)
        grad_ref[...] = (
            lax.dot_general(
                pre_grad.astype(jnp.bfloat16),
                dense_ref[...],
                (((1,), (1,)), ((), ())),
                preferred_element_type=jnp.float32,
            )
            + pair_grad * pooled
        )

    return pl.pallas_call(
        kernel,
        out_shape=(
            jax.ShapeDtypeStruct((samples, hidden), jnp.bfloat16),
            jax.ShapeDtypeStruct((samples, width), jnp.float32),
        ),
        in_specs=[whole()] * 6,
        out_specs=(whole(), whole()),
        cost_estimate=cost(5e7, 1e6),
        name="finish_dense",
    )(pooled, bottom_out, linear, top_pairs, cotangent, top_dense)


def row_grads(scores, sent, bag, block_rows):
    samples = scores[0].shape[1]
    width = sent[0].shape[1]
    count = len(scores)

    def kernel(*refs):
        score_refs = refs[:count]
        sent_refs = refs[count : 2 * count]
        own_ref, other_ref = refs[2 * count :]
        shard_pos = lax.axis_index("shard")
        rows = lax.broadcasted_iota(jnp.int32, (block_rows, samples), 0).astype(jnp.float32)
        for side, out_ref in ((1, other_ref), (0, own_ref)):
            base = (jnp.bitwise_xor(shard_pos, side) * block_rows).astype(jnp.float32)
            total = jnp.zeros((block_rows, width), jnp.float32)
            for score_ref, sent_ref in zip(score_refs, sent_refs):
                places = sent_ref[pl.ds(samples, 8), :] - base
                times = jnp.zeros((block_rows, samples), jnp.float32)
                for slot in range(bag):
                    times += jnp.where(places[slot : slot + 1, :] == rows, 1.0, 0.0)
                high, low = two_terms(times * score_ref[...])
                bottom = sent_ref[pl.ds(0, samples), :].astype(jnp.bfloat16)
                total += jnp.dot(high, bottom, preferred_element_type=jnp.float32)
                total += jnp.dot(low, bottom, preferred_element_type=jnp.float32)
            out_ref[...] = total

    part = jax.ShapeDtypeStruct((block_rows, width), jnp.float32)
    return pl.pallas_call(
        kernel,
        out_shape=(part, part),
        in_specs=[whole()] * (2 * count),
        out_specs=(whole(), whole()),
        cost_estimate=cost(2e8, 1e6),
        name="row_grads",
    )(*scores, *sent)


def split_owners(grad_own, grad_other, group_count):
    width = grad_own.shape[1]

    def kernel(own_ref, other_ref, *out_refs):
        grp_pos = lax.axis_index("grp")
        for step, out_ref in enumerate(out_refs):
            first = pl.multiple_of(jnp.bitwise_xor(grp_pos, step) * HOT, HOT)
            out_ref[...] = own_ref[pl.ds(first, HOT), :] + other_ref[pl.ds(first, HOT), :]

    part = jax.ShapeDtypeStruct((HOT, width), jnp.float32)
    return pl.pallas_call(
        kernel,
        out_shape=(part,) * group_count,
        in_specs=[whole()] * 2,
        out_specs=(whole(),) * group_count,
        cost_estimate=cost(1e6, 1e6),
        name="split_owners",
    )(grad_own, grad_other)


def place_rows(starts, blocks, win_size):
    width = blocks[0].shape[1]
    count = len(blocks)

    def kernel(starts_ref, *refs):
        block_refs = refs[:count]
        out_ref, held, sem = refs[count:]
        grp_pos = lax.axis_index("grp")
        column = lax.axis_index("shard") * count + grp_pos
        held[...] = jnp.zeros_like(held)
        for step, ref in enumerate(block_refs):
            start = starts_ref[jnp.bitwise_xor(grp_pos, step), column]
            held[pl.ds(start, HOT), :] += ref[...]
        held[pl.ds(0, HOT), :] += held[pl.ds(win_size, HOT), :]
        copy = pltpu.make_async_copy(held.at[pl.ds(0, win_size)], out_ref, sem)
        copy.start()
        copy.wait()

    return pl.pallas_call(
        kernel,
        out_shape=jax.ShapeDtypeStruct((win_size, width), jnp.float32),
        in_specs=[whole(pltpu.SMEM)] + [whole()] * count,
        out_specs=whole(pl.ANY),
        scratch_shapes=[pltpu.VMEM((win_size + HOT, width), jnp.float32), pltpu.SemaphoreType.DMA],
        cost_estimate=cost(1e6, 2e6),
        name="place_rows",
    )(starts, *blocks)


def by_hot_rows(bottom_out, lookups, starts, tables, top_dense, top_pairs, cotangent):
    group_count = lax.axis_size("grp")
    shard_count = lax.axis_size("shard")
    bag = lookups.shape[2]
    win_size = tables.shape[1] // group_count
    block_rows = group_count * HOT

    def across(axis, values, step):
        size = lax.axis_size(axis)
        return lax.ppermute(values, axis, [(pos, pos ^ step) for pos in range(size)])

    steps = list(range(0, shard_count, 2))
    looked = lookups[:, 0, :].T
    hot, sent, places = pack_hot(starts, looked, bottom_out, tables[0], group_count)
    places_other = across("shard", places, 1)
    hot_blocks = [hot] + [across("shard", hot, step) for step in steps[1:]]
    sent_blocks = [sent] + [across("shard", sent, step) for step in steps[1:]]
    counts, linear = count_rows(places, places_other, bottom_out, top_dense, bag, block_rows, steps)
    part_own, part_other = pool_hot(counts, hot_blocks)
    part_back = across("shard", part_other, 1)
    score_row, pooled = score(part_own, part_back, bottom_out, linear, top_pairs, cotangent)
    scores = [score_row] + [across("shard", score_row, step) for step in steps[1:]]
    activation, bottom_grad = finish_dense(
        pooled, bottom_out, linear, top_pairs, cotangent, top_dense
    )
    grad_own, grad_other = row_grads(scores, sent_blocks, bag, block_rows)
    grad_back = across("shard", grad_other, 1)
    owned = split_owners(grad_own, grad_back, group_count)
    blocks = [owned[0]] + [across("grp", owned[step], step) for step in range(1, group_count)]
    table_grad = place_rows(starts, blocks, win_size)
    return activation, bottom_grad, table_grad[None, None]


def is_power(number):
    return number & (number - 1) == 0


def on_device(bottom_out, lookups, starts, tables, top_dense, top_pairs, cotangent):
    group_count = lax.axis_size("grp")
    shard_count = lax.axis_size("shard")
    group_lookups = lookups.shape[0] * lookups.shape[2] * shard_count
    hot_rows = group_count * HOT * shard_count
    fits = (
        tables.shape[0] == 1
        and lookups.shape[2] <= 8
        and bottom_out.shape[0] == tables.shape[2]
        and is_power(group_count)
        and is_power(shard_count)
        and tables.shape[1] // group_count % 8 == 0
        and hot_rows <= group_lookups
    )
    plan = by_hot_rows if fits else by_row_sums
    return plan(bottom_out, lookups, starts, tables, top_dense, top_pairs, cotangent)


def solution(mesh):
    in_specs = (
        P(("grp", "shard"), None),
        P(("grp", "shard"), None, None),
        P(),
        P(None, "shard", None),
        P(),
        P(),
        P(("grp", "shard"), None),
    )
    out_specs = (
        P(("grp", "shard"), None),
        P(("grp", "shard"), None),
        P(None, "shard", "grp", None),
    )
    return jax.shard_map(
        on_device, mesh=mesh, in_specs=in_specs, out_specs=out_specs, check_vma=False
    )
```

```python
import math

import jax
import jax.numpy as jnp
from jax import lax
from jax.experimental import pallas as pl
from jax.experimental.pallas import tpu as pltpu
from jax.sharding import PartitionSpec as P

HOT = 64
GRANT = 8 * 1024 * 1024
WIDE_GRANT = 52 * 1024 * 1024


def pair_list(number):
    return [(former, latter) for former in range(number) for latter in range(former + 1, number)]


def pool_lookups(tables, picked, offset):
    rows_count = picked.shape[0]
    table_count = picked.shape[1]
    bag_count = picked.shape[2]
    rows_block = math.gcd(rows_count, 512)
    bag_block = math.gcd(bag_count, 8)
    bag_turns = bag_count // bag_block
    span_rows = tables.shape[1]
    table_ids = jnp.arange(table_count, dtype=jnp.int32)[None, :, None]

    def pool_step(turn, running):
        row_turn = turn // bag_turns
        bag_turn = turn % bag_turns
        chosen = lax.dynamic_slice(
            picked,
            (row_turn * rows_block, 0, bag_turn * bag_block),
            (rows_block, table_count, bag_block),
        )
        local = chosen - offset
        inside = (local >= 0) & (local < span_rows)
        fetched = tables[table_ids, jnp.clip(local, 0, span_rows - 1)]
        summed = jnp.sum(jnp.where(inside[..., None], fetched, 0.0), axis=2)
        current = lax.dynamic_slice_in_dim(running, row_turn * rows_block, rows_block, 0)
        return lax.dynamic_update_slice_in_dim(running, current + summed, row_turn * rows_block, 0)

    start_value = jnp.zeros((rows_count, table_count, tables.shape[2]), jnp.float32)
    return lax.fori_loop(0, rows_count // rows_block * bag_turns, pool_step, start_value)


def add_lookups(running_grad, grads, picked, offset, span_rows):
    rows_count = picked.shape[0]
    table_count = picked.shape[1]
    bag_count = picked.shape[2]
    rows_block = math.gcd(rows_count, 512)
    bag_block = math.gcd(bag_count, 8)
    bag_turns = bag_count // bag_block
    table_ids = jnp.arange(table_count, dtype=jnp.int32)[None, :, None]

    def add_step(turn, running):
        row_turn = turn // bag_turns
        bag_turn = turn % bag_turns
        chosen = lax.dynamic_slice(
            picked,
            (row_turn * rows_block, 0, bag_turn * bag_block),
            (rows_block, table_count, bag_block),
        )
        grads_block = lax.dynamic_slice_in_dim(grads, row_turn * rows_block, rows_block, 0)
        local = chosen - offset
        inside = (local >= 0) & (local < span_rows)
        updates = jnp.where(inside[..., None], grads_block[:, :, None, :], 0.0)
        return running.at[table_ids, jnp.clip(local, 0, span_rows - 1)].add(updates)

    return lax.fori_loop(0, rows_count // rows_block * bag_turns, add_step, running_grad)


def by_row_sums(bottom_out, lookups, starts, tables, top_dense, top_pairs, cotangent):
    shard_pos = lax.axis_index("shard")
    grp_pos = lax.axis_index("grp")
    group_count = lax.axis_size("grp")
    span_rows = tables.shape[1]
    table_count = tables.shape[0]
    width = tables.shape[2]
    win_size = span_rows // group_count
    offset = shard_pos * span_rows
    my_starts = lax.dynamic_index_in_dim(starts, grp_pos, 0, keepdims=False)
    window = lookups // win_size
    inner = lookups % win_size
    own_rows = window * win_size + (inner + my_starts[window]) % win_size
    group_idx = lax.all_gather(own_rows, "shard", axis=0, tiled=True)
    picked = group_idx
    pooled = lax.psum_scatter(
        pool_lookups(tables, picked, offset), "shard", scatter_dimension=0, tiled=True
    )
    vectors = [bottom_out.astype(jnp.float32)] + [pooled[:, 0]]
    couples = pair_list(table_count + 1)
    pair_dots = jnp.stack(
        [jnp.sum(vectors[former] * vectors[latter], axis=-1) for former, latter in couples], axis=1
    )
    preact = jnp.dot(bottom_out, top_dense, preferred_element_type=jnp.float32)
    preact = preact + jnp.dot(pair_dots, top_pairs, precision=lax.Precision.HIGHEST)
    sigmoid_pre = jax.nn.sigmoid(preact)
    activation = (preact * sigmoid_pre).astype(jnp.bfloat16)
    pre_grad = cotangent * sigmoid_pre * (1.0 + preact * (1.0 - sigmoid_pre))
    pair_grad = jnp.dot(pre_grad, top_pairs.T, precision=lax.Precision.HIGHEST)
    vec_grads = [jnp.zeros_like(vector) for vector in vectors]
    for place, (former, latter) in enumerate(couples):
        vec_grads[former] = pair_grad * vectors[latter]
        vec_grads[latter] = pair_grad * vectors[former]
    pre_half = pre_grad.astype(jnp.bfloat16)
    bottom_grad = (
        lax.dot_general(
            pre_half, top_dense, (((1,), (1,)), ((), ())), preferred_element_type=jnp.float32
        )
        + vec_grads[0]
    )
    pooled_grad = jnp.stack(vec_grads[1:], axis=1)
    start_grad = jnp.zeros((table_count, span_rows, width), jnp.float32)
    picked = group_idx
    local_grad = add_lookups(
        start_grad,
        lax.all_gather(pooled_grad, "shard", axis=0, tiled=True),
        picked,
        offset,
        span_rows,
    )
    hot_range = jnp.arange(HOT, dtype=jnp.int32)
    owner_range = jnp.arange(group_count, dtype=jnp.int32)
    send_starts = lax.dynamic_slice_in_dim(my_starts, shard_pos * group_count, group_count, 0)
    send_index = (
        owner_range[:, None] * win_size + (send_starts[:, None] + hot_range[None, :]) % win_size
    )
    packed = local_grad[:, send_index]
    received = lax.all_to_all(packed, "grp", split_axis=1, concat_axis=1, tiled=True)
    recv_starts = lax.dynamic_slice_in_dim(starts, shard_pos * group_count + grp_pos, 1, 1)[:, 0]
    places = ((recv_starts[:, None] + hot_range[None, :]) % win_size).reshape(-1)
    flat_rows = received.reshape(table_count, group_count * HOT, width)
    table_grad = jnp.zeros((table_count, win_size, width), jnp.float32).at[:, places].add(flat_rows)
    return (activation, bottom_grad, table_grad[:, None])


def whole(memory=pltpu.VMEM):
    return pl.BlockSpec(memory_space=memory)


def cost(flops, moved):
    return pl.CostEstimate(flops=int(flops), bytes_accessed=int(moved), transcendentals=0)


def two_terms(values):
    high = values.astype(jnp.bfloat16)
    low = (values - high.astype(jnp.float32)).astype(jnp.bfloat16)
    return high, low


def dot_two(counts, values):
    high, low = two_terms(values)
    return jnp.dot(counts, high, preferred_element_type=jnp.float32) + jnp.dot(
        counts, low, preferred_element_type=jnp.float32
    )


def pack_hot(starts, looked, bottom_out, table, group_count):
    span_rows, width = table.shape
    win_size = span_rows // group_count
    samples = bottom_out.shape[0]
    bag = looked.shape[0]
    head = min(HOT + 8, win_size)

    def kernel(starts_ref, looked_ref, bottom_ref, table_ref, hot_ref, sent_ref, places_ref, held, sems):
        grp_pos = lax.axis_index("grp")
        shard_pos = lax.axis_index("shard")
        shifts = []
        copies = []
        for window in range(group_count):
            start = starts_ref[grp_pos, shard_pos * group_count + window]
            aligned = jnp.minimum(start // 8 * 8, win_size - head)
            shifts.append(start - aligned)
            base = window * win_size
            first = pltpu.make_async_copy(
                table_ref.at[pl.ds(pl.multiple_of(base + aligned, 8), head)],
                held.at[window, pl.ds(0, head)],
                sems.at[window, 0],
            )
            second = pltpu.make_async_copy(
                table_ref.at[pl.ds(base, HOT)], held.at[window, pl.ds(head, HOT)], sems.at[window, 1]
            )
            first.start()
            second.start()
            copies += [first, second]
        found = looked_ref[...]
        window_of = jnp.floor((found.astype(jnp.float32) + 0.5) * (1.0 / win_size)).astype(jnp.int32)
        places = (found - window_of * (win_size - HOT)).astype(jnp.float32)
        places = jnp.concatenate([places, jnp.zeros((8 - bag, samples), jnp.float32)], axis=0)
        places_ref[...] = places
        sent_ref[pl.ds(0, samples), :] = bottom_ref[...].astype(jnp.float32)
        sent_ref[pl.ds(samples, 8), :] = places
        for copy in copies:
            copy.wait()
        for window in range(group_count):
            hot_ref[pl.ds(window * HOT, HOT), :] = held[window, pl.ds(shifts[window], HOT), :]

    hot_rows = group_count * HOT
    return pl.pallas_call(
        kernel,
        out_shape=(
            jax.ShapeDtypeStruct((hot_rows, width), jnp.float32),
            jax.ShapeDtypeStruct((samples + 8, width), jnp.float32),
            jax.ShapeDtypeStruct((8, samples), jnp.float32),
        ),
        in_specs=[whole(pltpu.SMEM), whole(), whole(), whole(pl.ANY)],
        out_specs=(whole(), whole(), whole()),
        scratch_shapes=[
            pltpu.VMEM((group_count, head + HOT, width), jnp.float32),
            pltpu.SemaphoreType.DMA((group_count, 2)),
        ],
        cost_estimate=cost(1e6, 1e6),
        compiler_params=pltpu.CompilerParams(vmem_limit_bytes=WIDE_GRANT),
        name="pack_hot",
    )(starts, looked, bottom_out, table)


def count_rows(places_own, places_other, bottom_out, top_dense, bag, block_rows, steps):
    samples = bottom_out.shape[0]
    hidden = top_dense.shape[1]

    def kernel(own_ref, other_ref, bottom_ref, dense_ref, counts_ref, linear_ref):
        shard_pos = lax.axis_index("shard")
        rows = lax.broadcasted_iota(jnp.int32, (samples, block_rows), 1).astype(jnp.float32)
        for part, ref in enumerate((own_ref, other_ref)):
            padded = jnp.concatenate(
                [ref[...], jnp.zeros((samples - 8, samples), jnp.float32)], axis=0
            )
            columns = padded.T
            for place, step in enumerate(steps):
                base = (jnp.bitwise_xor(shard_pos, step) * block_rows).astype(jnp.float32)
                total = jnp.zeros((samples, block_rows), jnp.float32)
                for slot in range(bag):
                    total += jnp.where(columns[:, slot : slot + 1] - base == rows, 1.0, 0.0)
                counts_ref[
                    pl.ds(part * samples, samples), pl.ds(place * block_rows, block_rows)
                ] = total.astype(jnp.bfloat16)
        linear_ref[...] = jnp.dot(bottom_ref[...], dense_ref[...], preferred_element_type=jnp.float32)

    return pl.pallas_call(
        kernel,
        out_shape=(
            jax.ShapeDtypeStruct((2 * samples, len(steps) * block_rows), jnp.bfloat16),
            jax.ShapeDtypeStruct((samples, hidden), jnp.float32),
        ),
        in_specs=[whole()] * 4,
        out_specs=(whole(), whole()),
        cost_estimate=cost(3e7, 1e6),
        compiler_params=pltpu.CompilerParams(vmem_limit_bytes=GRANT),
        name="count_rows",
    )(places_own, places_other, bottom_out, top_dense)


def pool_hot(counts, blocks):
    block_rows, width = blocks[0].shape
    samples = counts.shape[0] // 2

    def kernel(counts_ref, *refs):
        block_refs = refs[: len(blocks)]
        own_ref, other_ref = refs[len(blocks) :]
        total = jnp.zeros((2 * samples, width), jnp.float32)
        for place, ref in enumerate(block_refs):
            total += dot_two(counts_ref[:, pl.ds(place * block_rows, block_rows)], ref[...])
        own_ref[...] = total[:samples]
        other_ref[...] = total[samples:]

    part = jax.ShapeDtypeStruct((samples, width), jnp.float32)
    return pl.pallas_call(
        kernel,
        out_shape=(part, part),
        in_specs=[whole()] * (1 + len(blocks)),
        out_specs=(whole(), whole()),
        cost_estimate=cost(1e8, 1e6),
        compiler_params=pltpu.CompilerParams(vmem_limit_bytes=GRANT),
        name="pool_hot",
    )(counts, *blocks)


def head_terms(pooled, bottom_ref, linear_ref, pairs_ref, cot_ref):
    dots = jnp.sum(bottom_ref[...].astype(jnp.float32) * pooled, axis=1, keepdims=True)
    preact = linear_ref[...] + dots * pairs_ref[...]
    sig = 1.0 / (1.0 + jnp.exp(-preact))
    pre_grad = cot_ref[...] * sig * (1.0 + preact * (1.0 - sig))
    pair_grad = jnp.sum(pre_grad * pairs_ref[...], axis=1, keepdims=True)
    return preact, sig, pre_grad, pair_grad


def score(part_own, part_other, bottom_out, linear, top_pairs, cotangent):
    samples, width = bottom_out.shape

    def kernel(own_ref, other_ref, bottom_ref, linear_ref, pairs_ref, cot_ref, row_ref, pooled_ref):
        pooled = own_ref[...] + other_ref[...]
        pooled_ref[...] = pooled
        pair_grad = head_terms(pooled, bottom_ref, linear_ref, pairs_ref, cot_ref)[3]
        down = lax.broadcasted_iota(jnp.int32, (samples, samples), 0)
        across = lax.broadcasted_iota(jnp.int32, (samples, samples), 1)
        row_ref[...] = jnp.sum(jnp.where(down == across, pair_grad, 0.0), axis=0, keepdims=True)

    return pl.pallas_call(
        kernel,
        out_shape=(
            jax.ShapeDtypeStruct((1, samples), jnp.float32),
            jax.ShapeDtypeStruct((samples, width), jnp.float32),
        ),
        in_specs=[whole()] * 6,
        out_specs=(whole(), whole()),
        cost_estimate=cost(1e7, 1e6),
        compiler_params=pltpu.CompilerParams(vmem_limit_bytes=GRANT),
        name="score",
    )(part_own, part_other, bottom_out, linear, top_pairs, cotangent)


def finish_dense(pooled, bottom_out, linear, top_pairs, cotangent, top_dense):
    samples, width = bottom_out.shape
    hidden = top_dense.shape[1]

    def kernel(pooled_ref, bottom_ref, linear_ref, pairs_ref, cot_ref, dense_ref, act_ref, grad_ref):
        pooled = pooled_ref[...]
        preact, sig, pre_grad, pair_grad = head_terms(pooled, bottom_ref, linear_ref, pairs_ref, cot_ref)
        act_ref[...] = (preact * sig).astype(jnp.bfloat16)
        grad_ref[...] = (
            lax.dot_general(
                pre_grad.astype(jnp.bfloat16),
                dense_ref[...],
                (((1,), (1,)), ((), ())),
                preferred_element_type=jnp.float32,
            )
            + pair_grad * pooled
        )

    return pl.pallas_call(
        kernel,
        out_shape=(
            jax.ShapeDtypeStruct((samples, hidden), jnp.bfloat16),
            jax.ShapeDtypeStruct((samples, width), jnp.float32),
        ),
        in_specs=[whole()] * 6,
        out_specs=(whole(), whole()),
        cost_estimate=cost(5e7, 1e6),
        compiler_params=pltpu.CompilerParams(vmem_limit_bytes=GRANT),
        name="finish_dense",
    )(pooled, bottom_out, linear, top_pairs, cotangent, top_dense)


def row_grads(scores, sent, bag, block_rows):
    samples = scores[0].shape[1]
    width = sent[0].shape[1]
    count = len(scores)

    def kernel(*refs):
        score_refs = refs[:count]
        sent_refs = refs[count : 2 * count]
        own_ref, other_ref = refs[2 * count :]
        shard_pos = lax.axis_index("shard")
        rows = lax.broadcasted_iota(jnp.int32, (block_rows, samples), 0).astype(jnp.float32)
        for side, out_ref in ((1, other_ref), (0, own_ref)):
            base = (jnp.bitwise_xor(shard_pos, side) * block_rows).astype(jnp.float32)
            total = jnp.zeros((block_rows, width), jnp.float32)
            for score_ref, sent_ref in zip(score_refs, sent_refs):
                places = sent_ref[pl.ds(samples, 8), :] - base
                times = jnp.zeros((block_rows, samples), jnp.float32)
                for slot in range(bag):
                    times += jnp.where(places[slot : slot + 1, :] == rows, 1.0, 0.0)
                high, low = two_terms(times * score_ref[...])
                bottom = sent_ref[pl.ds(0, samples), :].astype(jnp.bfloat16)
                total += jnp.dot(high, bottom, preferred_element_type=jnp.float32)
                total += jnp.dot(low, bottom, preferred_element_type=jnp.float32)
            out_ref[...] = total

    part = jax.ShapeDtypeStruct((block_rows, width), jnp.float32)
    return pl.pallas_call(
        kernel,
        out_shape=(part, part),
        in_specs=[whole()] * (2 * count),
        out_specs=(whole(), whole()),
        cost_estimate=cost(2e8, 1e6),
        compiler_params=pltpu.CompilerParams(vmem_limit_bytes=GRANT),
        name="row_grads",
    )(*scores, *sent)


def split_owners(grad_own, grad_other, group_count):
    width = grad_own.shape[1]

    def kernel(own_ref, other_ref, *out_refs):
        grp_pos = lax.axis_index("grp")
        for step, out_ref in enumerate(out_refs):
            first = pl.multiple_of(jnp.bitwise_xor(grp_pos, step) * HOT, HOT)
            out_ref[...] = own_ref[pl.ds(first, HOT), :] + other_ref[pl.ds(first, HOT), :]

    part = jax.ShapeDtypeStruct((HOT, width), jnp.float32)
    return pl.pallas_call(
        kernel,
        out_shape=(part,) * group_count,
        in_specs=[whole()] * 2,
        out_specs=(whole(),) * group_count,
        cost_estimate=cost(1e6, 1e6),
        compiler_params=pltpu.CompilerParams(vmem_limit_bytes=GRANT),
        name="split_owners",
    )(grad_own, grad_other)


def place_rows(starts, blocks, win_size):
    width = blocks[0].shape[1]
    count = len(blocks)

    def kernel(starts_ref, *refs):
        block_refs = refs[:count]
        out_ref, held, sem = refs[count:]
        grp_pos = lax.axis_index("grp")
        column = lax.axis_index("shard") * count + grp_pos
        held[...] = jnp.zeros_like(held)
        for step, ref in enumerate(block_refs):
            start = starts_ref[jnp.bitwise_xor(grp_pos, step), column]
            held[pl.ds(start, HOT), :] += ref[...]
        held[pl.ds(0, HOT), :] += held[pl.ds(win_size, HOT), :]
        copy = pltpu.make_async_copy(held.at[pl.ds(0, win_size)], out_ref, sem)
        copy.start()
        copy.wait()

    return pl.pallas_call(
        kernel,
        out_shape=jax.ShapeDtypeStruct((win_size, width), jnp.float32),
        in_specs=[whole(pltpu.SMEM)] + [whole()] * count,
        out_specs=whole(pl.ANY),
        scratch_shapes=[pltpu.VMEM((win_size + HOT, width), jnp.float32), pltpu.SemaphoreType.DMA],
        cost_estimate=cost(1e6, 2e6),
        compiler_params=pltpu.CompilerParams(vmem_limit_bytes=GRANT),
        name="place_rows",
    )(starts, *blocks)


def by_hot_rows(bottom_out, lookups, starts, tables, top_dense, top_pairs, cotangent):
    group_count = lax.axis_size("grp")
    shard_count = lax.axis_size("shard")
    bag = lookups.shape[2]
    win_size = tables.shape[1] // group_count
    block_rows = group_count * HOT

    def across(axis, values, step):
        size = lax.axis_size(axis)
        return lax.ppermute(values, axis, [(pos, pos ^ step) for pos in range(size)])

    steps = list(range(0, shard_count, 2))
    looked = lookups[:, 0, :].T
    hot, sent, places = pack_hot(starts, looked, bottom_out, tables[0], group_count)
    places_other = across("shard", places, 1)
    hot_blocks = [hot] + [across("shard", hot, step) for step in steps[1:]]
    sent_blocks = [sent] + [across("shard", sent, step) for step in steps[1:]]
    counts, linear = count_rows(places, places_other, bottom_out, top_dense, bag, block_rows, steps)
    part_own, part_other = pool_hot(counts, hot_blocks)
    part_back = across("shard", part_other, 1)
    score_row, pooled = score(part_own, part_back, bottom_out, linear, top_pairs, cotangent)
    scores = [score_row] + [across("shard", score_row, step) for step in steps[1:]]
    activation, bottom_grad = finish_dense(
        pooled, bottom_out, linear, top_pairs, cotangent, top_dense
    )
    grad_own, grad_other = row_grads(scores, sent_blocks, bag, block_rows)
    grad_back = across("shard", grad_other, 1)
    owned = split_owners(grad_own, grad_back, group_count)
    blocks = [owned[0]] + [across("grp", owned[step], step) for step in range(1, group_count)]
    table_grad = place_rows(starts, blocks, win_size)
    return activation, bottom_grad, table_grad[None, None]


def is_power(number):
    return number & (number - 1) == 0


def on_device(bottom_out, lookups, starts, tables, top_dense, top_pairs, cotangent):
    group_count = lax.axis_size("grp")
    shard_count = lax.axis_size("shard")
    group_lookups = lookups.shape[0] * lookups.shape[2] * shard_count
    hot_rows = group_count * HOT * shard_count
    fits = (
        tables.shape[0] == 1
        and lookups.shape[2] <= 8
        and bottom_out.shape[0] == tables.shape[2]
        and is_power(group_count)
        and is_power(shard_count)
        and tables.shape[1] // group_count % 8 == 0
        and hot_rows <= group_lookups
    )
    plan = by_hot_rows if fits else by_row_sums
    return plan(bottom_out, lookups, starts, tables, top_dense, top_pairs, cotangent)


def solution(mesh):
    in_specs = (
        P(("grp", "shard"), None),
        P(("grp", "shard"), None, None),
        P(),
        P(None, "shard", None),
        P(),
        P(),
        P(("grp", "shard"), None),
    )
    out_specs = (
        P(("grp", "shard"), None),
        P(("grp", "shard"), None),
        P(None, "shard", "grp", None),
    )
    return jax.shard_map(
        on_device, mesh=mesh, in_specs=in_specs, out_specs=out_specs, check_vma=False
    )
```

```python
import math

import jax
import jax.numpy as jnp
from jax import lax
from jax.experimental import pallas as pl
from jax.experimental.pallas import tpu as pltpu
from jax.sharding import PartitionSpec as P

HOT = 64
GRANT = 8 * 1024 * 1024


def pair_list(number):
    return [(former, latter) for former in range(number) for latter in range(former + 1, number)]


def pool_lookups(tables, picked, offset):
    rows_count = picked.shape[0]
    table_count = picked.shape[1]
    bag_count = picked.shape[2]
    rows_block = math.gcd(rows_count, 512)
    bag_block = math.gcd(bag_count, 8)
    bag_turns = bag_count // bag_block
    span_rows = tables.shape[1]
    table_ids = jnp.arange(table_count, dtype=jnp.int32)[None, :, None]

    def pool_step(turn, running):
        row_turn = turn // bag_turns
        bag_turn = turn % bag_turns
        chosen = lax.dynamic_slice(
            picked,
            (row_turn * rows_block, 0, bag_turn * bag_block),
            (rows_block, table_count, bag_block),
        )
        local = chosen - offset
        inside = (local >= 0) & (local < span_rows)
        fetched = tables[table_ids, jnp.clip(local, 0, span_rows - 1)]
        summed = jnp.sum(jnp.where(inside[..., None], fetched, 0.0), axis=2)
        current = lax.dynamic_slice_in_dim(running, row_turn * rows_block, rows_block, 0)
        return lax.dynamic_update_slice_in_dim(running, current + summed, row_turn * rows_block, 0)

    start_value = jnp.zeros((rows_count, table_count, tables.shape[2]), jnp.float32)
    return lax.fori_loop(0, rows_count // rows_block * bag_turns, pool_step, start_value)


def add_lookups(running_grad, grads, picked, offset, span_rows):
    rows_count = picked.shape[0]
    table_count = picked.shape[1]
    bag_count = picked.shape[2]
    rows_block = math.gcd(rows_count, 512)
    bag_block = math.gcd(bag_count, 8)
    bag_turns = bag_count // bag_block
    table_ids = jnp.arange(table_count, dtype=jnp.int32)[None, :, None]

    def add_step(turn, running):
        row_turn = turn // bag_turns
        bag_turn = turn % bag_turns
        chosen = lax.dynamic_slice(
            picked,
            (row_turn * rows_block, 0, bag_turn * bag_block),
            (rows_block, table_count, bag_block),
        )
        grads_block = lax.dynamic_slice_in_dim(grads, row_turn * rows_block, rows_block, 0)
        local = chosen - offset
        inside = (local >= 0) & (local < span_rows)
        updates = jnp.where(inside[..., None], grads_block[:, :, None, :], 0.0)
        return running.at[table_ids, jnp.clip(local, 0, span_rows - 1)].add(updates)

    return lax.fori_loop(0, rows_count // rows_block * bag_turns, add_step, running_grad)


def by_row_sums(bottom_out, lookups, starts, tables, top_dense, top_pairs, cotangent):
    shard_pos = lax.axis_index("shard")
    grp_pos = lax.axis_index("grp")
    group_count = lax.axis_size("grp")
    span_rows = tables.shape[1]
    table_count = tables.shape[0]
    width = tables.shape[2]
    win_size = span_rows // group_count
    offset = shard_pos * span_rows
    my_starts = lax.dynamic_index_in_dim(starts, grp_pos, 0, keepdims=False)
    window = lookups // win_size
    inner = lookups % win_size
    own_rows = window * win_size + (inner + my_starts[window]) % win_size
    group_idx = lax.all_gather(own_rows, "shard", axis=0, tiled=True)
    picked = group_idx
    pooled = lax.psum_scatter(
        pool_lookups(tables, picked, offset), "shard", scatter_dimension=0, tiled=True
    )
    vectors = [bottom_out.astype(jnp.float32)] + [pooled[:, 0]]
    couples = pair_list(table_count + 1)
    pair_dots = jnp.stack(
        [jnp.sum(vectors[former] * vectors[latter], axis=-1) for former, latter in couples], axis=1
    )
    preact = jnp.dot(bottom_out, top_dense, preferred_element_type=jnp.float32)
    preact = preact + jnp.dot(pair_dots, top_pairs, precision=lax.Precision.HIGHEST)
    sigmoid_pre = jax.nn.sigmoid(preact)
    activation = (preact * sigmoid_pre).astype(jnp.bfloat16)
    pre_grad = cotangent * sigmoid_pre * (1.0 + preact * (1.0 - sigmoid_pre))
    pair_grad = jnp.dot(pre_grad, top_pairs.T, precision=lax.Precision.HIGHEST)
    vec_grads = [jnp.zeros_like(vector) for vector in vectors]
    for place, (former, latter) in enumerate(couples):
        vec_grads[former] = pair_grad * vectors[latter]
        vec_grads[latter] = pair_grad * vectors[former]
    pre_half = pre_grad.astype(jnp.bfloat16)
    bottom_grad = (
        lax.dot_general(
            pre_half, top_dense, (((1,), (1,)), ((), ())), preferred_element_type=jnp.float32
        )
        + vec_grads[0]
    )
    pooled_grad = jnp.stack(vec_grads[1:], axis=1)
    start_grad = jnp.zeros((table_count, span_rows, width), jnp.float32)
    picked = group_idx
    local_grad = add_lookups(
        start_grad,
        lax.all_gather(pooled_grad, "shard", axis=0, tiled=True),
        picked,
        offset,
        span_rows,
    )
    hot_range = jnp.arange(HOT, dtype=jnp.int32)
    owner_range = jnp.arange(group_count, dtype=jnp.int32)
    send_starts = lax.dynamic_slice_in_dim(my_starts, shard_pos * group_count, group_count, 0)
    send_index = (
        owner_range[:, None] * win_size + (send_starts[:, None] + hot_range[None, :]) % win_size
    )
    packed = local_grad[:, send_index]
    received = lax.all_to_all(packed, "grp", split_axis=1, concat_axis=1, tiled=True)
    recv_starts = lax.dynamic_slice_in_dim(starts, shard_pos * group_count + grp_pos, 1, 1)[:, 0]
    places = ((recv_starts[:, None] + hot_range[None, :]) % win_size).reshape(-1)
    flat_rows = received.reshape(table_count, group_count * HOT, width)
    table_grad = jnp.zeros((table_count, win_size, width), jnp.float32).at[:, places].add(flat_rows)
    return (activation, bottom_grad, table_grad[:, None])


def whole(memory=pltpu.VMEM):
    return pl.BlockSpec(memory_space=memory)


def cost(flops, moved):
    return pl.CostEstimate(flops=int(flops), bytes_accessed=int(moved), transcendentals=0)


def two_terms(values):
    high = values.astype(jnp.bfloat16)
    low = (values - high.astype(jnp.float32)).astype(jnp.bfloat16)
    return high, low


def dot_two(counts, values):
    high, low = two_terms(values)
    return jnp.dot(counts, high, preferred_element_type=jnp.float32) + jnp.dot(
        counts, low, preferred_element_type=jnp.float32
    )


def stay(values):
    return pltpu.with_memory_space_constraint(values, pltpu.HBM)


def pack_sent(looked, bottom_out, win_size):
    samples, width = bottom_out.shape
    bag = looked.shape[0]

    def kernel(looked_ref, bottom_ref, sent_ref):
        found = looked_ref[...]
        window_of = jnp.floor((found.astype(jnp.float32) + 0.5) * (1.0 / win_size)).astype(jnp.int32)
        places = (found - window_of * (win_size - HOT)).astype(jnp.float32)
        sent_ref[pl.ds(samples, 8), :] = jnp.concatenate(
            [places, jnp.zeros((8 - bag, samples), jnp.float32)], axis=0
        )
        sent_ref[pl.ds(0, samples), :] = bottom_ref[...].astype(jnp.float32)

    return pl.pallas_call(
        kernel,
        out_shape=jax.ShapeDtypeStruct((samples + 8, width), jnp.float32),
        in_specs=[whole()] * 2,
        out_specs=whole(),
        cost_estimate=cost(1e6, 1e5),
        compiler_params=pltpu.CompilerParams(vmem_limit_bytes=GRANT),
        name="pack_sent",
    )(stay(looked), stay(bottom_out))


def load_hot(starts, table, group_count):
    span_rows, width = table.shape
    win_size = span_rows // group_count
    head = min(HOT + 8, win_size)

    def kernel(starts_ref, table_ref, hot_ref, held, sems):
        grp_pos = lax.axis_index("grp")
        shard_pos = lax.axis_index("shard")
        shifts = []
        copies = []
        for window in range(group_count):
            start = starts_ref[grp_pos, shard_pos * group_count + window]
            aligned = jnp.minimum(start // 8 * 8, win_size - head)
            shifts.append(start - aligned)
            base = window * win_size
            first = pltpu.make_async_copy(
                table_ref.at[pl.ds(pl.multiple_of(base + aligned, 8), head)],
                held.at[window, pl.ds(0, head)],
                sems.at[window, 0],
            )
            second = pltpu.make_async_copy(
                table_ref.at[pl.ds(base, HOT)], held.at[window, pl.ds(head, HOT)], sems.at[window, 1]
            )
            first.start()
            second.start()
            copies += [first, second]
        for copy in copies:
            copy.wait()
        for window in range(group_count):
            hot_ref[pl.ds(window * HOT, HOT), :] = held[window, pl.ds(shifts[window], HOT), :]

    return pl.pallas_call(
        kernel,
        out_shape=jax.ShapeDtypeStruct((group_count * HOT, width), jnp.float32),
        in_specs=[whole(pltpu.SMEM), whole(pl.ANY)],
        out_specs=whole(),
        scratch_shapes=[
            pltpu.VMEM((group_count, head + HOT, width), jnp.float32),
            pltpu.SemaphoreType.DMA((group_count, 2)),
        ],
        cost_estimate=cost(1e6, 1e6),
        compiler_params=pltpu.CompilerParams(vmem_limit_bytes=GRANT),
        name="load_hot",
    )(stay(starts), stay(table))


def linear_part(bottom_out, top_dense):
    def kernel(bottom_ref, dense_ref, linear_ref):
        linear_ref[...] = jnp.dot(bottom_ref[...], dense_ref[...], preferred_element_type=jnp.float32)

    return pl.pallas_call(
        kernel,
        out_shape=jax.ShapeDtypeStruct((bottom_out.shape[0], top_dense.shape[1]), jnp.float32),
        in_specs=[whole()] * 2,
        out_specs=whole(),
        cost_estimate=cost(3e7, 1e6),
        compiler_params=pltpu.CompilerParams(vmem_limit_bytes=GRANT),
        name="linear_part",
    )(bottom_out, top_dense)


def pool_rows(sent, hot_own, hot_other, bag):
    block_rows, width = hot_own.shape
    samples = sent.shape[0] - 8

    def kernel(sent_ref, own_ref, other_ref, part_ref):
        shard_pos = lax.axis_index("shard")
        rows = lax.broadcasted_iota(jnp.int32, (samples, block_rows), 1).astype(jnp.float32)
        columns = jnp.concatenate(
            [sent_ref[pl.ds(samples, 8), :], jnp.zeros((samples - 8, samples), jnp.float32)], axis=0
        ).T
        total = jnp.zeros((samples, width), jnp.float32)
        for side, ref in enumerate((own_ref, other_ref)):
            base = (jnp.bitwise_xor(shard_pos, side) * block_rows).astype(jnp.float32)
            times = jnp.zeros((samples, block_rows), jnp.float32)
            for slot in range(bag):
                times += jnp.where(columns[:, slot : slot + 1] - base == rows, 1.0, 0.0)
            total += dot_two(times.astype(jnp.bfloat16), ref[...])
        part_ref[...] = total

    return pl.pallas_call(
        kernel,
        out_shape=jax.ShapeDtypeStruct((samples, width), jnp.float32),
        in_specs=[whole()] * 3,
        out_specs=whole(),
        cost_estimate=cost(5e7, 1e6),
        compiler_params=pltpu.CompilerParams(vmem_limit_bytes=GRANT),
        name="pool_rows",
    )(sent, hot_own, hot_other)


def head_terms(pooled, bottom_ref, linear_ref, pairs_ref, cot_ref):
    dots = jnp.sum(bottom_ref[...].astype(jnp.float32) * pooled, axis=1, keepdims=True)
    preact = linear_ref[...] + dots * pairs_ref[...]
    sig = 1.0 / (1.0 + jnp.exp(-preact))
    pre_grad = cot_ref[...] * sig * (1.0 + preact * (1.0 - sig))
    pair_grad = jnp.sum(pre_grad * pairs_ref[...], axis=1, keepdims=True)
    return preact, sig, pre_grad, pair_grad


def score(parts, bottom_out, linear, top_pairs, cotangent):
    samples, width = bottom_out.shape
    count = len(parts)

    def kernel(*refs):
        bottom_ref, linear_ref, pairs_ref, cot_ref, row_ref, pooled_ref = refs[count:]
        pooled = refs[0][...]
        for ref in refs[1:count]:
            pooled = pooled + ref[...]
        pooled_ref[...] = pooled
        pair_grad = head_terms(pooled, bottom_ref, linear_ref, pairs_ref, cot_ref)[3]
        down = lax.broadcasted_iota(jnp.int32, (samples, samples), 0)
        across = lax.broadcasted_iota(jnp.int32, (samples, samples), 1)
        row_ref[...] = jnp.sum(jnp.where(down == across, pair_grad, 0.0), axis=0, keepdims=True)

    return pl.pallas_call(
        kernel,
        out_shape=(
            jax.ShapeDtypeStruct((1, samples), jnp.float32),
            jax.ShapeDtypeStruct((samples, width), jnp.float32),
        ),
        in_specs=[whole()] * (count + 4),
        out_specs=(whole(), whole()),
        cost_estimate=cost(1e7, 1e6),
        compiler_params=pltpu.CompilerParams(vmem_limit_bytes=GRANT),
        name="score",
    )(*parts, bottom_out, linear, top_pairs, cotangent)


def finish_dense(pooled, bottom_out, linear, top_pairs, cotangent, top_dense):
    samples, width = bottom_out.shape
    hidden = top_dense.shape[1]

    def kernel(pooled_ref, bottom_ref, linear_ref, pairs_ref, cot_ref, dense_ref, act_ref, grad_ref):
        pooled = pooled_ref[...]
        preact, sig, pre_grad, pair_grad = head_terms(pooled, bottom_ref, linear_ref, pairs_ref, cot_ref)
        act_ref[...] = (preact * sig).astype(jnp.bfloat16)
        grad_ref[...] = (
            lax.dot_general(
                pre_grad.astype(jnp.bfloat16),
                dense_ref[...],
                (((1,), (1,)), ((), ())),
                preferred_element_type=jnp.float32,
            )
            + pair_grad * pooled
        )

    return pl.pallas_call(
        kernel,
        out_shape=(
            jax.ShapeDtypeStruct((samples, hidden), jnp.bfloat16),
            jax.ShapeDtypeStruct((samples, width), jnp.float32),
        ),
        in_specs=[whole()] * 6,
        out_specs=(whole(), whole()),
        cost_estimate=cost(5e7, 1e6),
        compiler_params=pltpu.CompilerParams(vmem_limit_bytes=GRANT),
        name="finish_dense",
    )(pooled, bottom_out, linear, top_pairs, cotangent, top_dense)


def row_grads(scores, sent, bag, block_rows):
    samples = scores[0].shape[1]
    width = sent[0].shape[1]
    count = len(scores)

    def kernel(*refs):
        score_refs = refs[:count]
        sent_refs = refs[count : 2 * count]
        own_ref, other_ref = refs[2 * count :]
        shard_pos = lax.axis_index("shard")
        rows = lax.broadcasted_iota(jnp.int32, (block_rows, samples), 0).astype(jnp.float32)
        for side, out_ref in ((1, other_ref), (0, own_ref)):
            base = (jnp.bitwise_xor(shard_pos, side) * block_rows).astype(jnp.float32)
            total = jnp.zeros((block_rows, width), jnp.float32)
            for score_ref, sent_ref in zip(score_refs, sent_refs):
                places = sent_ref[pl.ds(samples, 8), :] - base
                times = jnp.zeros((block_rows, samples), jnp.float32)
                for slot in range(bag):
                    times += jnp.where(places[slot : slot + 1, :] == rows, 1.0, 0.0)
                high, low = two_terms(times * score_ref[...])
                bottom = sent_ref[pl.ds(0, samples), :].astype(jnp.bfloat16)
                total += jnp.dot(high, bottom, preferred_element_type=jnp.float32)
                total += jnp.dot(low, bottom, preferred_element_type=jnp.float32)
            out_ref[...] = total

    part = jax.ShapeDtypeStruct((block_rows, width), jnp.float32)
    return pl.pallas_call(
        kernel,
        out_shape=(part, part),
        in_specs=[whole()] * (2 * count),
        out_specs=(whole(), whole()),
        cost_estimate=cost(2e8, 1e6),
        compiler_params=pltpu.CompilerParams(vmem_limit_bytes=GRANT),
        name="row_grads",
    )(*scores, *sent)


def split_owners(grad_own, grad_other, group_count):
    width = grad_own.shape[1]

    def kernel(own_ref, other_ref, *out_refs):
        grp_pos = lax.axis_index("grp")
        for step, out_ref in enumerate(out_refs):
            first = pl.multiple_of(jnp.bitwise_xor(grp_pos, step) * HOT, HOT)
            out_ref[...] = own_ref[pl.ds(first, HOT), :] + other_ref[pl.ds(first, HOT), :]

    part = jax.ShapeDtypeStruct((HOT, width), jnp.float32)
    return pl.pallas_call(
        kernel,
        out_shape=(part,) * group_count,
        in_specs=[whole()] * 2,
        out_specs=(whole(),) * group_count,
        cost_estimate=cost(1e6, 1e6),
        compiler_params=pltpu.CompilerParams(vmem_limit_bytes=GRANT),
        name="split_owners",
    )(grad_own, grad_other)


def place_rows(starts, blocks, win_size):
    width = blocks[0].shape[1]
    count = len(blocks)

    def kernel(starts_ref, *refs):
        block_refs = refs[:count]
        out_ref, held, sem = refs[count:]
        grp_pos = lax.axis_index("grp")
        column = lax.axis_index("shard") * count + grp_pos
        held[...] = jnp.zeros_like(held)
        for step, ref in enumerate(block_refs):
            start = starts_ref[jnp.bitwise_xor(grp_pos, step), column]
            held[pl.ds(start, HOT), :] += ref[...]
        held[pl.ds(0, HOT), :] += held[pl.ds(win_size, HOT), :]
        copy = pltpu.make_async_copy(held.at[pl.ds(0, win_size)], out_ref, sem)
        copy.start()
        copy.wait()

    return pl.pallas_call(
        kernel,
        out_shape=jax.ShapeDtypeStruct((win_size, width), jnp.float32),
        in_specs=[whole(pltpu.SMEM)] + [whole()] * count,
        out_specs=whole(pl.ANY),
        scratch_shapes=[pltpu.VMEM((win_size + HOT, width), jnp.float32), pltpu.SemaphoreType.DMA],
        cost_estimate=cost(1e6, 2e6),
        compiler_params=pltpu.CompilerParams(vmem_limit_bytes=GRANT),
        name="place_rows",
    )(starts, *blocks)


def by_hot_rows(bottom_out, lookups, starts, tables, top_dense, top_pairs, cotangent):
    group_count = lax.axis_size("grp")
    shard_count = lax.axis_size("shard")
    bag = lookups.shape[2]
    win_size = tables.shape[1] // group_count
    block_rows = group_count * HOT

    def across(axis, values, step):
        size = lax.axis_size(axis)
        return lax.ppermute(values, axis, [(pos, pos ^ step) for pos in range(size)])

    steps = list(range(0, shard_count, 2))
    looked = lookups[:, 0, :].T
    sent = pack_sent(looked, bottom_out, win_size)
    sent_blocks = [sent] + [across("shard", sent, step) for step in steps[1:]]
    hot_own = load_hot(starts, tables[0], group_count)
    hot_other = across("shard", hot_own, 1)
    linear = linear_part(bottom_out, top_dense)
    sums = [pool_rows(block, hot_own, hot_other, bag) for block in sent_blocks]
    parts = [sums[0]] + [across("shard", part, step) for part, step in zip(sums[1:], steps[1:])]
    score_row, pooled = score(parts, bottom_out, linear, top_pairs, cotangent)
    scores = [score_row] + [across("shard", score_row, step) for step in steps[1:]]
    activation, bottom_grad = finish_dense(
        pooled, bottom_out, linear, top_pairs, cotangent, top_dense
    )
    grad_own, grad_other = row_grads(scores, sent_blocks, bag, block_rows)
    grad_back = across("shard", grad_other, 1)
    owned = split_owners(grad_own, grad_back, group_count)
    blocks = [owned[0]] + [across("grp", owned[step], step) for step in range(1, group_count)]
    table_grad = place_rows(starts, blocks, win_size)
    return activation, bottom_grad, table_grad[None, None]


def is_power(number):
    return number & (number - 1) == 0


def on_device(bottom_out, lookups, starts, tables, top_dense, top_pairs, cotangent):
    group_count = lax.axis_size("grp")
    shard_count = lax.axis_size("shard")
    group_lookups = lookups.shape[0] * lookups.shape[2] * shard_count
    hot_rows = group_count * HOT * shard_count
    fits = (
        tables.shape[0] == 1
        and lookups.shape[2] <= 8
        and bottom_out.shape[0] == tables.shape[2]
        and is_power(group_count)
        and is_power(shard_count)
        and tables.shape[1] // group_count % 8 == 0
        and hot_rows <= group_lookups
        and shard_count % 2 == 0
    )
    plan = by_hot_rows if fits else by_row_sums
    return plan(bottom_out, lookups, starts, tables, top_dense, top_pairs, cotangent)


def solution(mesh):
    in_specs = (
        P(("grp", "shard"), None),
        P(("grp", "shard"), None, None),
        P(),
        P(None, "shard", None),
        P(),
        P(),
        P(("grp", "shard"), None),
    )
    out_specs = (
        P(("grp", "shard"), None),
        P(("grp", "shard"), None),
        P(None, "shard", "grp", None),
    )
    return jax.shard_map(
        on_device, mesh=mesh, in_specs=in_specs, out_specs=out_specs, check_vma=False
    )
```

```python
import math

import jax
import jax.numpy as jnp
from jax import lax
from jax.experimental import pallas as pl
from jax.experimental.pallas import tpu as pltpu
from jax.sharding import PartitionSpec as P

HOT = 64
GRANT = 8 * 1024 * 1024


def pair_list(number):
    return [(former, latter) for former in range(number) for latter in range(former + 1, number)]


def pool_lookups(tables, picked, offset):
    rows_count = picked.shape[0]
    table_count = picked.shape[1]
    bag_count = picked.shape[2]
    rows_block = math.gcd(rows_count, 512)
    bag_block = math.gcd(bag_count, 8)
    bag_turns = bag_count // bag_block
    span_rows = tables.shape[1]
    table_ids = jnp.arange(table_count, dtype=jnp.int32)[None, :, None]

    def pool_step(turn, running):
        row_turn = turn // bag_turns
        bag_turn = turn % bag_turns
        chosen = lax.dynamic_slice(
            picked,
            (row_turn * rows_block, 0, bag_turn * bag_block),
            (rows_block, table_count, bag_block),
        )
        local = chosen - offset
        inside = (local >= 0) & (local < span_rows)
        fetched = tables[table_ids, jnp.clip(local, 0, span_rows - 1)]
        summed = jnp.sum(jnp.where(inside[..., None], fetched, 0.0), axis=2)
        current = lax.dynamic_slice_in_dim(running, row_turn * rows_block, rows_block, 0)
        return lax.dynamic_update_slice_in_dim(running, current + summed, row_turn * rows_block, 0)

    start_value = jnp.zeros((rows_count, table_count, tables.shape[2]), jnp.float32)
    return lax.fori_loop(0, rows_count // rows_block * bag_turns, pool_step, start_value)


def add_lookups(running_grad, grads, picked, offset, span_rows):
    rows_count = picked.shape[0]
    table_count = picked.shape[1]
    bag_count = picked.shape[2]
    rows_block = math.gcd(rows_count, 512)
    bag_block = math.gcd(bag_count, 8)
    bag_turns = bag_count // bag_block
    table_ids = jnp.arange(table_count, dtype=jnp.int32)[None, :, None]

    def add_step(turn, running):
        row_turn = turn // bag_turns
        bag_turn = turn % bag_turns
        chosen = lax.dynamic_slice(
            picked,
            (row_turn * rows_block, 0, bag_turn * bag_block),
            (rows_block, table_count, bag_block),
        )
        grads_block = lax.dynamic_slice_in_dim(grads, row_turn * rows_block, rows_block, 0)
        local = chosen - offset
        inside = (local >= 0) & (local < span_rows)
        updates = jnp.where(inside[..., None], grads_block[:, :, None, :], 0.0)
        return running.at[table_ids, jnp.clip(local, 0, span_rows - 1)].add(updates)

    return lax.fori_loop(0, rows_count // rows_block * bag_turns, add_step, running_grad)


def by_row_sums(bottom_out, lookups, starts, tables, top_dense, top_pairs, cotangent):
    shard_pos = lax.axis_index("shard")
    grp_pos = lax.axis_index("grp")
    group_count = lax.axis_size("grp")
    span_rows = tables.shape[1]
    table_count = tables.shape[0]
    width = tables.shape[2]
    win_size = span_rows // group_count
    offset = shard_pos * span_rows
    my_starts = lax.dynamic_index_in_dim(starts, grp_pos, 0, keepdims=False)
    window = lookups // win_size
    inner = lookups % win_size
    own_rows = window * win_size + (inner + my_starts[window]) % win_size
    group_idx = lax.all_gather(own_rows, "shard", axis=0, tiled=True)
    picked = group_idx
    pooled = lax.psum_scatter(
        pool_lookups(tables, picked, offset), "shard", scatter_dimension=0, tiled=True
    )
    vectors = [bottom_out.astype(jnp.float32)] + [pooled[:, 0]]
    couples = pair_list(table_count + 1)
    pair_dots = jnp.stack(
        [jnp.sum(vectors[former] * vectors[latter], axis=-1) for former, latter in couples], axis=1
    )
    preact = jnp.dot(bottom_out, top_dense, preferred_element_type=jnp.float32)
    preact = preact + jnp.dot(pair_dots, top_pairs, precision=lax.Precision.HIGHEST)
    sigmoid_pre = jax.nn.sigmoid(preact)
    activation = (preact * sigmoid_pre).astype(jnp.bfloat16)
    pre_grad = cotangent * sigmoid_pre * (1.0 + preact * (1.0 - sigmoid_pre))
    pair_grad = jnp.dot(pre_grad, top_pairs.T, precision=lax.Precision.HIGHEST)
    vec_grads = [jnp.zeros_like(vector) for vector in vectors]
    for place, (former, latter) in enumerate(couples):
        vec_grads[former] = pair_grad * vectors[latter]
        vec_grads[latter] = pair_grad * vectors[former]
    pre_half = pre_grad.astype(jnp.bfloat16)
    bottom_grad = (
        lax.dot_general(
            pre_half, top_dense, (((1,), (1,)), ((), ())), preferred_element_type=jnp.float32
        )
        + vec_grads[0]
    )
    pooled_grad = jnp.stack(vec_grads[1:], axis=1)
    start_grad = jnp.zeros((table_count, span_rows, width), jnp.float32)
    picked = group_idx
    local_grad = add_lookups(
        start_grad,
        lax.all_gather(pooled_grad, "shard", axis=0, tiled=True),
        picked,
        offset,
        span_rows,
    )
    hot_range = jnp.arange(HOT, dtype=jnp.int32)
    owner_range = jnp.arange(group_count, dtype=jnp.int32)
    send_starts = lax.dynamic_slice_in_dim(my_starts, shard_pos * group_count, group_count, 0)
    send_index = (
        owner_range[:, None] * win_size + (send_starts[:, None] + hot_range[None, :]) % win_size
    )
    packed = local_grad[:, send_index]
    received = lax.all_to_all(packed, "grp", split_axis=1, concat_axis=1, tiled=True)
    recv_starts = lax.dynamic_slice_in_dim(starts, shard_pos * group_count + grp_pos, 1, 1)[:, 0]
    places = ((recv_starts[:, None] + hot_range[None, :]) % win_size).reshape(-1)
    flat_rows = received.reshape(table_count, group_count * HOT, width)
    table_grad = jnp.zeros((table_count, win_size, width), jnp.float32).at[:, places].add(flat_rows)
    return (activation, bottom_grad, table_grad[:, None])


def whole(memory=pltpu.VMEM):
    return pl.BlockSpec(memory_space=memory)


def cost(flops, moved):
    return pl.CostEstimate(flops=int(flops), bytes_accessed=int(moved), transcendentals=0)


def two_terms(values):
    high = values.astype(jnp.bfloat16)
    low = (values - high.astype(jnp.float32)).astype(jnp.bfloat16)
    return high, low


def dot_two(counts, values):
    high, low = two_terms(values)
    return jnp.dot(counts, high, preferred_element_type=jnp.float32) + jnp.dot(
        counts, low, preferred_element_type=jnp.float32
    )


def stay(values):
    return pltpu.with_memory_space_constraint(values, pltpu.HBM)


def load_first(starts, looked, bottom_out, table, group_count):
    span_rows, width = table.shape
    win_size = span_rows // group_count
    samples = bottom_out.shape[0]
    bag = looked.shape[0]
    head = min(HOT + 8, win_size)

    def kernel(starts_ref, looked_ref, bottom_ref, table_ref, hot_ref, places_ref, wide_ref, held, sems):
        grp_pos = lax.axis_index("grp")
        shard_pos = lax.axis_index("shard")
        shifts = []
        copies = []
        for window in range(group_count):
            start = starts_ref[grp_pos, shard_pos * group_count + window]
            aligned = jnp.minimum(start // 8 * 8, win_size - head)
            shifts.append(start - aligned)
            base = window * win_size
            first = pltpu.make_async_copy(
                table_ref.at[pl.ds(pl.multiple_of(base + aligned, 8), head)],
                held.at[window, pl.ds(0, head)],
                sems.at[window, 0],
            )
            second = pltpu.make_async_copy(
                table_ref.at[pl.ds(base, HOT)], held.at[window, pl.ds(head, HOT)], sems.at[window, 1]
            )
            first.start()
            second.start()
            copies += [first, second]
        found = looked_ref[...]
        window_of = jnp.floor((found.astype(jnp.float32) + 0.5) * (1.0 / win_size)).astype(jnp.int32)
        places = (found - window_of * (win_size - HOT)).astype(jnp.float32)
        places_ref[...] = jnp.concatenate(
            [places, jnp.zeros((8 - bag, samples), jnp.float32)], axis=0
        )
        wide_ref[...] = bottom_ref[...].astype(jnp.float32)
        for copy in copies:
            copy.wait()
        for window in range(group_count):
            hot_ref[pl.ds(window * HOT, HOT), :] = held[window, pl.ds(shifts[window], HOT), :]

    return pl.pallas_call(
        kernel,
        out_shape=(
            jax.ShapeDtypeStruct((group_count * HOT, width), jnp.float32),
            jax.ShapeDtypeStruct((8, samples), jnp.float32),
            jax.ShapeDtypeStruct((samples, width), jnp.float32),
        ),
        in_specs=[whole(pltpu.SMEM), whole(), whole(), whole(pl.ANY)],
        out_specs=(whole(), whole(), whole()),
        scratch_shapes=[
            pltpu.VMEM((group_count, head + HOT, width), jnp.float32),
            pltpu.SemaphoreType.DMA((group_count, 2)),
        ],
        cost_estimate=cost(1e6, 1e6),
        compiler_params=pltpu.CompilerParams(vmem_limit_bytes=GRANT),
        name="load_first",
    )(stay(starts), stay(looked), stay(bottom_out), stay(table))


def linear_part(bottom_out, top_dense):
    def kernel(bottom_ref, dense_ref, linear_ref):
        linear_ref[...] = jnp.dot(bottom_ref[...], dense_ref[...], preferred_element_type=jnp.float32)

    return pl.pallas_call(
        kernel,
        out_shape=jax.ShapeDtypeStruct((bottom_out.shape[0], top_dense.shape[1]), jnp.float32),
        in_specs=[whole()] * 2,
        out_specs=whole(),
        cost_estimate=cost(3e7, 1e6),
        compiler_params=pltpu.CompilerParams(vmem_limit_bytes=GRANT),
        name="linear_part",
    )(bottom_out, top_dense)


def pool_rows(places, hot_own, hot_other, bag):
    block_rows, width = hot_own.shape
    samples = places.shape[1]

    def kernel(places_ref, own_ref, other_ref, part_ref):
        shard_pos = lax.axis_index("shard")
        rows = lax.broadcasted_iota(jnp.int32, (samples, block_rows), 1).astype(jnp.float32)
        columns = jnp.concatenate(
            [places_ref[...], jnp.zeros((samples - 8, samples), jnp.float32)], axis=0
        ).T
        total = jnp.zeros((samples, width), jnp.float32)
        for side, ref in enumerate((own_ref, other_ref)):
            base = (jnp.bitwise_xor(shard_pos, side) * block_rows).astype(jnp.float32)
            times = jnp.zeros((samples, block_rows), jnp.float32)
            for slot in range(bag):
                times += jnp.where(columns[:, slot : slot + 1] - base == rows, 1.0, 0.0)
            total += dot_two(times.astype(jnp.bfloat16), ref[...])
        part_ref[...] = total

    return pl.pallas_call(
        kernel,
        out_shape=jax.ShapeDtypeStruct((samples, width), jnp.float32),
        in_specs=[whole()] * 3,
        out_specs=whole(),
        cost_estimate=cost(5e7, 1e6),
        compiler_params=pltpu.CompilerParams(vmem_limit_bytes=GRANT),
        name="pool_rows",
    )(places, hot_own, hot_other)


def head_terms(pooled, bottom_ref, linear_ref, pairs_ref, cot_ref):
    dots = jnp.sum(bottom_ref[...].astype(jnp.float32) * pooled, axis=1, keepdims=True)
    preact = linear_ref[...] + dots * pairs_ref[...]
    sig = 1.0 / (1.0 + jnp.exp(-preact))
    pre_grad = cot_ref[...] * sig * (1.0 + preact * (1.0 - sig))
    pair_grad = jnp.sum(pre_grad * pairs_ref[...], axis=1, keepdims=True)
    return preact, sig, pre_grad, pair_grad


def score(parts, bottom_out, linear, top_pairs, cotangent):
    samples, width = bottom_out.shape
    count = len(parts)

    def kernel(*refs):
        bottom_ref, linear_ref, pairs_ref, cot_ref, row_ref, pooled_ref = refs[count:]
        pooled = refs[0][...]
        for ref in refs[1:count]:
            pooled = pooled + ref[...]
        pooled_ref[...] = pooled
        pair_grad = head_terms(pooled, bottom_ref, linear_ref, pairs_ref, cot_ref)[3]
        down = lax.broadcasted_iota(jnp.int32, (samples, samples), 0)
        across = lax.broadcasted_iota(jnp.int32, (samples, samples), 1)
        row_ref[...] = jnp.sum(jnp.where(down == across, pair_grad, 0.0), axis=0, keepdims=True)

    return pl.pallas_call(
        kernel,
        out_shape=(
            jax.ShapeDtypeStruct((1, samples), jnp.float32),
            jax.ShapeDtypeStruct((samples, width), jnp.float32),
        ),
        in_specs=[whole()] * (count + 4),
        out_specs=(whole(), whole()),
        cost_estimate=cost(1e7, 1e6),
        compiler_params=pltpu.CompilerParams(vmem_limit_bytes=GRANT),
        name="score",
    )(*parts, bottom_out, linear, top_pairs, cotangent)


def finish_dense(pooled, bottom_out, linear, top_pairs, cotangent, top_dense):
    samples, width = bottom_out.shape
    hidden = top_dense.shape[1]

    def kernel(pooled_ref, bottom_ref, linear_ref, pairs_ref, cot_ref, dense_ref, act_ref, grad_ref):
        pooled = pooled_ref[...]
        preact, sig, pre_grad, pair_grad = head_terms(pooled, bottom_ref, linear_ref, pairs_ref, cot_ref)
        act_ref[...] = (preact * sig).astype(jnp.bfloat16)
        grad_ref[...] = (
            lax.dot_general(
                pre_grad.astype(jnp.bfloat16),
                dense_ref[...],
                (((1,), (1,)), ((), ())),
                preferred_element_type=jnp.float32,
            )
            + pair_grad * pooled
        )

    return pl.pallas_call(
        kernel,
        out_shape=(
            jax.ShapeDtypeStruct((samples, hidden), jnp.bfloat16),
            jax.ShapeDtypeStruct((samples, width), jnp.float32),
        ),
        in_specs=[whole()] * 6,
        out_specs=(whole(), whole()),
        cost_estimate=cost(5e7, 1e6),
        compiler_params=pltpu.CompilerParams(vmem_limit_bytes=GRANT),
        name="finish_dense",
    )(pooled, bottom_out, linear, top_pairs, cotangent, top_dense)


def row_grads(scores, places, wides, bag, group_count, kept):
    samples, width = wides[0].shape
    count = len(scores)

    def kernel(*refs):
        score_refs, place_refs, wide_refs = refs[:count], refs[count : 2 * count], refs[2 * count : -1]
        grp_pos = lax.axis_index("grp")
        shard_pos = lax.axis_index("shard")
        ids = []
        for step in range(group_count):
            holder = shard_pos if kept == (step == 0) else jnp.bitwise_xor(shard_pos, 1)
            first = (holder * group_count + jnp.bitwise_xor(grp_pos, step)) * HOT
            ids.append(lax.broadcasted_iota(jnp.int32, (HOT, samples), 0) + first)
        rows = jnp.concatenate(ids, axis=0).astype(jnp.float32)
        total = jnp.zeros((group_count * HOT, width), jnp.float32)
        for score_ref, place_ref, wide_ref in zip(score_refs, place_refs, wide_refs):
            times = jnp.zeros(rows.shape, jnp.float32)
            for slot in range(bag):
                times += jnp.where(place_ref[pl.ds(slot, 1), :] == rows, 1.0, 0.0)
            high, low = two_terms(times * score_ref[...])
            bottom = wide_ref[...].astype(jnp.bfloat16)
            total += jnp.dot(high, bottom, preferred_element_type=jnp.float32)
            total += jnp.dot(low, bottom, preferred_element_type=jnp.float32)
        refs[-1][...] = total

    return pl.pallas_call(
        kernel,
        out_shape=jax.ShapeDtypeStruct((group_count * HOT, width), jnp.float32),
        in_specs=[whole()] * (3 * count),
        out_specs=whole(),
        cost_estimate=cost(1e8, 1e6),
        compiler_params=pltpu.CompilerParams(vmem_limit_bytes=GRANT),
        name="row_grads_kept" if kept else "row_grads_given",
    )(*scores, *places, *wides)


def split_owners(kept, received, group_count):
    width = kept.shape[1]

    def kernel(kept_ref, received_ref, *out_refs):
        for step, out_ref in enumerate(out_refs):
            chosen = pl.ds(step * HOT, HOT)
            out_ref[...] = kept_ref[chosen, :] + received_ref[chosen, :]

    part = jax.ShapeDtypeStruct((HOT, width), jnp.float32)
    return pl.pallas_call(
        kernel,
        out_shape=(part,) * group_count,
        in_specs=[whole()] * 2,
        out_specs=(whole(),) * group_count,
        cost_estimate=cost(1e6, 1e6),
        compiler_params=pltpu.CompilerParams(vmem_limit_bytes=GRANT),
        name="split_owners",
    )(kept, received)


def place_rows(starts, blocks, win_size):
    width = blocks[0].shape[1]
    count = len(blocks)

    def kernel(starts_ref, *refs):
        block_refs = refs[:count]
        out_ref, held, sem = refs[count:]
        grp_pos = lax.axis_index("grp")
        column = lax.axis_index("shard") * count + grp_pos
        held[...] = jnp.zeros_like(held)
        for step, ref in enumerate(block_refs):
            start = starts_ref[jnp.bitwise_xor(grp_pos, step), column]
            held[pl.ds(start, HOT), :] += ref[...]
        held[pl.ds(0, HOT), :] += held[pl.ds(win_size, HOT), :]
        copy = pltpu.make_async_copy(held.at[pl.ds(0, win_size)], out_ref, sem)
        copy.start()
        copy.wait()

    return pl.pallas_call(
        kernel,
        out_shape=jax.ShapeDtypeStruct((win_size, width), jnp.float32),
        in_specs=[whole(pltpu.SMEM)] + [whole()] * count,
        out_specs=whole(pl.ANY),
        scratch_shapes=[pltpu.VMEM((win_size + HOT, width), jnp.float32), pltpu.SemaphoreType.DMA],
        cost_estimate=cost(1e6, 2e6),
        compiler_params=pltpu.CompilerParams(vmem_limit_bytes=GRANT),
        name="place_rows",
    )(starts, *blocks)


def by_hot_rows(bottom_out, lookups, starts, tables, top_dense, top_pairs, cotangent):
    group_count = lax.axis_size("grp")
    shard_count = lax.axis_size("shard")
    bag = lookups.shape[2]
    win_size = tables.shape[1] // group_count

    def across(label, values, grp_step, shard_step):
        pairs = [
            (grp * shard_count + shard, (grp ^ grp_step) * shard_count + (shard ^ shard_step))
            for grp in range(group_count)
            for shard in range(shard_count)
        ]
        with jax.named_scope(label):
            return lax.ppermute(values, ("grp", "shard"), pairs)

    steps = list(range(shard_count - 1, 1, -2))
    looked = lookups[:, 0, :].T
    hot_own, places_own, wide_own = load_first(starts, looked, bottom_out, tables[0], group_count)
    hot_other = across("hot", hot_own, 0, 1)
    places = [places_own] + [across(f"place{step}", places_own, 0, step) for step in steps]
    linear = linear_part(bottom_out, top_dense)
    sums = [pool_rows(block, hot_own, hot_other, bag) for block in places]
    parts = [sums[0]] + [
        across(f"part{step}", part, 0, step) for part, step in zip(sums[1:], steps)
    ]
    wides = [wide_own] + [across(f"wide{step}", wide_own, 0, step) for step in steps]
    score_row, pooled = score(parts, bottom_out, linear, top_pairs, cotangent)
    scores = [score_row] + [across(f"score{step}", score_row, 0, step) for step in steps]
    activation, bottom_grad = finish_dense(
        pooled, bottom_out, linear, top_pairs, cotangent, top_dense
    )
    given = row_grads(scores, places, wides, bag, group_count, False)
    received = across("rows", given, 0, 1)
    kept = row_grads(scores, places, wides, bag, group_count, True)
    owned = split_owners(kept, received, group_count)
    blocks = [owned[0]] + [
        across(f"owned{step}", owned[step], step, 1) for step in range(1, group_count)
    ]
    table_grad = place_rows(starts, blocks, win_size)
    return activation, bottom_grad, table_grad[None, None]


def is_power(number):
    return number & (number - 1) == 0


def on_device(bottom_out, lookups, starts, tables, top_dense, top_pairs, cotangent):
    group_count = lax.axis_size("grp")
    shard_count = lax.axis_size("shard")
    group_lookups = lookups.shape[0] * lookups.shape[2] * shard_count
    hot_rows = group_count * HOT * shard_count
    fits = (
        tables.shape[0] == 1
        and lookups.shape[2] <= 8
        and bottom_out.shape[0] == tables.shape[2]
        and is_power(group_count)
        and is_power(shard_count)
        and tables.shape[1] // group_count % 8 == 0
        and hot_rows <= group_lookups
        and shard_count % 2 == 0
    )
    plan = by_hot_rows if fits else by_row_sums
    return plan(bottom_out, lookups, starts, tables, top_dense, top_pairs, cotangent)


def solution(mesh):
    in_specs = (
        P(("grp", "shard"), None),
        P(("grp", "shard"), None, None),
        P(),
        P(None, "shard", None),
        P(),
        P(),
        P(("grp", "shard"), None),
    )
    out_specs = (
        P(("grp", "shard"), None),
        P(("grp", "shard"), None),
        P(None, "shard", "grp", None),
    )
    return jax.shard_map(
        on_device, mesh=mesh, in_specs=in_specs, out_specs=out_specs, check_vma=False
    )
```

```python
import math

import jax
import jax.numpy as jnp
from jax import lax
from jax.experimental import pallas as pl
from jax.experimental.pallas import tpu as pltpu
from jax.sharding import PartitionSpec as P


HOT = 64
GRANT = 8 * 1024 * 1024


def pair_list(number):
    return [(former, latter) for former in range(number) for latter in range(former + 1, number)]


def pool_lookups(tables, picked, offset):
    rows_count = picked.shape[0]
    table_count = picked.shape[1]
    bag_count = picked.shape[2]
    rows_block = math.gcd(rows_count, 512)
    bag_block = math.gcd(bag_count, 8)
    bag_turns = bag_count // bag_block
    span_rows = tables.shape[1]
    table_ids = jnp.arange(table_count, dtype=jnp.int32)[None, :, None]

    def pool_step(turn, running):
        row_turn = turn // bag_turns
        bag_turn = turn % bag_turns
        chosen = lax.dynamic_slice(
            picked,
            (row_turn * rows_block, 0, bag_turn * bag_block),
            (rows_block, table_count, bag_block),
        )
        local = chosen - offset
        inside = (local >= 0) & (local < span_rows)
        fetched = tables[table_ids, jnp.clip(local, 0, span_rows - 1)]
        summed = jnp.sum(jnp.where(inside[..., None], fetched, 0.0), axis=2)
        current = lax.dynamic_slice_in_dim(running, row_turn * rows_block, rows_block, 0)
        return lax.dynamic_update_slice_in_dim(running, current + summed, row_turn * rows_block, 0)

    start_value = jnp.zeros((rows_count, table_count, tables.shape[2]), jnp.float32)
    return lax.fori_loop(0, rows_count // rows_block * bag_turns, pool_step, start_value)


def add_lookups(running_grad, grads, picked, offset, span_rows):
    rows_count = picked.shape[0]
    table_count = picked.shape[1]
    bag_count = picked.shape[2]
    rows_block = math.gcd(rows_count, 512)
    bag_block = math.gcd(bag_count, 8)
    bag_turns = bag_count // bag_block
    table_ids = jnp.arange(table_count, dtype=jnp.int32)[None, :, None]

    def add_step(turn, running):
        row_turn = turn // bag_turns
        bag_turn = turn % bag_turns
        chosen = lax.dynamic_slice(
            picked,
            (row_turn * rows_block, 0, bag_turn * bag_block),
            (rows_block, table_count, bag_block),
        )
        grads_block = lax.dynamic_slice_in_dim(grads, row_turn * rows_block, rows_block, 0)
        local = chosen - offset
        inside = (local >= 0) & (local < span_rows)
        updates = jnp.where(inside[..., None], grads_block[:, :, None, :], 0.0)
        return running.at[table_ids, jnp.clip(local, 0, span_rows - 1)].add(updates)

    return lax.fori_loop(0, rows_count // rows_block * bag_turns, add_step, running_grad)


def by_row_sums(bottom_out, lookups, starts, tables, top_dense, top_pairs, cotangent):
    shard_pos = lax.axis_index("shard")
    grp_pos = lax.axis_index("grp")
    group_count = lax.axis_size("grp")
    span_rows = tables.shape[1]
    table_count = tables.shape[0]
    width = tables.shape[2]
    win_size = span_rows // group_count
    offset = shard_pos * span_rows
    my_starts = lax.dynamic_index_in_dim(starts, grp_pos, 0, keepdims=False)
    window = lookups // win_size
    inner = lookups % win_size
    own_rows = window * win_size + (inner + my_starts[window]) % win_size
    group_idx = lax.all_gather(own_rows, "shard", axis=0, tiled=True)
    picked = group_idx
    pooled = lax.psum_scatter(
        pool_lookups(tables, picked, offset), "shard", scatter_dimension=0, tiled=True
    )
    vectors = [bottom_out.astype(jnp.float32)] + [pooled[:, 0]]
    couples = pair_list(table_count + 1)
    pair_dots = jnp.stack(
        [jnp.sum(vectors[former] * vectors[latter], axis=-1) for former, latter in couples], axis=1
    )
    preact = jnp.dot(bottom_out, top_dense, preferred_element_type=jnp.float32)
    preact = preact + jnp.dot(pair_dots, top_pairs, precision=lax.Precision.HIGHEST)
    sigmoid_pre = jax.nn.sigmoid(preact)
    activation = (preact * sigmoid_pre).astype(jnp.bfloat16)
    pre_grad = cotangent * sigmoid_pre * (1.0 + preact * (1.0 - sigmoid_pre))
    pair_grad = jnp.dot(pre_grad, top_pairs.T, precision=lax.Precision.HIGHEST)
    vec_grads = [jnp.zeros_like(vector) for vector in vectors]
    for former, latter in couples:
        vec_grads[former] = pair_grad * vectors[latter]
        vec_grads[latter] = pair_grad * vectors[former]
    pre_half = pre_grad.astype(jnp.bfloat16)
    bottom_grad = (
        lax.dot_general(
            pre_half, top_dense, (((1,), (1,)), ((), ())), preferred_element_type=jnp.float32
        )
        + vec_grads[0]
    )
    pooled_grad = jnp.stack(vec_grads[1:], axis=1)
    start_grad = jnp.zeros((table_count, span_rows, width), jnp.float32)
    picked = group_idx
    local_grad = add_lookups(
        start_grad,
        lax.all_gather(pooled_grad, "shard", axis=0, tiled=True),
        picked,
        offset,
        span_rows,
    )
    hot_range = jnp.arange(HOT, dtype=jnp.int32)
    owner_range = jnp.arange(group_count, dtype=jnp.int32)
    send_starts = lax.dynamic_slice_in_dim(my_starts, shard_pos * group_count, group_count, 0)
    send_index = (
        owner_range[:, None] * win_size + (send_starts[:, None] + hot_range[None, :]) % win_size
    )
    packed = local_grad[:, send_index]
    received = lax.all_to_all(packed, "grp", split_axis=1, concat_axis=1, tiled=True)
    recv_starts = lax.dynamic_slice_in_dim(starts, shard_pos * group_count + grp_pos, 1, 1)[:, 0]
    places = ((recv_starts[:, None] + hot_range[None, :]) % win_size).reshape(-1)
    flat_rows = received.reshape(table_count, group_count * HOT, width)
    table_grad = jnp.zeros((table_count, win_size, width), jnp.float32).at[:, places].add(flat_rows)
    return (activation, bottom_grad, table_grad[:, None])


def whole(memory=pltpu.VMEM):
    return pl.BlockSpec(memory_space=memory)


def cost(flops, moved):
    return pl.CostEstimate(flops=int(flops), bytes_accessed=int(moved), transcendentals=0)


def two_terms(values):
    high = values.astype(jnp.bfloat16)
    low = (values - high.astype(jnp.float32)).astype(jnp.bfloat16)
    return high, low


def dot_two(counts, values):
    high, low = two_terms(values)
    return jnp.dot(counts, high, preferred_element_type=jnp.float32) + jnp.dot(
        counts, low, preferred_element_type=jnp.float32
    )


def stay(values):
    return pltpu.with_memory_space_constraint(values, pltpu.HBM)


def load_first(starts, looked, bottom_out, table, group_count):
    span_rows, width = table.shape
    win_size = span_rows // group_count
    samples = bottom_out.shape[0]
    bag = looked.shape[0]
    head = min(HOT + 8, win_size)

    def kernel(starts_ref, looked_ref, bottom_ref, table_ref, hot_ref, places_ref, near_ref, wide_ref, held, sems):
        grp_pos = lax.axis_index("grp")
        shard_pos = lax.axis_index("shard")
        shifts = []
        copies = []
        for window in range(group_count):
            start = starts_ref[grp_pos, shard_pos * group_count + window]
            aligned = jnp.minimum(start // 8 * 8, win_size - head)
            shifts.append(start - aligned)
            base = window * win_size
            first = pltpu.make_async_copy(
                table_ref.at[pl.ds(pl.multiple_of(base + aligned, 8), head)],
                held.at[window, pl.ds(0, head)],
                sems.at[window, 0],
            )
            second = pltpu.make_async_copy(
                table_ref.at[pl.ds(base, HOT)], held.at[window, pl.ds(head, HOT)], sems.at[window, 1]
            )
            first.start()
            second.start()
            copies += [first, second]
        found = looked_ref[...]
        window_of = jnp.floor((found.astype(jnp.float32) + 0.5) * (1.0 / win_size)).astype(jnp.int32)
        places = (found - window_of * (win_size - HOT)).astype(jnp.float32)
        places = jnp.concatenate([places, jnp.zeros((8 - bag, samples), jnp.float32)], axis=0)
        places_ref[...] = places
        near_ref[pl.ds(0, 8), :] = places
        wide = bottom_ref[...].astype(jnp.float32)
        near_ref[pl.ds(8, samples), :] = wide
        wide_ref[...] = wide
        for copy in copies:
            copy.wait()
        for window in range(group_count):
            hot_ref[pl.ds(window * HOT, HOT), :] = held[window, pl.ds(shifts[window], HOT), :]

    return pl.pallas_call(
        kernel,
        out_shape=(
            jax.ShapeDtypeStruct((group_count * HOT, width), jnp.float32),
            jax.ShapeDtypeStruct((8, samples), jnp.float32),
            jax.ShapeDtypeStruct((samples + 8, width), jnp.float32),
            jax.ShapeDtypeStruct((samples, width), jnp.float32),
        ),
        in_specs=[whole(pltpu.SMEM), whole(), whole(), whole(pl.ANY)],
        out_specs=(whole(), whole(), whole(), whole()),
        scratch_shapes=[
            pltpu.VMEM((group_count, head + HOT, width), jnp.float32),
            pltpu.SemaphoreType.DMA((group_count, 2)),
        ],
        cost_estimate=cost(1e6, 1e6),
        compiler_params=pltpu.CompilerParams(vmem_limit_bytes=GRANT),
        name="load_first",
    )(stay(starts), stay(looked), stay(bottom_out), stay(table))


def linear_part(bottom_out, top_dense):
    def kernel(bottom_ref, dense_ref, linear_ref):
        linear_ref[...] = jnp.dot(bottom_ref[...], dense_ref[...], preferred_element_type=jnp.float32)

    return pl.pallas_call(
        kernel,
        out_shape=jax.ShapeDtypeStruct((bottom_out.shape[0], top_dense.shape[1]), jnp.float32),
        in_specs=[whole()] * 2,
        out_specs=whole(),
        cost_estimate=cost(3e7, 1e6),
        compiler_params=pltpu.CompilerParams(vmem_limit_bytes=GRANT),
        name="linear_part",
    )(bottom_out, top_dense)


def pool_rows(places, hot_own, hot_other, bag):
    block_rows, width = hot_own.shape
    samples = places.shape[1]

    def kernel(places_ref, own_ref, other_ref, part_ref):
        shard_pos = lax.axis_index("shard")
        rows = lax.broadcasted_iota(jnp.int32, (samples, block_rows), 1).astype(jnp.float32)
        columns = jnp.concatenate(
            [places_ref[pl.ds(0, 8), :], jnp.zeros((samples - 8, samples), jnp.float32)], axis=0
        ).T
        total = jnp.zeros((samples, width), jnp.float32)
        for side, ref in enumerate((own_ref, other_ref)):
            base = (jnp.bitwise_xor(shard_pos, side) * block_rows).astype(jnp.float32)
            times = jnp.zeros((samples, block_rows), jnp.float32)
            for slot in range(bag):
                times += jnp.where(columns[:, slot : slot + 1] - base == rows, 1.0, 0.0)
            total += dot_two(times.astype(jnp.bfloat16), ref[...])
        part_ref[...] = total

    return pl.pallas_call(
        kernel,
        out_shape=jax.ShapeDtypeStruct((samples, width), jnp.float32),
        in_specs=[whole()] * 3,
        out_specs=whole(),
        cost_estimate=cost(5e7, 1e6),
        compiler_params=pltpu.CompilerParams(vmem_limit_bytes=GRANT),
        name="pool_rows",
    )(places, hot_own, hot_other)


def head_terms(pooled, bottom_ref, linear_ref, pairs_ref, cot_ref):
    dots = jnp.sum(bottom_ref[...].astype(jnp.float32) * pooled, axis=1, keepdims=True)
    preact = linear_ref[...] + dots * pairs_ref[...]
    sig = 1.0 / (1.0 + jnp.exp(-preact))
    pre_grad = cot_ref[...] * sig * (1.0 + preact * (1.0 - sig))
    pair_grad = jnp.sum(pre_grad * pairs_ref[...], axis=1, keepdims=True)
    return preact, sig, pre_grad, pair_grad


def score(parts, bottom_out, linear, top_pairs, cotangent):
    samples, width = bottom_out.shape
    count = len(parts)

    def kernel(*refs):
        bottom_ref, linear_ref, pairs_ref, cot_ref, row_ref, pooled_ref = refs[count:]
        pooled = refs[0][...]
        for ref in refs[1:count]:
            pooled = pooled + ref[...]
        pooled_ref[...] = pooled
        pair_grad = head_terms(pooled, bottom_ref, linear_ref, pairs_ref, cot_ref)[3]
        down = lax.broadcasted_iota(jnp.int32, (samples, samples), 0)
        across = lax.broadcasted_iota(jnp.int32, (samples, samples), 1)
        row_ref[...] = jnp.sum(jnp.where(down == across, pair_grad, 0.0), axis=0, keepdims=True)

    return pl.pallas_call(
        kernel,
        out_shape=(
            jax.ShapeDtypeStruct((1, samples), jnp.float32),
            jax.ShapeDtypeStruct((samples, width), jnp.float32),
        ),
        in_specs=[whole()] * (count + 4),
        out_specs=(whole(), whole()),
        cost_estimate=cost(1e7, 1e6),
        compiler_params=pltpu.CompilerParams(vmem_limit_bytes=GRANT),
        name="score",
    )(*parts, bottom_out, linear, top_pairs, cotangent)


def finish_dense(pooled, bottom_out, linear, top_pairs, cotangent, top_dense):
    samples, width = bottom_out.shape
    hidden = top_dense.shape[1]

    def kernel(pooled_ref, bottom_ref, linear_ref, pairs_ref, cot_ref, dense_ref, act_ref, grad_ref):
        pooled = pooled_ref[...]
        preact, sig, pre_grad, pair_grad = head_terms(pooled, bottom_ref, linear_ref, pairs_ref, cot_ref)
        act_ref[...] = (preact * sig).astype(jnp.bfloat16)
        grad_ref[...] = (
            lax.dot_general(
                pre_grad.astype(jnp.bfloat16),
                dense_ref[...],
                (((1,), (1,)), ((), ())),
                preferred_element_type=jnp.float32,
            )
            + pair_grad * pooled
        )

    return pl.pallas_call(
        kernel,
        out_shape=(
            jax.ShapeDtypeStruct((samples, hidden), jnp.bfloat16),
            jax.ShapeDtypeStruct((samples, width), jnp.float32),
        ),
        in_specs=[whole()] * 6,
        out_specs=(whole(), whole()),
        cost_estimate=cost(5e7, 1e6),
        compiler_params=pltpu.CompilerParams(vmem_limit_bytes=GRANT),
        name="finish_dense",
    )(pooled, bottom_out, linear, top_pairs, cotangent, top_dense)


def row_grads(scores, places, wides, bag, group_count, kept):
    samples = scores[0].shape[1]
    width = wides[0].shape[1]
    count = len(scores)

    def kernel(*refs):
        score_refs, place_refs, wide_refs = refs[:count], refs[count : 2 * count], refs[2 * count : -1]
        grp_pos = lax.axis_index("grp")
        shard_pos = lax.axis_index("shard")
        ids = []
        for step in range(group_count):
            holder = shard_pos if kept == (step == 0) else jnp.bitwise_xor(shard_pos, 1)
            first = (holder * group_count + jnp.bitwise_xor(grp_pos, step)) * HOT
            ids.append(lax.broadcasted_iota(jnp.int32, (HOT, samples), 0) + first)
        rows = jnp.concatenate(ids, axis=0).astype(jnp.float32)
        total = jnp.zeros((group_count * HOT, width), jnp.float32)
        for score_ref, place_ref, wide_ref in zip(score_refs, place_refs, wide_refs):
            times = jnp.zeros(rows.shape, jnp.float32)
            for slot in range(bag):
                times += jnp.where(place_ref[pl.ds(slot, 1), :] == rows, 1.0, 0.0)
            high, low = two_terms(times * score_ref[...])
            bottom = wide_ref[pl.ds(wide_ref.shape[0] - samples, samples), :].astype(jnp.bfloat16)
            total += jnp.dot(high, bottom, preferred_element_type=jnp.float32)
            total += jnp.dot(low, bottom, preferred_element_type=jnp.float32)
        refs[-1][...] = total

    return pl.pallas_call(
        kernel,
        out_shape=jax.ShapeDtypeStruct((group_count * HOT, width), jnp.float32),
        in_specs=[whole()] * (3 * count),
        out_specs=whole(),
        cost_estimate=cost(1e8, 1e6),
        compiler_params=pltpu.CompilerParams(vmem_limit_bytes=GRANT),
        name="row_grads_kept" if kept else "row_grads_given",
    )(*scores, *places, *wides)


def split_owners(kept, received, group_count):
    width = kept.shape[1]

    def kernel(kept_ref, received_ref, *out_refs):
        for step, out_ref in enumerate(out_refs):
            chosen = pl.ds(step * HOT, HOT)
            out_ref[...] = kept_ref[chosen, :] + received_ref[chosen, :]

    part = jax.ShapeDtypeStruct((HOT, width), jnp.float32)
    return pl.pallas_call(
        kernel,
        out_shape=(part,) * group_count,
        in_specs=[whole()] * 2,
        out_specs=(whole(),) * group_count,
        cost_estimate=cost(1e6, 1e6),
        compiler_params=pltpu.CompilerParams(vmem_limit_bytes=GRANT),
        name="split_owners",
    )(kept, received)


def place_rows(starts, blocks, win_size):
    width = blocks[0].shape[1]
    count = len(blocks)

    def kernel(starts_ref, *refs):
        block_refs = refs[:count]
        out_ref, held, sem = refs[count:]
        grp_pos = lax.axis_index("grp")
        column = lax.axis_index("shard") * count + grp_pos
        held[...] = jnp.zeros_like(held)
        for step, ref in enumerate(block_refs):
            start = starts_ref[jnp.bitwise_xor(grp_pos, step), column]
            held[pl.ds(start, HOT), :] += ref[...]
        held[pl.ds(0, HOT), :] += held[pl.ds(win_size, HOT), :]
        copy = pltpu.make_async_copy(held.at[pl.ds(0, win_size)], out_ref, sem)
        copy.start()
        copy.wait()

    return pl.pallas_call(
        kernel,
        out_shape=jax.ShapeDtypeStruct((win_size, width), jnp.float32),
        in_specs=[whole(pltpu.SMEM)] + [whole()] * count,
        out_specs=whole(pl.ANY),
        scratch_shapes=[pltpu.VMEM((win_size + HOT, width), jnp.float32), pltpu.SemaphoreType.DMA],
        cost_estimate=cost(1e6, 2e6),
        compiler_params=pltpu.CompilerParams(vmem_limit_bytes=GRANT),
        name="place_rows",
    )(starts, *blocks)


def by_hot_rows(bottom_out, lookups, starts, tables, top_dense, top_pairs, cotangent):
    group_count = lax.axis_size("grp")
    shard_count = lax.axis_size("shard")
    bag = lookups.shape[2]
    win_size = tables.shape[1] // group_count

    def across(values, grp_step, shard_step):
        pairs = [
            (grp * shard_count + shard, (grp ^ grp_step) * shard_count + (shard ^ shard_step))
            for grp in range(group_count)
            for shard in range(shard_count)
        ]
        return lax.ppermute(values, ("grp", "shard"), pairs)

    near = 3
    steps = list(range(shard_count - 1, near, -2))
    looked = lookups[:, 0, :].T
    hot_own, places_own, near_own, wide_own = load_first(
        starts, looked, bottom_out, tables[0], group_count
    )
    hot_other = across(hot_own, 0, 1)
    places = [across(places_own, 0, step) for step in steps]
    near_back = across(near_own, 0, near)
    linear = linear_part(bottom_out, top_dense)
    own_sums = pool_rows(places_own, hot_own, hot_other, bag)
    parts = [own_sums]
    for step, block in zip(steps + [near], places + [near_back]):
        part = pool_rows(block, hot_own, hot_other, bag)
        parts.append(across(part, 0, step))
    wides = [across(wide_own, 0, step) for step in steps]
    score_row, pooled = score(parts, bottom_out, linear, top_pairs, cotangent)
    scores = [score_row] + [across(score_row, 0, step) for step in steps + [near]]
    activation, bottom_grad = finish_dense(
        pooled, bottom_out, linear, top_pairs, cotangent, top_dense
    )
    places = [places_own] + places + [near_back]
    wides = [near_own] + wides + [near_back]
    given = row_grads(scores, places, wides, bag, group_count, False)
    received = across(given, 0, 1)
    kept = row_grads(scores, places, wides, bag, group_count, True)
    owned = split_owners(kept, received, group_count)
    blocks = [owned[0]] + [across(owned[step], step, 1) for step in range(1, group_count)]
    table_grad = place_rows(starts, blocks, win_size)
    return activation, bottom_grad, table_grad[None, None]


def is_power(number):
    return number & (number - 1) == 0


def on_device(bottom_out, lookups, starts, tables, top_dense, top_pairs, cotangent):
    group_count = lax.axis_size("grp")
    shard_count = lax.axis_size("shard")
    group_lookups = lookups.shape[0] * lookups.shape[2] * shard_count
    hot_rows = group_count * HOT * shard_count
    fits = (
        tables.shape[0] == 1
        and lookups.shape[2] <= 8
        and bottom_out.shape[0] == tables.shape[2]
        and is_power(group_count)
        and is_power(shard_count)
        and tables.shape[1] // group_count % 8 == 0
        and hot_rows <= group_lookups
        and shard_count >= 8
    )
    plan = by_hot_rows if fits else by_row_sums
    return plan(bottom_out, lookups, starts, tables, top_dense, top_pairs, cotangent)


def solution(mesh):
    in_specs = (
        P(("grp", "shard"), None),
        P(("grp", "shard"), None, None),
        P(),
        P(None, "shard", None),
        P(),
        P(),
        P(("grp", "shard"), None),
    )
    out_specs = (
        P(("grp", "shard"), None),
        P(("grp", "shard"), None),
        P(None, "shard", "grp", None),
    )
    return jax.shard_map(
        on_device, mesh=mesh, in_specs=in_specs, out_specs=out_specs, check_vma=False
    )
```

```python
import math

import jax
import jax.numpy as jnp
from jax import lax
from jax.experimental import pallas as pl
from jax.experimental.pallas import tpu as pltpu
from jax.sharding import PartitionSpec as P


HOT = 64
GRANT = 8 * 1024 * 1024


def pair_list(number):
    return [(former, latter) for former in range(number) for latter in range(former + 1, number)]


def pool_lookups(tables, picked, offset):
    rows_count = picked.shape[0]
    table_count = picked.shape[1]
    bag_count = picked.shape[2]
    rows_block = math.gcd(rows_count, 512)
    bag_block = math.gcd(bag_count, 8)
    bag_turns = bag_count // bag_block
    span_rows = tables.shape[1]
    table_ids = jnp.arange(table_count, dtype=jnp.int32)[None, :, None]

    def pool_step(turn, running):
        row_turn = turn // bag_turns
        bag_turn = turn % bag_turns
        chosen = lax.dynamic_slice(
            picked,
            (row_turn * rows_block, 0, bag_turn * bag_block),
            (rows_block, table_count, bag_block),
        )
        local = chosen - offset
        inside = (local >= 0) & (local < span_rows)
        fetched = tables[table_ids, jnp.clip(local, 0, span_rows - 1)]
        summed = jnp.sum(jnp.where(inside[..., None], fetched, 0.0), axis=2)
        current = lax.dynamic_slice_in_dim(running, row_turn * rows_block, rows_block, 0)
        return lax.dynamic_update_slice_in_dim(running, current + summed, row_turn * rows_block, 0)

    start_value = jnp.zeros((rows_count, table_count, tables.shape[2]), jnp.float32)
    return lax.fori_loop(0, rows_count // rows_block * bag_turns, pool_step, start_value)


def add_lookups(running_grad, grads, picked, offset, span_rows):
    rows_count = picked.shape[0]
    table_count = picked.shape[1]
    bag_count = picked.shape[2]
    rows_block = math.gcd(rows_count, 512)
    bag_block = math.gcd(bag_count, 8)
    bag_turns = bag_count // bag_block
    table_ids = jnp.arange(table_count, dtype=jnp.int32)[None, :, None]

    def add_step(turn, running):
        row_turn = turn // bag_turns
        bag_turn = turn % bag_turns
        chosen = lax.dynamic_slice(
            picked,
            (row_turn * rows_block, 0, bag_turn * bag_block),
            (rows_block, table_count, bag_block),
        )
        grads_block = lax.dynamic_slice_in_dim(grads, row_turn * rows_block, rows_block, 0)
        local = chosen - offset
        inside = (local >= 0) & (local < span_rows)
        updates = jnp.where(inside[..., None], grads_block[:, :, None, :], 0.0)
        return running.at[table_ids, jnp.clip(local, 0, span_rows - 1)].add(updates)

    return lax.fori_loop(0, rows_count // rows_block * bag_turns, add_step, running_grad)


def by_row_sums(bottom_out, lookups, starts, tables, top_dense, top_pairs, cotangent):
    shard_pos = lax.axis_index("shard")
    grp_pos = lax.axis_index("grp")
    group_count = lax.axis_size("grp")
    span_rows = tables.shape[1]
    table_count = tables.shape[0]
    width = tables.shape[2]
    win_size = span_rows // group_count
    offset = shard_pos * span_rows
    my_starts = lax.dynamic_index_in_dim(starts, grp_pos, 0, keepdims=False)
    window = lookups // win_size
    inner = lookups % win_size
    own_rows = window * win_size + (inner + my_starts[window]) % win_size
    group_idx = lax.all_gather(own_rows, "shard", axis=0, tiled=True)
    picked = group_idx
    pooled = lax.psum_scatter(
        pool_lookups(tables, picked, offset), "shard", scatter_dimension=0, tiled=True
    )
    vectors = [bottom_out.astype(jnp.float32)] + [pooled[:, 0]]
    couples = pair_list(table_count + 1)
    pair_dots = jnp.stack(
        [jnp.sum(vectors[former] * vectors[latter], axis=-1) for former, latter in couples], axis=1
    )
    preact = jnp.dot(bottom_out, top_dense, preferred_element_type=jnp.float32)
    preact = preact + jnp.dot(pair_dots, top_pairs, precision=lax.Precision.HIGHEST)
    sigmoid_pre = jax.nn.sigmoid(preact)
    activation = (preact * sigmoid_pre).astype(jnp.bfloat16)
    pre_grad = cotangent * sigmoid_pre * (1.0 + preact * (1.0 - sigmoid_pre))
    pair_grad = jnp.dot(pre_grad, top_pairs.T, precision=lax.Precision.HIGHEST)
    vec_grads = [jnp.zeros_like(vector) for vector in vectors]
    for former, latter in couples:
        vec_grads[former] = pair_grad * vectors[latter]
        vec_grads[latter] = pair_grad * vectors[former]
    pre_half = pre_grad.astype(jnp.bfloat16)
    bottom_grad = (
        lax.dot_general(
            pre_half, top_dense, (((1,), (1,)), ((), ())), preferred_element_type=jnp.float32
        )
        + vec_grads[0]
    )
    pooled_grad = jnp.stack(vec_grads[1:], axis=1)
    start_grad = jnp.zeros((table_count, span_rows, width), jnp.float32)
    picked = group_idx
    local_grad = add_lookups(
        start_grad,
        lax.all_gather(pooled_grad, "shard", axis=0, tiled=True),
        picked,
        offset,
        span_rows,
    )
    hot_range = jnp.arange(HOT, dtype=jnp.int32)
    owner_range = jnp.arange(group_count, dtype=jnp.int32)
    send_starts = lax.dynamic_slice_in_dim(my_starts, shard_pos * group_count, group_count, 0)
    send_index = (
        owner_range[:, None] * win_size + (send_starts[:, None] + hot_range[None, :]) % win_size
    )
    packed = local_grad[:, send_index]
    received = lax.all_to_all(packed, "grp", split_axis=1, concat_axis=1, tiled=True)
    recv_starts = lax.dynamic_slice_in_dim(starts, shard_pos * group_count + grp_pos, 1, 1)[:, 0]
    places = ((recv_starts[:, None] + hot_range[None, :]) % win_size).reshape(-1)
    flat_rows = received.reshape(table_count, group_count * HOT, width)
    table_grad = jnp.zeros((table_count, win_size, width), jnp.float32).at[:, places].add(flat_rows)
    return (activation, bottom_grad, table_grad[:, None])


def whole(memory=pltpu.VMEM):
    return pl.BlockSpec(memory_space=memory)


def cost(flops, moved):
    return pl.CostEstimate(flops=int(flops), bytes_accessed=int(moved), transcendentals=0)


def two_terms(values):
    high = values.astype(jnp.bfloat16)
    low = (values - high.astype(jnp.float32)).astype(jnp.bfloat16)
    return high, low


def stay(values):
    return pltpu.with_memory_space_constraint(values, pltpu.HBM)


def load_first(starts, looked, bottom_out, table, group_count):
    span_rows, width = table.shape
    win_size = span_rows // group_count
    samples = bottom_out.shape[0]
    bag = looked.shape[0]
    head = min(HOT + 8, win_size)

    def kernel(starts_ref, looked_ref, bottom_ref, table_ref, hot_ref, places_ref, near_ref, wide_ref, held, sems):
        grp_pos = lax.axis_index("grp")
        shard_pos = lax.axis_index("shard")
        shifts = []
        copies = []
        for window in range(group_count):
            start = starts_ref[grp_pos, shard_pos * group_count + window]
            aligned = jnp.minimum(start // 8 * 8, win_size - head)
            shifts.append(start - aligned)
            base = window * win_size
            first = pltpu.make_async_copy(
                table_ref.at[pl.ds(pl.multiple_of(base + aligned, 8), head)],
                held.at[window, pl.ds(0, head)],
                sems.at[window, 0],
            )
            second = pltpu.make_async_copy(
                table_ref.at[pl.ds(base, HOT)], held.at[window, pl.ds(head, HOT)], sems.at[window, 1]
            )
            first.start()
            second.start()
            copies += [first, second]
        found = looked_ref[...]
        window_of = jnp.floor((found.astype(jnp.float32) + 0.5) * (1.0 / win_size)).astype(jnp.int32)
        places = (found - window_of * (win_size - HOT)).astype(jnp.float32)
        places = jnp.concatenate([places, jnp.zeros((8 - bag, samples), jnp.float32)], axis=0)
        places_ref[...] = places
        near_ref[pl.ds(0, 8), :] = places
        wide = bottom_ref[...].astype(jnp.float32)
        near_ref[pl.ds(8, samples), :] = wide
        wide_ref[...] = wide
        for copy in copies:
            copy.wait()
        for window in range(group_count):
            hot_ref[pl.ds(window * HOT, HOT), :] = held[window, pl.ds(shifts[window], HOT), :]

    return pl.pallas_call(
        kernel,
        out_shape=(
            jax.ShapeDtypeStruct((group_count * HOT, width), jnp.float32),
            jax.ShapeDtypeStruct((8, samples), jnp.float32),
            jax.ShapeDtypeStruct((samples + 8, width), jnp.float32),
            jax.ShapeDtypeStruct((samples, width), jnp.float32),
        ),
        in_specs=[whole(pltpu.SMEM), whole(), whole(), whole(pl.ANY)],
        out_specs=(whole(), whole(), whole(), whole()),
        scratch_shapes=[
            pltpu.VMEM((group_count, head + HOT, width), jnp.float32),
            pltpu.SemaphoreType.DMA((group_count, 2)),
        ],
        cost_estimate=cost(1e6, 1e6),
        compiler_params=pltpu.CompilerParams(vmem_limit_bytes=GRANT),
        name="load_first",
    )(stay(starts), stay(looked), stay(bottom_out), stay(table))


def linear_part(bottom_out, top_dense):
    def kernel(bottom_ref, dense_ref, linear_ref):
        linear_ref[...] = jnp.dot(bottom_ref[...], dense_ref[...], preferred_element_type=jnp.float32)

    return pl.pallas_call(
        kernel,
        out_shape=jax.ShapeDtypeStruct((bottom_out.shape[0], top_dense.shape[1]), jnp.float32),
        in_specs=[whole()] * 2,
        out_specs=whole(),
        cost_estimate=cost(3e7, 1e6),
        compiler_params=pltpu.CompilerParams(vmem_limit_bytes=GRANT),
        name="linear_part",
    )(bottom_out, top_dense)


def hot_terms(hot_own, hot_other):
    block_rows, width = hot_own.shape

    def kernel(own_ref, other_ref, terms_ref):
        for side, ref in enumerate((own_ref, other_ref)):
            high, low = two_terms(ref[...])
            chosen = pl.ds(side * block_rows, block_rows)
            terms_ref[chosen, pl.ds(0, width)] = high
            terms_ref[chosen, pl.ds(width, width)] = low

    return pl.pallas_call(
        kernel,
        out_shape=jax.ShapeDtypeStruct((2 * block_rows, 2 * width), jnp.bfloat16),
        in_specs=[whole()] * 2,
        out_specs=whole(),
        cost_estimate=cost(1e6, 1e6),
        compiler_params=pltpu.CompilerParams(vmem_limit_bytes=GRANT),
        name="hot_terms",
    )(hot_own, hot_other)


def pool_rows(places, terms, bag):
    block_rows = terms.shape[0] // 2
    width = terms.shape[1] // 2
    samples = places.shape[1]

    def kernel(places_ref, terms_ref, part_ref):
        shard_pos = lax.axis_index("shard")
        columns = jnp.concatenate(
            [places_ref[pl.ds(0, 8), :], jnp.zeros((samples - 8, samples), jnp.float32)], axis=0
        ).T
        spread = [
            jnp.broadcast_to(columns[:, slot : slot + 1], (samples, block_rows)) for slot in range(bag)
        ]
        both = []
        for side in range(2):
            first = jnp.bitwise_xor(shard_pos, side) * block_rows
            rows = lax.broadcasted_iota(jnp.int32, (samples, block_rows), 1) + first
            rows = rows.astype(jnp.float32)
            times = jnp.where(spread[0] == rows, 1.0, 0.0)
            for column in spread[1:]:
                times = jnp.where(column == rows, times + 1.0, times)
            both.append(times.astype(jnp.bfloat16))
        total = jnp.dot(
            jnp.concatenate(both, axis=1), terms_ref[...], preferred_element_type=jnp.float32
        )
        part_ref[...] = total[:, :width] + total[:, width:]

    return pl.pallas_call(
        kernel,
        out_shape=jax.ShapeDtypeStruct((samples, width), jnp.float32),
        in_specs=[whole()] * 2,
        out_specs=whole(),
        cost_estimate=cost(5e7, 1e6),
        compiler_params=pltpu.CompilerParams(vmem_limit_bytes=GRANT),
        name="pool_rows",
    )(places, terms)


def head_terms(pooled, bottom_ref, linear_ref, pairs_ref, cot_ref):
    dots = jnp.sum(bottom_ref[...].astype(jnp.float32) * pooled, axis=1, keepdims=True)
    preact = linear_ref[...] + dots * pairs_ref[...]
    sig = 1.0 / (1.0 + jnp.exp(-preact))
    pre_grad = cot_ref[...] * sig * (1.0 + preact * (1.0 - sig))
    pair_grad = jnp.sum(pre_grad * pairs_ref[...], axis=1, keepdims=True)
    return preact, sig, pre_grad, pair_grad


def score(parts, bottom_out, linear, top_pairs, cotangent):
    samples, width = bottom_out.shape
    count = len(parts)

    def kernel(*refs):
        bottom_ref, linear_ref, pairs_ref, cot_ref, row_ref, pooled_ref = refs[count:]
        pooled = refs[0][...]
        for ref in refs[1:count]:
            pooled = pooled + ref[...]
        pooled_ref[...] = pooled
        pair_grad = head_terms(pooled, bottom_ref, linear_ref, pairs_ref, cot_ref)[3]
        down = lax.broadcasted_iota(jnp.int32, (samples, samples), 0)
        across = lax.broadcasted_iota(jnp.int32, (samples, samples), 1)
        row_ref[...] = jnp.sum(jnp.where(down == across, pair_grad, 0.0), axis=0, keepdims=True)

    return pl.pallas_call(
        kernel,
        out_shape=(
            jax.ShapeDtypeStruct((1, samples), jnp.float32),
            jax.ShapeDtypeStruct((samples, width), jnp.float32),
        ),
        in_specs=[whole()] * (count + 4),
        out_specs=(whole(), whole()),
        cost_estimate=cost(1e7, 1e6),
        compiler_params=pltpu.CompilerParams(vmem_limit_bytes=GRANT),
        name="score",
    )(*parts, bottom_out, linear, top_pairs, cotangent)


def finish_dense(pooled, bottom_out, linear, top_pairs, cotangent, top_dense, win_size):
    samples, width = bottom_out.shape
    hidden = top_dense.shape[1]

    def kernel(
        pooled_ref, bottom_ref, linear_ref, pairs_ref, cot_ref, dense_ref, act_ref, grad_ref,
        blank_ref, zeros, sem,
    ):
        zeros[...] = jnp.zeros_like(zeros)
        copy = pltpu.make_async_copy(zeros, blank_ref, sem)
        copy.start()
        pooled = pooled_ref[...]
        preact, sig, pre_grad, pair_grad = head_terms(pooled, bottom_ref, linear_ref, pairs_ref, cot_ref)
        act_ref[...] = (preact * sig).astype(jnp.bfloat16)
        grad_ref[...] = (
            lax.dot_general(
                pre_grad.astype(jnp.bfloat16),
                dense_ref[...],
                (((1,), (1,)), ((), ())),
                preferred_element_type=jnp.float32,
            )
            + pair_grad * pooled
        )
        copy.wait()

    return pl.pallas_call(
        kernel,
        out_shape=(
            jax.ShapeDtypeStruct((samples, hidden), jnp.bfloat16),
            jax.ShapeDtypeStruct((samples, width), jnp.float32),
            jax.ShapeDtypeStruct((win_size, width), jnp.float32),
        ),
        in_specs=[whole()] * 6,
        out_specs=(whole(), whole(), whole(pltpu.HBM)),
        scratch_shapes=[pltpu.VMEM((win_size, width), jnp.float32), pltpu.SemaphoreType.DMA],
        cost_estimate=cost(5e7, 1e6),
        compiler_params=pltpu.CompilerParams(vmem_limit_bytes=GRANT),
        name="finish_dense",
    )(pooled, bottom_out, linear, top_pairs, cotangent, top_dense)


def row_grads(scores, places, wides, bag, group_count, kept):
    samples = scores[0].shape[1]
    width = wides[0].shape[1]
    count = len(scores)

    def kernel(*refs):
        score_refs, place_refs, wide_refs = refs[:count], refs[count : 2 * count], refs[2 * count : -1]
        grp_pos = lax.axis_index("grp")
        shard_pos = lax.axis_index("shard")
        ids = []
        for step in range(group_count):
            holder = shard_pos if kept == (step == 0) else jnp.bitwise_xor(shard_pos, 1)
            first = (holder * group_count + jnp.bitwise_xor(grp_pos, step)) * HOT
            ids.append(lax.broadcasted_iota(jnp.int32, (HOT, samples), 0) + first)
        rows = jnp.concatenate(ids, axis=0).astype(jnp.float32)
        total = jnp.zeros((group_count * HOT, width), jnp.float32)
        for score_ref, place_ref, wide_ref in zip(score_refs, place_refs, wide_refs):
            times = jnp.zeros(rows.shape, jnp.float32)
            for slot in range(bag):
                times += jnp.where(place_ref[pl.ds(slot, 1), :] == rows, 1.0, 0.0)
            high, low = two_terms(times * score_ref[...])
            bottom = wide_ref[pl.ds(wide_ref.shape[0] - samples, samples), :].astype(jnp.bfloat16)
            total += jnp.dot(high, bottom, preferred_element_type=jnp.float32)
            total += jnp.dot(low, bottom, preferred_element_type=jnp.float32)
        refs[-1][...] = total

    return pl.pallas_call(
        kernel,
        out_shape=jax.ShapeDtypeStruct((group_count * HOT, width), jnp.float32),
        in_specs=[whole()] * (3 * count),
        out_specs=whole(),
        cost_estimate=cost(1e8, 1e6),
        compiler_params=pltpu.CompilerParams(vmem_limit_bytes=GRANT),
        name="row_grads_kept" if kept else "row_grads_given",
    )(*scores, *places, *wides)


def split_owners(kept, received, group_count):
    width = kept.shape[1]

    def kernel(kept_ref, received_ref, *out_refs):
        for step, out_ref in enumerate(out_refs):
            chosen = pl.ds(step * HOT, HOT)
            out_ref[...] = kept_ref[chosen, :] + received_ref[chosen, :]

    part = jax.ShapeDtypeStruct((HOT, width), jnp.float32)
    return pl.pallas_call(
        kernel,
        out_shape=(part,) * group_count,
        in_specs=[whole()] * 2,
        out_specs=(whole(),) * group_count,
        cost_estimate=cost(1e6, 1e6),
        compiler_params=pltpu.CompilerParams(vmem_limit_bytes=GRANT),
        name="split_owners",
    )(kept, received)


def place_rows(starts, blocks, blank):
    win_size, width = blank.shape
    count = len(blocks)
    head = min(HOT + 8, win_size)

    def kernel(starts_ref, *refs):
        block_refs = refs[:count]
        out_ref, held, sems = refs[count + 1 :]
        grp_pos = lax.axis_index("grp")
        column = lax.axis_index("shard") * count + grp_pos
        held[...] = jnp.zeros_like(held)
        firsts = [jnp.int32(0)]
        for step, ref in enumerate(block_refs):
            start = starts_ref[jnp.bitwise_xor(grp_pos, step), column]
            firsts.append(jnp.minimum(start // 8 * 8, win_size - head))
            held[pl.ds(start, HOT), :] += ref[...]
        held[pl.ds(0, HOT), :] += held[pl.ds(win_size, HOT), :]
        copies = []
        for place, first in enumerate(firsts):
            chosen = pl.ds(pl.multiple_of(first, 8), head)
            copy = pltpu.make_async_copy(held.at[chosen], out_ref.at[chosen], sems.at[place])
            copy.start()
            copies.append(copy)
        for copy in copies:
            copy.wait()

    return pl.pallas_call(
        kernel,
        out_shape=jax.ShapeDtypeStruct((win_size, width), jnp.float32),
        in_specs=[whole(pltpu.SMEM)] + [whole()] * count + [whole(pltpu.HBM)],
        out_specs=whole(pltpu.HBM),
        input_output_aliases={1 + count: 0},
        scratch_shapes=[
            pltpu.VMEM((win_size + HOT, width), jnp.float32),
            pltpu.SemaphoreType.DMA((count + 1,)),
        ],
        cost_estimate=cost(1e6, 2e6),
        compiler_params=pltpu.CompilerParams(vmem_limit_bytes=GRANT),
        name="place_rows",
    )(starts, *blocks, blank)


def by_hot_rows(bottom_out, lookups, starts, tables, top_dense, top_pairs, cotangent):
    group_count = lax.axis_size("grp")
    shard_count = lax.axis_size("shard")
    bag = lookups.shape[2]
    win_size = tables.shape[1] // group_count

    def across(values, grp_step, shard_step):
        pairs = [
            (grp * shard_count + shard, (grp ^ grp_step) * shard_count + (shard ^ shard_step))
            for grp in range(group_count)
            for shard in range(shard_count)
        ]
        return lax.ppermute(values, ("grp", "shard"), pairs)

    near = 3
    steps = list(range(shard_count - 1, near, -2))
    looked = lookups[:, 0, :].T
    hot_own, places_own, near_own, wide_own = load_first(
        starts, looked, bottom_out, tables[0], group_count
    )
    hot_other = across(hot_own, 0, 1)
    places = [across(places_own, 0, step) for step in steps]
    near_back = across(near_own, 0, near)
    terms = hot_terms(hot_own, hot_other)
    linear = linear_part(bottom_out, top_dense)
    own_sums = pool_rows(places_own, terms, bag)
    parts = [own_sums]
    for step, block in zip(steps + [near], places + [near_back]):
        part = pool_rows(block, terms, bag)
        parts.append(across(part, 0, step))
    wides = [across(wide_own, 0, step) for step in steps]
    score_row, pooled = score(parts, bottom_out, linear, top_pairs, cotangent)
    scores = [score_row] + [across(score_row, 0, step) for step in steps + [near]]
    activation, bottom_grad, blank = finish_dense(
        pooled, bottom_out, linear, top_pairs, cotangent, top_dense, win_size
    )
    places = [places_own] + places + [near_back]
    wides = [near_own] + wides + [near_back]
    given = row_grads(scores, places, wides, bag, group_count, False)
    received = across(given, 0, 1)
    kept = row_grads(scores, places, wides, bag, group_count, True)
    owned = split_owners(kept, received, group_count)
    blocks = [owned[0]] + [across(owned[step], step, 1) for step in range(1, group_count)]
    table_grad = place_rows(starts, blocks, blank)
    return activation, bottom_grad, table_grad[None, None]


def is_power(number):
    return number & (number - 1) == 0


def on_device(bottom_out, lookups, starts, tables, top_dense, top_pairs, cotangent):
    group_count = lax.axis_size("grp")
    shard_count = lax.axis_size("shard")
    group_lookups = lookups.shape[0] * lookups.shape[2] * shard_count
    hot_rows = group_count * HOT * shard_count
    fits = (
        tables.shape[0] == 1
        and lookups.shape[2] <= 8
        and bottom_out.shape[0] == tables.shape[2]
        and is_power(group_count)
        and is_power(shard_count)
        and tables.shape[1] // group_count % 8 == 0
        and hot_rows <= group_lookups
        and shard_count >= 8
    )
    plan = by_hot_rows if fits else by_row_sums
    return plan(bottom_out, lookups, starts, tables, top_dense, top_pairs, cotangent)


def solution(mesh):
    in_specs = (
        P(("grp", "shard"), None),
        P(("grp", "shard"), None, None),
        P(),
        P(None, "shard", None),
        P(),
        P(),
        P(("grp", "shard"), None),
    )
    out_specs = (
        P(("grp", "shard"), None),
        P(("grp", "shard"), None),
        P(None, "shard", "grp", None),
    )
    return jax.shard_map(
        on_device, mesh=mesh, in_specs=in_specs, out_specs=out_specs, check_vma=False
    )
```

```python
import math

import jax
import jax.numpy as jnp
from jax import lax
from jax.experimental import pallas as pl
from jax.experimental.pallas import tpu as pltpu
from jax.sharding import PartitionSpec as P


HOT = 64
GRANT = 8 * 1024 * 1024


def pair_list(number):
    return [(former, latter) for former in range(number) for latter in range(former + 1, number)]


def pool_lookups(tables, picked, offset):
    rows_count = picked.shape[0]
    table_count = picked.shape[1]
    bag_count = picked.shape[2]
    rows_block = math.gcd(rows_count, 512)
    bag_block = math.gcd(bag_count, 8)
    bag_turns = bag_count // bag_block
    span_rows = tables.shape[1]
    table_ids = jnp.arange(table_count, dtype=jnp.int32)[None, :, None]

    def pool_step(turn, running):
        row_turn = turn // bag_turns
        bag_turn = turn % bag_turns
        chosen = lax.dynamic_slice(
            picked,
            (row_turn * rows_block, 0, bag_turn * bag_block),
            (rows_block, table_count, bag_block),
        )
        local = chosen - offset
        inside = (local >= 0) & (local < span_rows)
        fetched = tables[table_ids, jnp.clip(local, 0, span_rows - 1)]
        summed = jnp.sum(jnp.where(inside[..., None], fetched, 0.0), axis=2)
        current = lax.dynamic_slice_in_dim(running, row_turn * rows_block, rows_block, 0)
        return lax.dynamic_update_slice_in_dim(running, current + summed, row_turn * rows_block, 0)

    start_value = jnp.zeros((rows_count, table_count, tables.shape[2]), jnp.float32)
    return lax.fori_loop(0, rows_count // rows_block * bag_turns, pool_step, start_value)


def add_lookups(running_grad, grads, picked, offset, span_rows):
    rows_count = picked.shape[0]
    table_count = picked.shape[1]
    bag_count = picked.shape[2]
    rows_block = math.gcd(rows_count, 512)
    bag_block = math.gcd(bag_count, 8)
    bag_turns = bag_count // bag_block
    table_ids = jnp.arange(table_count, dtype=jnp.int32)[None, :, None]

    def add_step(turn, running):
        row_turn = turn // bag_turns
        bag_turn = turn % bag_turns
        chosen = lax.dynamic_slice(
            picked,
            (row_turn * rows_block, 0, bag_turn * bag_block),
            (rows_block, table_count, bag_block),
        )
        grads_block = lax.dynamic_slice_in_dim(grads, row_turn * rows_block, rows_block, 0)
        local = chosen - offset
        inside = (local >= 0) & (local < span_rows)
        updates = jnp.where(inside[..., None], grads_block[:, :, None, :], 0.0)
        return running.at[table_ids, jnp.clip(local, 0, span_rows - 1)].add(updates)

    return lax.fori_loop(0, rows_count // rows_block * bag_turns, add_step, running_grad)


def by_row_sums(bottom_out, lookups, starts, tables, top_dense, top_pairs, cotangent):
    shard_pos = lax.axis_index("shard")
    grp_pos = lax.axis_index("grp")
    group_count = lax.axis_size("grp")
    span_rows = tables.shape[1]
    table_count = tables.shape[0]
    width = tables.shape[2]
    win_size = span_rows // group_count
    offset = shard_pos * span_rows
    my_starts = lax.dynamic_index_in_dim(starts, grp_pos, 0, keepdims=False)
    window = lookups // win_size
    inner = lookups % win_size
    own_rows = window * win_size + (inner + my_starts[window]) % win_size
    group_idx = lax.all_gather(own_rows, "shard", axis=0, tiled=True)
    picked = group_idx
    pooled = lax.psum_scatter(
        pool_lookups(tables, picked, offset), "shard", scatter_dimension=0, tiled=True
    )
    vectors = [bottom_out.astype(jnp.float32)] + [pooled[:, 0]]
    couples = pair_list(table_count + 1)
    pair_dots = jnp.stack(
        [jnp.sum(vectors[former] * vectors[latter], axis=-1) for former, latter in couples], axis=1
    )
    preact = jnp.dot(bottom_out, top_dense, preferred_element_type=jnp.float32)
    preact = preact + jnp.dot(pair_dots, top_pairs, precision=lax.Precision.HIGHEST)
    sigmoid_pre = jax.nn.sigmoid(preact)
    activation = (preact * sigmoid_pre).astype(jnp.bfloat16)
    pre_grad = cotangent * sigmoid_pre * (1.0 + preact * (1.0 - sigmoid_pre))
    pair_grad = jnp.dot(pre_grad, top_pairs.T, precision=lax.Precision.HIGHEST)
    vec_grads = [jnp.zeros_like(vector) for vector in vectors]
    for former, latter in couples:
        vec_grads[former] = pair_grad * vectors[latter]
        vec_grads[latter] = pair_grad * vectors[former]
    pre_half = pre_grad.astype(jnp.bfloat16)
    bottom_grad = (
        lax.dot_general(
            pre_half, top_dense, (((1,), (1,)), ((), ())), preferred_element_type=jnp.float32
        )
        + vec_grads[0]
    )
    pooled_grad = jnp.stack(vec_grads[1:], axis=1)
    start_grad = jnp.zeros((table_count, span_rows, width), jnp.float32)
    picked = group_idx
    local_grad = add_lookups(
        start_grad,
        lax.all_gather(pooled_grad, "shard", axis=0, tiled=True),
        picked,
        offset,
        span_rows,
    )
    hot_range = jnp.arange(HOT, dtype=jnp.int32)
    owner_range = jnp.arange(group_count, dtype=jnp.int32)
    send_starts = lax.dynamic_slice_in_dim(my_starts, shard_pos * group_count, group_count, 0)
    send_index = (
        owner_range[:, None] * win_size + (send_starts[:, None] + hot_range[None, :]) % win_size
    )
    packed = local_grad[:, send_index]
    received = lax.all_to_all(packed, "grp", split_axis=1, concat_axis=1, tiled=True)
    recv_starts = lax.dynamic_slice_in_dim(starts, shard_pos * group_count + grp_pos, 1, 1)[:, 0]
    places = ((recv_starts[:, None] + hot_range[None, :]) % win_size).reshape(-1)
    flat_rows = received.reshape(table_count, group_count * HOT, width)
    table_grad = jnp.zeros((table_count, win_size, width), jnp.float32).at[:, places].add(flat_rows)
    return (activation, bottom_grad, table_grad[:, None])


def whole(memory=pltpu.VMEM):
    return pl.BlockSpec(memory_space=memory)


def cost(flops, moved):
    return pl.CostEstimate(flops=int(flops), bytes_accessed=int(moved), transcendentals=0)


def two_terms(values):
    high = values.astype(jnp.bfloat16)
    low = (values - high.astype(jnp.float32)).astype(jnp.bfloat16)
    return high, low


def stay(values):
    return pltpu.with_memory_space_constraint(values, pltpu.HBM)


def load_first(starts, looked, bottom_out, table, group_count):
    span_rows, width = table.shape
    win_size = span_rows // group_count
    samples = bottom_out.shape[0]
    bag = looked.shape[0]
    head = min(HOT + 8, win_size)

    def kernel(starts_ref, looked_ref, bottom_ref, table_ref, hot_ref, places_ref, near_ref, wide_ref, held, sems):
        grp_pos = lax.axis_index("grp")
        shard_pos = lax.axis_index("shard")
        shifts = []
        copies = []
        for window in range(group_count):
            start = starts_ref[grp_pos, shard_pos * group_count + window]
            aligned = jnp.minimum(start // 8 * 8, win_size - head)
            shifts.append(start - aligned)
            base = window * win_size
            first = pltpu.make_async_copy(
                table_ref.at[pl.ds(pl.multiple_of(base + aligned, 8), head)],
                held.at[window, pl.ds(0, head)],
                sems.at[window, 0],
            )
            second = pltpu.make_async_copy(
                table_ref.at[pl.ds(base, HOT)], held.at[window, pl.ds(head, HOT)], sems.at[window, 1]
            )
            first.start()
            second.start()
            copies += [first, second]
        found = looked_ref[...]
        window_of = jnp.floor((found.astype(jnp.float32) + 0.5) * (1.0 / win_size)).astype(jnp.int32)
        places = (found - window_of * (win_size - HOT)).astype(jnp.float32)
        places = jnp.concatenate([places, jnp.zeros((8 - bag, samples), jnp.float32)], axis=0)
        places_ref[...] = places
        near_ref[pl.ds(0, 8), :] = places
        wide = bottom_ref[...].astype(jnp.float32)
        near_ref[pl.ds(8, samples), :] = wide
        wide_ref[...] = wide
        for copy in copies:
            copy.wait()
        for window in range(group_count):
            hot_ref[pl.ds(window * HOT, HOT), :] = held[window, pl.ds(shifts[window], HOT), :]

    return pl.pallas_call(
        kernel,
        out_shape=(
            jax.ShapeDtypeStruct((group_count * HOT, width), jnp.float32),
            jax.ShapeDtypeStruct((8, samples), jnp.float32),
            jax.ShapeDtypeStruct((samples + 8, width), jnp.float32),
            jax.ShapeDtypeStruct((samples, width), jnp.float32),
        ),
        in_specs=[whole(pltpu.SMEM), whole(), whole(), whole(pl.ANY)],
        out_specs=(whole(), whole(), whole(), whole()),
        scratch_shapes=[
            pltpu.VMEM((group_count, head + HOT, width), jnp.float32),
            pltpu.SemaphoreType.DMA((group_count, 2)),
        ],
        cost_estimate=cost(1e6, 1e6),
        compiler_params=pltpu.CompilerParams(vmem_limit_bytes=GRANT),
        name="load_first",
    )(stay(starts), stay(looked), stay(bottom_out), stay(table))


def linear_part(bottom_out, top_dense):
    def kernel(bottom_ref, dense_ref, linear_ref):
        linear_ref[...] = jnp.dot(bottom_ref[...], dense_ref[...], preferred_element_type=jnp.float32)

    return pl.pallas_call(
        kernel,
        out_shape=jax.ShapeDtypeStruct((bottom_out.shape[0], top_dense.shape[1]), jnp.float32),
        in_specs=[whole()] * 2,
        out_specs=whole(),
        cost_estimate=cost(3e7, 1e6),
        compiler_params=pltpu.CompilerParams(vmem_limit_bytes=GRANT),
        name="linear_part",
    )(bottom_out, top_dense)


def hot_terms(hot_own, hot_other):
    block_rows, width = hot_own.shape

    def kernel(own_ref, other_ref, terms_ref):
        for side, ref in enumerate((own_ref, other_ref)):
            high, low = two_terms(ref[...])
            chosen = pl.ds(side * block_rows, block_rows)
            terms_ref[chosen, pl.ds(0, width)] = high
            terms_ref[chosen, pl.ds(width, width)] = low

    return pl.pallas_call(
        kernel,
        out_shape=jax.ShapeDtypeStruct((2 * block_rows, 2 * width), jnp.bfloat16),
        in_specs=[whole()] * 2,
        out_specs=whole(),
        cost_estimate=cost(1e6, 1e6),
        compiler_params=pltpu.CompilerParams(vmem_limit_bytes=GRANT),
        name="hot_terms",
    )(hot_own, hot_other)


def pool_rows(places, terms, bag):
    block_rows = terms.shape[0] // 2
    width = terms.shape[1] // 2
    samples = places.shape[1]

    def kernel(places_ref, terms_ref, part_ref):
        shard_pos = lax.axis_index("shard")
        columns = jnp.concatenate(
            [places_ref[pl.ds(0, 8), :], jnp.zeros((samples - 8, samples), jnp.float32)], axis=0
        ).T
        spread = [
            jnp.broadcast_to(columns[:, slot : slot + 1], (samples, block_rows)) for slot in range(bag)
        ]
        both = []
        for side in range(2):
            first = jnp.bitwise_xor(shard_pos, side) * block_rows
            rows = lax.broadcasted_iota(jnp.int32, (samples, block_rows), 1) + first
            rows = rows.astype(jnp.float32)
            times = jnp.where(spread[0] == rows, 1.0, 0.0)
            for column in spread[1:]:
                times = jnp.where(column == rows, times + 1.0, times)
            both.append(times.astype(jnp.bfloat16))
        total = jnp.dot(
            jnp.concatenate(both, axis=1), terms_ref[...], preferred_element_type=jnp.float32
        )
        part_ref[...] = total[:, :width] + total[:, width:]

    return pl.pallas_call(
        kernel,
        out_shape=jax.ShapeDtypeStruct((samples, width), jnp.float32),
        in_specs=[whole()] * 2,
        out_specs=whole(),
        cost_estimate=cost(5e7, 1e6),
        compiler_params=pltpu.CompilerParams(vmem_limit_bytes=GRANT),
        name="pool_rows",
    )(places, terms)


def head_terms(pooled, bottom_ref, linear_ref, pairs_ref, cot_ref):
    dots = jnp.sum(bottom_ref[...].astype(jnp.float32) * pooled, axis=1, keepdims=True)
    preact = linear_ref[...] + dots * pairs_ref[...]
    sig = 1.0 / (1.0 + jnp.exp(-preact))
    pre_grad = cot_ref[...] * sig * (1.0 + preact * (1.0 - sig))
    pair_grad = jnp.sum(pre_grad * pairs_ref[...], axis=1, keepdims=True)
    return preact, sig, pre_grad, pair_grad


def score(parts, bottom_out, linear, top_pairs, cotangent):
    samples, width = bottom_out.shape
    count = len(parts)

    def kernel(*refs):
        bottom_ref, linear_ref, pairs_ref, cot_ref, row_ref, pooled_ref = refs[count:]
        pooled = refs[0][...]
        for ref in refs[1:count]:
            pooled = pooled + ref[...]
        pooled_ref[...] = pooled
        pair_grad = head_terms(pooled, bottom_ref, linear_ref, pairs_ref, cot_ref)[3]
        down = lax.broadcasted_iota(jnp.int32, (samples, samples), 0)
        across = lax.broadcasted_iota(jnp.int32, (samples, samples), 1)
        row_ref[...] = jnp.sum(jnp.where(down == across, pair_grad, 0.0), axis=0, keepdims=True)

    return pl.pallas_call(
        kernel,
        out_shape=(
            jax.ShapeDtypeStruct((1, samples), jnp.float32),
            jax.ShapeDtypeStruct((samples, width), jnp.float32),
        ),
        in_specs=[whole()] * (count + 4),
        out_specs=(whole(), whole()),
        cost_estimate=cost(1e7, 1e6),
        compiler_params=pltpu.CompilerParams(vmem_limit_bytes=GRANT),
        name="score",
    )(*parts, bottom_out, linear, top_pairs, cotangent)


def finish_dense(pooled, bottom_out, linear, top_pairs, cotangent, top_dense, win_size):
    samples, width = bottom_out.shape
    hidden = top_dense.shape[1]

    def kernel(
        pooled_ref, bottom_ref, linear_ref, pairs_ref, cot_ref, dense_ref, act_ref, grad_ref,
        blank_ref, zeros, sem,
    ):
        zeros[...] = jnp.zeros_like(zeros)
        copy = pltpu.make_async_copy(zeros, blank_ref, sem)
        copy.start()
        pooled = pooled_ref[...]
        preact, sig, pre_grad, pair_grad = head_terms(pooled, bottom_ref, linear_ref, pairs_ref, cot_ref)
        act_ref[...] = (preact * sig).astype(jnp.bfloat16)
        grad_ref[...] = (
            lax.dot_general(
                pre_grad.astype(jnp.bfloat16),
                dense_ref[...],
                (((1,), (1,)), ((), ())),
                preferred_element_type=jnp.float32,
            )
            + pair_grad * pooled
        )
        copy.wait()

    return pl.pallas_call(
        kernel,
        out_shape=(
            jax.ShapeDtypeStruct((samples, hidden), jnp.bfloat16),
            jax.ShapeDtypeStruct((samples, width), jnp.float32),
            jax.ShapeDtypeStruct((win_size, width), jnp.float32),
        ),
        in_specs=[whole()] * 6,
        out_specs=(whole(), whole(), whole(pltpu.HBM)),
        scratch_shapes=[pltpu.VMEM((win_size, width), jnp.float32), pltpu.SemaphoreType.DMA],
        cost_estimate=cost(5e7, 1e6),
        compiler_params=pltpu.CompilerParams(vmem_limit_bytes=GRANT),
        name="finish_dense",
    )(pooled, bottom_out, linear, top_pairs, cotangent, top_dense)


def row_grads(scores, places, wides, bag, group_count, kept):
    samples = scores[0].shape[1]
    width = wides[0].shape[1]
    count = len(scores)

    def kernel(*refs):
        score_refs, place_refs, wide_refs = refs[:count], refs[count : 2 * count], refs[2 * count : -1]
        grp_pos = lax.axis_index("grp")
        shard_pos = lax.axis_index("shard")
        ids = []
        for step in range(group_count):
            holder = shard_pos if kept == (step == 0) else jnp.bitwise_xor(shard_pos, 1)
            first = (holder * group_count + jnp.bitwise_xor(grp_pos, step)) * HOT
            ids.append(lax.broadcasted_iota(jnp.int32, (HOT, samples), 0) + first)
        rows = jnp.concatenate(ids, axis=0).astype(jnp.float32)
        total = jnp.zeros((group_count * HOT, width), jnp.float32)
        for score_ref, place_ref, wide_ref in zip(score_refs, place_refs, wide_refs):
            times = jnp.zeros(rows.shape, jnp.float32)
            for slot in range(bag):
                times += jnp.where(place_ref[pl.ds(slot, 1), :] == rows, 1.0, 0.0)
            high, low = two_terms(times * score_ref[...])
            bottom = wide_ref[pl.ds(wide_ref.shape[0] - samples, samples), :].astype(jnp.bfloat16)
            total += jnp.dot(high, bottom, preferred_element_type=jnp.float32)
            total += jnp.dot(low, bottom, preferred_element_type=jnp.float32)
        refs[-1][...] = total

    return pl.pallas_call(
        kernel,
        out_shape=jax.ShapeDtypeStruct((group_count * HOT, width), jnp.float32),
        in_specs=[whole()] * (3 * count),
        out_specs=whole(),
        cost_estimate=cost(1e8, 1e6),
        compiler_params=pltpu.CompilerParams(vmem_limit_bytes=GRANT),
        name="row_grads_kept" if kept else "row_grads_given",
    )(*scores, *places, *wides)


def split_owners(kept, received, group_count):
    width = kept.shape[1]

    def kernel(kept_ref, received_ref, *out_refs):
        for step, out_ref in enumerate(out_refs):
            chosen = pl.ds(step * HOT, HOT)
            out_ref[...] = kept_ref[chosen, :] + received_ref[chosen, :]

    part = jax.ShapeDtypeStruct((HOT, width), jnp.float32)
    return pl.pallas_call(
        kernel,
        out_shape=(part,) * group_count,
        in_specs=[whole()] * 2,
        out_specs=(whole(),) * group_count,
        cost_estimate=cost(1e6, 1e6),
        compiler_params=pltpu.CompilerParams(vmem_limit_bytes=GRANT),
        name="split_owners",
    )(kept, received)


def place_rows(starts, blocks, blank):
    win_size, width = blank.shape
    count = len(blocks)
    head = min(HOT + 8, win_size)

    def kernel(starts_ref, *refs):
        block_refs = refs[:count]
        out_ref, held, sems = refs[count + 1 :]
        grp_pos = lax.axis_index("grp")
        column = lax.axis_index("shard") * count + grp_pos
        known = starts_ref[...]
        lines = lax.broadcasted_iota(jnp.int32, known.shape, 0)
        windows = lax.broadcasted_iota(jnp.int32, known.shape, 1)
        held[...] = jnp.zeros_like(held)
        firsts = [jnp.int32(0)]
        for step, ref in enumerate(block_refs):
            asked = (lines == jnp.bitwise_xor(grp_pos, step)) & (windows == column)
            start = jnp.sum(jnp.where(asked, known, 0))
            firsts.append(jnp.minimum(start // 8 * 8, win_size - head))
            held[pl.ds(start, HOT), :] += ref[...]
        held[pl.ds(0, HOT), :] += held[pl.ds(win_size, HOT), :]
        copies = []
        for place, first in enumerate(firsts):
            chosen = pl.ds(pl.multiple_of(first, 8), head)
            copy = pltpu.make_async_copy(held.at[chosen], out_ref.at[chosen], sems.at[place])
            copy.start()
            copies.append(copy)
        for copy in copies:
            copy.wait()

    return pl.pallas_call(
        kernel,
        out_shape=jax.ShapeDtypeStruct((win_size, width), jnp.float32),
        in_specs=[whole()] * (1 + count) + [whole(pltpu.HBM)],
        out_specs=whole(pltpu.HBM),
        input_output_aliases={1 + count: 0},
        scratch_shapes=[
            pltpu.VMEM((win_size + HOT, width), jnp.float32),
            pltpu.SemaphoreType.DMA((count + 1,)),
        ],
        cost_estimate=cost(1e6, 2e6),
        compiler_params=pltpu.CompilerParams(vmem_limit_bytes=GRANT),
        name="place_rows",
    )(starts, *blocks, blank)


def by_hot_rows(bottom_out, lookups, starts, tables, top_dense, top_pairs, cotangent):
    group_count = lax.axis_size("grp")
    shard_count = lax.axis_size("shard")
    bag = lookups.shape[2]
    win_size = tables.shape[1] // group_count

    def across(values, grp_step, shard_step):
        pairs = [
            (grp * shard_count + shard, (grp ^ grp_step) * shard_count + (shard ^ shard_step))
            for grp in range(group_count)
            for shard in range(shard_count)
        ]
        return lax.ppermute(values, ("grp", "shard"), pairs)

    near = 3
    steps = list(range(shard_count - 1, near, -2))
    looked = lookups[:, 0, :].T
    hot_own, places_own, near_own, wide_own = load_first(
        starts, looked, bottom_out, tables[0], group_count
    )
    hot_other = across(hot_own, 0, 1)
    places = [across(places_own, 0, step) for step in steps]
    near_back = across(near_own, 0, near)
    terms = hot_terms(hot_own, hot_other)
    linear = linear_part(bottom_out, top_dense)
    own_sums = pool_rows(places_own, terms, bag)
    parts = [own_sums]
    for step, block in zip(steps + [near], places + [near_back]):
        part = pool_rows(block, terms, bag)
        parts.append(across(part, 0, step))
    wides = [across(wide_own, 0, step) for step in steps]
    score_row, pooled = score(parts, bottom_out, linear, top_pairs, cotangent)
    scores = [score_row] + [across(score_row, 0, step) for step in steps + [near]]
    activation, bottom_grad, blank = finish_dense(
        pooled, bottom_out, linear, top_pairs, cotangent, top_dense, win_size
    )
    places = [places_own] + places + [near_back]
    wides = [near_own] + wides + [near_back]
    given = row_grads(scores, places, wides, bag, group_count, False)
    received = across(given, 0, 1)
    kept = row_grads(scores, places, wides, bag, group_count, True)
    owned = split_owners(kept, received, group_count)
    blocks = [owned[0]] + [across(owned[step], step, 1) for step in range(1, group_count)]
    table_grad = place_rows(starts, blocks, blank)
    return activation, bottom_grad, table_grad[None, None]


def is_power(number):
    return number & (number - 1) == 0


def on_device(bottom_out, lookups, starts, tables, top_dense, top_pairs, cotangent):
    group_count = lax.axis_size("grp")
    shard_count = lax.axis_size("shard")
    group_lookups = lookups.shape[0] * lookups.shape[2] * shard_count
    hot_rows = group_count * HOT * shard_count
    fits = (
        tables.shape[0] == 1
        and lookups.shape[2] <= 8
        and bottom_out.shape[0] == tables.shape[2]
        and is_power(group_count)
        and is_power(shard_count)
        and tables.shape[1] // group_count % 8 == 0
        and hot_rows <= group_lookups
        and shard_count >= 8
    )
    plan = by_hot_rows if fits else by_row_sums
    return plan(bottom_out, lookups, starts, tables, top_dense, top_pairs, cotangent)


def solution(mesh):
    in_specs = (
        P(("grp", "shard"), None),
        P(("grp", "shard"), None, None),
        P(),
        P(None, "shard", None),
        P(),
        P(),
        P(("grp", "shard"), None),
    )
    out_specs = (
        P(("grp", "shard"), None),
        P(("grp", "shard"), None),
        P(None, "shard", "grp", None),
    )
    return jax.shard_map(
        on_device, mesh=mesh, in_specs=in_specs, out_specs=out_specs, check_vma=False
    )
```

```python
import math

import jax
import jax.numpy as jnp
from jax import lax
from jax.experimental import pallas as pl
from jax.experimental.pallas import tpu as pltpu
from jax.sharding import PartitionSpec as P


HOT = 64
GRANT = 8 * 1024 * 1024


def pair_list(number):
    return [(former, latter) for former in range(number) for latter in range(former + 1, number)]


def pool_lookups(tables, picked, offset):
    rows_count = picked.shape[0]
    table_count = picked.shape[1]
    bag_count = picked.shape[2]
    rows_block = math.gcd(rows_count, 512)
    bag_block = math.gcd(bag_count, 8)
    bag_turns = bag_count // bag_block
    span_rows = tables.shape[1]
    table_ids = jnp.arange(table_count, dtype=jnp.int32)[None, :, None]

    def pool_step(turn, running):
        row_turn = turn // bag_turns
        bag_turn = turn % bag_turns
        chosen = lax.dynamic_slice(
            picked,
            (row_turn * rows_block, 0, bag_turn * bag_block),
            (rows_block, table_count, bag_block),
        )
        local = chosen - offset
        inside = (local >= 0) & (local < span_rows)
        fetched = tables[table_ids, jnp.clip(local, 0, span_rows - 1)]
        summed = jnp.sum(jnp.where(inside[..., None], fetched, 0.0), axis=2)
        current = lax.dynamic_slice_in_dim(running, row_turn * rows_block, rows_block, 0)
        return lax.dynamic_update_slice_in_dim(running, current + summed, row_turn * rows_block, 0)

    start_value = jnp.zeros((rows_count, table_count, tables.shape[2]), jnp.float32)
    return lax.fori_loop(0, rows_count // rows_block * bag_turns, pool_step, start_value)


def add_lookups(running_grad, grads, picked, offset, span_rows):
    rows_count = picked.shape[0]
    table_count = picked.shape[1]
    bag_count = picked.shape[2]
    rows_block = math.gcd(rows_count, 512)
    bag_block = math.gcd(bag_count, 8)
    bag_turns = bag_count // bag_block
    table_ids = jnp.arange(table_count, dtype=jnp.int32)[None, :, None]

    def add_step(turn, running):
        row_turn = turn // bag_turns
        bag_turn = turn % bag_turns
        chosen = lax.dynamic_slice(
            picked,
            (row_turn * rows_block, 0, bag_turn * bag_block),
            (rows_block, table_count, bag_block),
        )
        grads_block = lax.dynamic_slice_in_dim(grads, row_turn * rows_block, rows_block, 0)
        local = chosen - offset
        inside = (local >= 0) & (local < span_rows)
        updates = jnp.where(inside[..., None], grads_block[:, :, None, :], 0.0)
        return running.at[table_ids, jnp.clip(local, 0, span_rows - 1)].add(updates)

    return lax.fori_loop(0, rows_count // rows_block * bag_turns, add_step, running_grad)


def by_row_sums(bottom_out, lookups, starts, tables, top_dense, top_pairs, cotangent):
    shard_pos = lax.axis_index("shard")
    grp_pos = lax.axis_index("grp")
    group_count = lax.axis_size("grp")
    span_rows = tables.shape[1]
    table_count = tables.shape[0]
    width = tables.shape[2]
    win_size = span_rows // group_count
    offset = shard_pos * span_rows
    my_starts = lax.dynamic_index_in_dim(starts, grp_pos, 0, keepdims=False)
    window = lookups // win_size
    inner = lookups % win_size
    own_rows = window * win_size + (inner + my_starts[window]) % win_size
    group_idx = lax.all_gather(own_rows, "shard", axis=0, tiled=True)
    picked = group_idx
    pooled = lax.psum_scatter(
        pool_lookups(tables, picked, offset), "shard", scatter_dimension=0, tiled=True
    )
    vectors = [bottom_out.astype(jnp.float32)] + [pooled[:, 0]]
    couples = pair_list(table_count + 1)
    pair_dots = jnp.stack(
        [jnp.sum(vectors[former] * vectors[latter], axis=-1) for former, latter in couples], axis=1
    )
    preact = jnp.dot(bottom_out, top_dense, preferred_element_type=jnp.float32)
    preact = preact + jnp.dot(pair_dots, top_pairs, precision=lax.Precision.HIGHEST)
    sigmoid_pre = jax.nn.sigmoid(preact)
    activation = (preact * sigmoid_pre).astype(jnp.bfloat16)
    pre_grad = cotangent * sigmoid_pre * (1.0 + preact * (1.0 - sigmoid_pre))
    pair_grad = jnp.dot(pre_grad, top_pairs.T, precision=lax.Precision.HIGHEST)
    vec_grads = [jnp.zeros_like(vector) for vector in vectors]
    for former, latter in couples:
        vec_grads[former] = pair_grad * vectors[latter]
        vec_grads[latter] = pair_grad * vectors[former]
    pre_half = pre_grad.astype(jnp.bfloat16)
    bottom_grad = (
        lax.dot_general(
            pre_half, top_dense, (((1,), (1,)), ((), ())), preferred_element_type=jnp.float32
        )
        + vec_grads[0]
    )
    pooled_grad = jnp.stack(vec_grads[1:], axis=1)
    start_grad = jnp.zeros((table_count, span_rows, width), jnp.float32)
    picked = group_idx
    local_grad = add_lookups(
        start_grad,
        lax.all_gather(pooled_grad, "shard", axis=0, tiled=True),
        picked,
        offset,
        span_rows,
    )
    hot_range = jnp.arange(HOT, dtype=jnp.int32)
    owner_range = jnp.arange(group_count, dtype=jnp.int32)
    send_starts = lax.dynamic_slice_in_dim(my_starts, shard_pos * group_count, group_count, 0)
    send_index = (
        owner_range[:, None] * win_size + (send_starts[:, None] + hot_range[None, :]) % win_size
    )
    packed = local_grad[:, send_index]
    received = lax.all_to_all(packed, "grp", split_axis=1, concat_axis=1, tiled=True)
    recv_starts = lax.dynamic_slice_in_dim(starts, shard_pos * group_count + grp_pos, 1, 1)[:, 0]
    places = ((recv_starts[:, None] + hot_range[None, :]) % win_size).reshape(-1)
    flat_rows = received.reshape(table_count, group_count * HOT, width)
    table_grad = jnp.zeros((table_count, win_size, width), jnp.float32).at[:, places].add(flat_rows)
    return (activation, bottom_grad, table_grad[:, None])


def whole(memory=pltpu.VMEM):
    return pl.BlockSpec(memory_space=memory)


def cost(flops, moved):
    return pl.CostEstimate(flops=int(flops), bytes_accessed=int(moved), transcendentals=0)


def two_terms(values):
    high = values.astype(jnp.bfloat16)
    low = (values - high.astype(jnp.float32)).astype(jnp.bfloat16)
    return high, low


def stay(values):
    return pltpu.with_memory_space_constraint(values, pltpu.HBM)


def load_first(starts, looked, bottom_out, table, group_count):
    span_rows, width = table.shape
    win_size = span_rows // group_count
    samples = bottom_out.shape[0]
    bag = looked.shape[0]
    head = min(HOT + 8, win_size)

    def kernel(starts_ref, looked_ref, bottom_ref, table_ref, hot_ref, places_ref, near_ref, wide_ref, held, sems):
        grp_pos = lax.axis_index("grp")
        shard_pos = lax.axis_index("shard")
        shifts = []
        copies = []
        for window in range(group_count):
            start = starts_ref[grp_pos, shard_pos * group_count + window]
            aligned = jnp.minimum(start // 8 * 8, win_size - head)
            shifts.append(start - aligned)
            base = window * win_size
            first = pltpu.make_async_copy(
                table_ref.at[pl.ds(pl.multiple_of(base + aligned, 8), head)],
                held.at[window, pl.ds(0, head)],
                sems.at[window, 0],
            )
            second = pltpu.make_async_copy(
                table_ref.at[pl.ds(base, HOT)], held.at[window, pl.ds(head, HOT)], sems.at[window, 1]
            )
            first.start()
            second.start()
            copies += [first, second]
        found = looked_ref[...]
        window_of = jnp.floor((found.astype(jnp.float32) + 0.5) * (1.0 / win_size)).astype(jnp.int32)
        places = (found - window_of * (win_size - HOT)).astype(jnp.float32)
        places = jnp.concatenate([places, jnp.zeros((8 - bag, samples), jnp.float32)], axis=0)
        places_ref[...] = places
        near_ref[pl.ds(0, 8), :] = places
        wide = bottom_ref[...].astype(jnp.float32)
        near_ref[pl.ds(8, samples), :] = wide
        wide_ref[...] = wide
        for copy in copies:
            copy.wait()
        for window in range(group_count):
            hot_ref[pl.ds(window * HOT, HOT), :] = held[window, pl.ds(shifts[window], HOT), :]

    return pl.pallas_call(
        kernel,
        out_shape=(
            jax.ShapeDtypeStruct((group_count * HOT, width), jnp.float32),
            jax.ShapeDtypeStruct((8, samples), jnp.float32),
            jax.ShapeDtypeStruct((samples + 8, width), jnp.float32),
            jax.ShapeDtypeStruct((samples, width), jnp.float32),
        ),
        in_specs=[whole(pltpu.SMEM), whole(), whole(), whole(pl.ANY)],
        out_specs=(whole(), whole(), whole(), whole()),
        scratch_shapes=[
            pltpu.VMEM((group_count, head + HOT, width), jnp.float32),
            pltpu.SemaphoreType.DMA((group_count, 2)),
        ],
        cost_estimate=cost(1e6, 1e6),
        compiler_params=pltpu.CompilerParams(vmem_limit_bytes=GRANT),
        name="load_first",
    )(stay(starts), stay(looked), stay(bottom_out), stay(table))


def linear_part(bottom_out, top_dense):
    def kernel(bottom_ref, dense_ref, linear_ref):
        linear_ref[...] = jnp.dot(bottom_ref[...], dense_ref[...], preferred_element_type=jnp.float32)

    return pl.pallas_call(
        kernel,
        out_shape=jax.ShapeDtypeStruct((bottom_out.shape[0], top_dense.shape[1]), jnp.float32),
        in_specs=[whole()] * 2,
        out_specs=whole(),
        cost_estimate=cost(3e7, 1e6),
        compiler_params=pltpu.CompilerParams(vmem_limit_bytes=GRANT),
        name="linear_part",
    )(bottom_out, top_dense)


def hot_terms(hot_own, hot_other):
    block_rows, width = hot_own.shape

    def kernel(own_ref, other_ref, terms_ref):
        for side, ref in enumerate((own_ref, other_ref)):
            high, low = two_terms(ref[...])
            chosen = pl.ds(side * block_rows, block_rows)
            terms_ref[chosen, pl.ds(0, width)] = high
            terms_ref[chosen, pl.ds(width, width)] = low

    return pl.pallas_call(
        kernel,
        out_shape=jax.ShapeDtypeStruct((2 * block_rows, 2 * width), jnp.bfloat16),
        in_specs=[whole()] * 2,
        out_specs=whole(),
        cost_estimate=cost(1e6, 1e6),
        compiler_params=pltpu.CompilerParams(vmem_limit_bytes=GRANT),
        name="hot_terms",
    )(hot_own, hot_other)


def pool_rows(places, terms, bag):
    block_rows = terms.shape[0] // 2
    width = terms.shape[1] // 2
    samples = places.shape[1]

    def kernel(places_ref, terms_ref, part_ref):
        shard_pos = lax.axis_index("shard")
        columns = jnp.concatenate(
            [places_ref[pl.ds(0, 8), :], jnp.zeros((samples - 8, samples), jnp.float32)], axis=0
        ).T
        spread = [
            jnp.broadcast_to(columns[:, slot : slot + 1], (samples, block_rows)) for slot in range(bag)
        ]
        both = []
        for side in range(2):
            first = jnp.bitwise_xor(shard_pos, side) * block_rows
            rows = lax.broadcasted_iota(jnp.int32, (samples, block_rows), 1) + first
            rows = rows.astype(jnp.float32)
            times = jnp.where(spread[0] == rows, 1.0, 0.0)
            for column in spread[1:]:
                times = jnp.where(column == rows, times + 1.0, times)
            both.append(times.astype(jnp.bfloat16))
        total = jnp.dot(
            jnp.concatenate(both, axis=1), terms_ref[...], preferred_element_type=jnp.float32
        )
        part_ref[...] = total[:, :width] + total[:, width:]

    return pl.pallas_call(
        kernel,
        out_shape=jax.ShapeDtypeStruct((samples, width), jnp.float32),
        in_specs=[whole()] * 2,
        out_specs=whole(),
        cost_estimate=cost(5e7, 1e6),
        compiler_params=pltpu.CompilerParams(vmem_limit_bytes=GRANT),
        name="pool_rows",
    )(places, terms)


def head_terms(pooled, bottom_ref, linear_ref, pairs_ref, cot_ref):
    dots = jnp.sum(bottom_ref[...].astype(jnp.float32) * pooled, axis=1, keepdims=True)
    preact = linear_ref[...] + dots * pairs_ref[...]
    sig = 1.0 / (1.0 + jnp.exp(-preact))
    pre_grad = cot_ref[...] * sig * (1.0 + preact * (1.0 - sig))
    pair_grad = jnp.sum(pre_grad * pairs_ref[...], axis=1, keepdims=True)
    return preact, sig, pre_grad, pair_grad


def score(parts, bottom_out, linear, top_pairs, cotangent):
    samples, width = bottom_out.shape
    count = len(parts)

    def kernel(*refs):
        bottom_ref, linear_ref, pairs_ref, cot_ref, row_ref, pooled_ref = refs[count:]
        pooled = refs[0][...]
        for ref in refs[1:count]:
            pooled = pooled + ref[...]
        pooled_ref[...] = pooled
        pair_grad = head_terms(pooled, bottom_ref, linear_ref, pairs_ref, cot_ref)[3]
        down = lax.broadcasted_iota(jnp.int32, (samples, samples), 0)
        across = lax.broadcasted_iota(jnp.int32, (samples, samples), 1)
        row_ref[...] = jnp.sum(jnp.where(down == across, pair_grad, 0.0), axis=0, keepdims=True)

    return pl.pallas_call(
        kernel,
        out_shape=(
            jax.ShapeDtypeStruct((1, samples), jnp.float32),
            jax.ShapeDtypeStruct((samples, width), jnp.float32),
        ),
        in_specs=[whole()] * (count + 4),
        out_specs=(whole(), whole()),
        cost_estimate=cost(1e7, 1e6),
        compiler_params=pltpu.CompilerParams(vmem_limit_bytes=GRANT),
        name="score",
    )(*parts, bottom_out, linear, top_pairs, cotangent)


def finish_dense(pooled, bottom_out, linear, top_pairs, cotangent, top_dense, win_size):
    samples, width = bottom_out.shape
    hidden = top_dense.shape[1]

    def kernel(
        pooled_ref, bottom_ref, linear_ref, pairs_ref, cot_ref, dense_ref, act_ref, grad_ref,
        blank_ref, zeros, sem,
    ):
        zeros[...] = jnp.zeros_like(zeros)
        copy = pltpu.make_async_copy(zeros, blank_ref, sem)
        copy.start()
        pooled = pooled_ref[...]
        preact, sig, pre_grad, pair_grad = head_terms(pooled, bottom_ref, linear_ref, pairs_ref, cot_ref)
        act_ref[...] = (preact * sig).astype(jnp.bfloat16)
        grad_ref[...] = (
            lax.dot_general(
                pre_grad.astype(jnp.bfloat16),
                dense_ref[...],
                (((1,), (1,)), ((), ())),
                preferred_element_type=jnp.float32,
            )
            + pair_grad * pooled
        )
        copy.wait()

    return pl.pallas_call(
        kernel,
        out_shape=(
            jax.ShapeDtypeStruct((samples, hidden), jnp.bfloat16),
            jax.ShapeDtypeStruct((samples, width), jnp.float32),
            jax.ShapeDtypeStruct((win_size, width), jnp.float32),
        ),
        in_specs=[whole()] * 6,
        out_specs=(whole(), whole(), whole(pltpu.HBM)),
        scratch_shapes=[pltpu.VMEM((win_size, width), jnp.float32), pltpu.SemaphoreType.DMA],
        cost_estimate=cost(5e7, 1e6),
        compiler_params=pltpu.CompilerParams(vmem_limit_bytes=GRANT),
        name="finish_dense",
    )(pooled, bottom_out, linear, top_pairs, cotangent, top_dense)


def count_grads(places, bag, group_count):
    samples = places[0].shape[1]
    count = len(places)
    held_rows = group_count * HOT

    def kernel(*refs):
        place_refs, out_refs = refs[:count], refs[count:]
        grp_pos = lax.axis_index("grp")
        shard_pos = lax.axis_index("shard")
        for kept, out_ref in enumerate(out_refs):
            ids = []
            for step in range(group_count):
                holder = shard_pos if (kept == 1) == (step == 0) else jnp.bitwise_xor(shard_pos, 1)
                first = (holder * group_count + jnp.bitwise_xor(grp_pos, step)) * HOT
                ids.append(lax.broadcasted_iota(jnp.int32, (HOT, samples), 0) + first)
            rows = jnp.concatenate(ids, axis=0).astype(jnp.float32)
            for place, ref in enumerate(place_refs):
                times = jnp.zeros(rows.shape, jnp.float32)
                for slot in range(bag):
                    times += jnp.where(ref[pl.ds(slot, 1), :] == rows, 1.0, 0.0)
                out_ref[:, pl.ds(place * samples, samples)] = times

    part = jax.ShapeDtypeStruct((held_rows, count * samples), jnp.float32)
    return pl.pallas_call(
        kernel,
        out_shape=(part, part),
        in_specs=[whole()] * count,
        out_specs=(whole(),) * 2,
        cost_estimate=cost(1e7, 1e6),
        compiler_params=pltpu.CompilerParams(vmem_limit_bytes=GRANT),
        name="count_grads",
    )(*places)


def row_grads(times, scores, wides):
    samples = scores[0].shape[1]
    width = wides[0].shape[1]
    count = len(scores)

    def kernel(times_ref, *refs):
        score_refs, wide_refs = refs[:count], refs[count:-1]
        total = jnp.zeros((times_ref.shape[0], width), jnp.float32)
        for place, (score_ref, wide_ref) in enumerate(zip(score_refs, wide_refs)):
            weights = times_ref[:, pl.ds(place * samples, samples)] * score_ref[...]
            high, low = two_terms(weights)
            bottom = wide_ref[pl.ds(wide_ref.shape[0] - samples, samples), :].astype(jnp.bfloat16)
            total += jnp.dot(high, bottom, preferred_element_type=jnp.float32)
            total += jnp.dot(low, bottom, preferred_element_type=jnp.float32)
        refs[-1][...] = total

    return pl.pallas_call(
        kernel,
        out_shape=jax.ShapeDtypeStruct((times.shape[0], width), jnp.float32),
        in_specs=[whole()] * (1 + 2 * count),
        out_specs=whole(),
        cost_estimate=cost(1e8, 1e6),
        compiler_params=pltpu.CompilerParams(vmem_limit_bytes=GRANT),
        name="row_grads",
    )(times, *scores, *wides)


def split_owners(kept, received, group_count):
    width = kept.shape[1]

    def kernel(kept_ref, received_ref, *out_refs):
        for step, out_ref in enumerate(out_refs):
            chosen = pl.ds(step * HOT, HOT)
            out_ref[...] = kept_ref[chosen, :] + received_ref[chosen, :]

    part = jax.ShapeDtypeStruct((HOT, width), jnp.float32)
    return pl.pallas_call(
        kernel,
        out_shape=(part,) * group_count,
        in_specs=[whole()] * 2,
        out_specs=(whole(),) * group_count,
        cost_estimate=cost(1e6, 1e6),
        compiler_params=pltpu.CompilerParams(vmem_limit_bytes=GRANT),
        name="split_owners",
    )(kept, received)


def place_rows(starts, blocks, blank):
    win_size, width = blank.shape
    count = len(blocks)
    head = min(HOT + 8, win_size)

    def kernel(starts_ref, *refs):
        block_refs = refs[:count]
        out_ref, held, sems = refs[count + 1 :]
        grp_pos = lax.axis_index("grp")
        column = lax.axis_index("shard") * count + grp_pos
        known = starts_ref[...]
        lines = lax.broadcasted_iota(jnp.int32, known.shape, 0)
        windows = lax.broadcasted_iota(jnp.int32, known.shape, 1)
        held[...] = jnp.zeros_like(held)
        firsts = [jnp.int32(0)]
        for step, ref in enumerate(block_refs):
            asked = (lines == jnp.bitwise_xor(grp_pos, step)) & (windows == column)
            start = jnp.sum(jnp.where(asked, known, 0))
            firsts.append(jnp.minimum(start // 8 * 8, win_size - head))
            held[pl.ds(start, HOT), :] += ref[...]
        held[pl.ds(0, HOT), :] += held[pl.ds(win_size, HOT), :]
        copies = []
        for place, first in enumerate(firsts):
            chosen = pl.ds(pl.multiple_of(first, 8), head)
            copy = pltpu.make_async_copy(held.at[chosen], out_ref.at[chosen], sems.at[place])
            copy.start()
            copies.append(copy)
        for copy in copies:
            copy.wait()

    return pl.pallas_call(
        kernel,
        out_shape=jax.ShapeDtypeStruct((win_size, width), jnp.float32),
        in_specs=[whole()] * (1 + count) + [whole(pltpu.HBM)],
        out_specs=whole(pltpu.HBM),
        input_output_aliases={1 + count: 0},
        scratch_shapes=[
            pltpu.VMEM((win_size + HOT, width), jnp.float32),
            pltpu.SemaphoreType.DMA((count + 1,)),
        ],
        cost_estimate=cost(1e6, 2e6),
        compiler_params=pltpu.CompilerParams(vmem_limit_bytes=GRANT),
        name="place_rows",
    )(starts, *blocks, blank)


def far_steps(shard_count):
    return [2 * chips + chips % 2 for chips in range(shard_count // 2 - 1, 1, -1)]


def by_hot_rows(bottom_out, lookups, starts, tables, top_dense, top_pairs, cotangent):
    group_count = lax.axis_size("grp")
    shard_count = lax.axis_size("shard")
    bag = lookups.shape[2]
    win_size = tables.shape[1] // group_count

    def across(values, grp_step, shard_step):
        pairs = [
            (grp * shard_count + shard, (grp ^ grp_step) * shard_count + (shard ^ shard_step))
            for grp in range(group_count)
            for shard in range(shard_count)
        ]
        return lax.ppermute(values, ("grp", "shard"), pairs)

    near, steps = 3, far_steps(shard_count)
    looked = lookups[:, 0, :].T
    hot_own, places_own, near_own, wide_own = load_first(
        starts, looked, bottom_out, tables[0], group_count
    )
    hot_other = across(hot_own, 0, 1)
    places = [across(places_own, 0, step) for step in steps]
    near_back = across(near_own, 0, near)
    terms = hot_terms(hot_own, hot_other)
    linear = linear_part(bottom_out, top_dense)
    own_sums = pool_rows(places_own, terms, bag)
    parts = [own_sums]
    for step, block in zip(steps + [near], places + [near_back]):
        part = pool_rows(block, terms, bag)
        parts.append(across(part, 0, step))
    wides = [across(wide_own, 0, step) for step in steps]
    score_row, pooled = score(parts, bottom_out, linear, top_pairs, cotangent)
    scores = [score_row] + [across(score_row, 0, step) for step in steps + [near]]
    activation, bottom_grad, blank = finish_dense(
        pooled, bottom_out, linear, top_pairs, cotangent, top_dense, win_size
    )
    places = [places_own] + places + [near_back]
    wides = [near_own] + wides + [near_back]
    times_given, times_kept = count_grads(places, bag, group_count)
    given = row_grads(times_given, scores, wides)
    received = across(given, 0, 1)
    kept = row_grads(times_kept, scores, wides)
    owned = split_owners(kept, received, group_count)
    blocks = [owned[0]] + [across(owned[step], step, 1) for step in range(1, group_count)]
    table_grad = place_rows(starts, blocks, blank)
    return activation, bottom_grad, table_grad[None, None]


def is_power(number):
    return number & (number - 1) == 0


def on_device(bottom_out, lookups, starts, tables, top_dense, top_pairs, cotangent):
    group_count = lax.axis_size("grp")
    shard_count = lax.axis_size("shard")
    group_lookups = lookups.shape[0] * lookups.shape[2] * shard_count
    hot_rows = group_count * HOT * shard_count
    fits = (
        tables.shape[0] == 1
        and lookups.shape[2] <= 8
        and bottom_out.shape[0] == tables.shape[2]
        and is_power(group_count)
        and is_power(shard_count)
        and tables.shape[1] // group_count % 8 == 0
        and hot_rows <= group_lookups
        and shard_count >= 8
    )
    plan = by_hot_rows if fits else by_row_sums
    return plan(bottom_out, lookups, starts, tables, top_dense, top_pairs, cotangent)


def solution(mesh):
    in_specs = (
        P(("grp", "shard"), None),
        P(("grp", "shard"), None, None),
        P(),
        P(None, "shard", None),
        P(),
        P(),
        P(("grp", "shard"), None),
    )
    out_specs = (
        P(("grp", "shard"), None),
        P(("grp", "shard"), None),
        P(None, "shard", "grp", None),
    )
    return jax.shard_map(
        on_device, mesh=mesh, in_specs=in_specs, out_specs=out_specs, check_vma=False
    )
```

```python
import math

import jax
import jax.numpy as jnp
from jax import lax
from jax.experimental import pallas as pl
from jax.experimental.pallas import tpu as pltpu
from jax.sharding import PartitionSpec as P


HOT = 64
GRANT = 8 * 1024 * 1024


def pair_list(number):
    return [(former, latter) for former in range(number) for latter in range(former + 1, number)]


def pool_lookups(tables, picked, offset):
    rows_count = picked.shape[0]
    table_count = picked.shape[1]
    bag_count = picked.shape[2]
    rows_block = math.gcd(rows_count, 512)
    bag_block = math.gcd(bag_count, 8)
    bag_turns = bag_count // bag_block
    span_rows = tables.shape[1]
    table_ids = jnp.arange(table_count, dtype=jnp.int32)[None, :, None]

    def pool_step(turn, running):
        row_turn = turn // bag_turns
        bag_turn = turn % bag_turns
        chosen = lax.dynamic_slice(
            picked,
            (row_turn * rows_block, 0, bag_turn * bag_block),
            (rows_block, table_count, bag_block),
        )
        local = chosen - offset
        inside = (local >= 0) & (local < span_rows)
        fetched = tables[table_ids, jnp.clip(local, 0, span_rows - 1)]
        summed = jnp.sum(jnp.where(inside[..., None], fetched, 0.0), axis=2)
        current = lax.dynamic_slice_in_dim(running, row_turn * rows_block, rows_block, 0)
        return lax.dynamic_update_slice_in_dim(running, current + summed, row_turn * rows_block, 0)

    start_value = jnp.zeros((rows_count, table_count, tables.shape[2]), jnp.float32)
    return lax.fori_loop(0, rows_count // rows_block * bag_turns, pool_step, start_value)


def add_lookups(running_grad, grads, picked, offset, span_rows):
    rows_count = picked.shape[0]
    table_count = picked.shape[1]
    bag_count = picked.shape[2]
    rows_block = math.gcd(rows_count, 512)
    bag_block = math.gcd(bag_count, 8)
    bag_turns = bag_count // bag_block
    table_ids = jnp.arange(table_count, dtype=jnp.int32)[None, :, None]

    def add_step(turn, running):
        row_turn = turn // bag_turns
        bag_turn = turn % bag_turns
        chosen = lax.dynamic_slice(
            picked,
            (row_turn * rows_block, 0, bag_turn * bag_block),
            (rows_block, table_count, bag_block),
        )
        grads_block = lax.dynamic_slice_in_dim(grads, row_turn * rows_block, rows_block, 0)
        local = chosen - offset
        inside = (local >= 0) & (local < span_rows)
        updates = jnp.where(inside[..., None], grads_block[:, :, None, :], 0.0)
        return running.at[table_ids, jnp.clip(local, 0, span_rows - 1)].add(updates)

    return lax.fori_loop(0, rows_count // rows_block * bag_turns, add_step, running_grad)


def by_row_sums(bottom_out, lookups, starts, tables, top_dense, top_pairs, cotangent):
    shard_pos = lax.axis_index("shard")
    grp_pos = lax.axis_index("grp")
    group_count = lax.axis_size("grp")
    span_rows = tables.shape[1]
    table_count = tables.shape[0]
    width = tables.shape[2]
    win_size = span_rows // group_count
    offset = shard_pos * span_rows
    my_starts = lax.dynamic_index_in_dim(starts, grp_pos, 0, keepdims=False)
    window = lookups // win_size
    inner = lookups % win_size
    own_rows = window * win_size + (inner + my_starts[window]) % win_size
    group_idx = lax.all_gather(own_rows, "shard", axis=0, tiled=True)
    picked = group_idx
    pooled = lax.psum_scatter(
        pool_lookups(tables, picked, offset), "shard", scatter_dimension=0, tiled=True
    )
    vectors = [bottom_out.astype(jnp.float32)] + [pooled[:, 0]]
    couples = pair_list(table_count + 1)
    pair_dots = jnp.stack(
        [jnp.sum(vectors[former] * vectors[latter], axis=-1) for former, latter in couples], axis=1
    )
    preact = jnp.dot(bottom_out, top_dense, preferred_element_type=jnp.float32)
    preact = preact + jnp.dot(pair_dots, top_pairs, precision=lax.Precision.HIGHEST)
    sigmoid_pre = jax.nn.sigmoid(preact)
    activation = (preact * sigmoid_pre).astype(jnp.bfloat16)
    pre_grad = cotangent * sigmoid_pre * (1.0 + preact * (1.0 - sigmoid_pre))
    pair_grad = jnp.dot(pre_grad, top_pairs.T, precision=lax.Precision.HIGHEST)
    vec_grads = [jnp.zeros_like(vector) for vector in vectors]
    for former, latter in couples:
        vec_grads[former] = pair_grad * vectors[latter]
        vec_grads[latter] = pair_grad * vectors[former]
    pre_half = pre_grad.astype(jnp.bfloat16)
    bottom_grad = (
        lax.dot_general(
            pre_half, top_dense, (((1,), (1,)), ((), ())), preferred_element_type=jnp.float32
        )
        + vec_grads[0]
    )
    pooled_grad = jnp.stack(vec_grads[1:], axis=1)
    start_grad = jnp.zeros((table_count, span_rows, width), jnp.float32)
    picked = group_idx
    local_grad = add_lookups(
        start_grad,
        lax.all_gather(pooled_grad, "shard", axis=0, tiled=True),
        picked,
        offset,
        span_rows,
    )
    hot_range = jnp.arange(HOT, dtype=jnp.int32)
    owner_range = jnp.arange(group_count, dtype=jnp.int32)
    send_starts = lax.dynamic_slice_in_dim(my_starts, shard_pos * group_count, group_count, 0)
    send_index = (
        owner_range[:, None] * win_size + (send_starts[:, None] + hot_range[None, :]) % win_size
    )
    packed = local_grad[:, send_index]
    received = lax.all_to_all(packed, "grp", split_axis=1, concat_axis=1, tiled=True)
    recv_starts = lax.dynamic_slice_in_dim(starts, shard_pos * group_count + grp_pos, 1, 1)[:, 0]
    places = ((recv_starts[:, None] + hot_range[None, :]) % win_size).reshape(-1)
    flat_rows = received.reshape(table_count, group_count * HOT, width)
    table_grad = jnp.zeros((table_count, win_size, width), jnp.float32).at[:, places].add(flat_rows)
    return (activation, bottom_grad, table_grad[:, None])


def whole(memory=pltpu.VMEM):
    return pl.BlockSpec(memory_space=memory)


def cost(flops, moved):
    return pl.CostEstimate(flops=int(flops), bytes_accessed=int(moved), transcendentals=0)


def two_terms(values):
    high = values.astype(jnp.bfloat16)
    low = (values - high.astype(jnp.float32)).astype(jnp.bfloat16)
    return high, low


def stay(values):
    return pltpu.with_memory_space_constraint(values, pltpu.HBM)


def load_first(starts, looked, bottom_out, table, group_count):
    span_rows, width = table.shape
    win_size = span_rows // group_count
    samples = bottom_out.shape[0]
    bag = looked.shape[0]
    head = min(HOT + 8, win_size)

    def kernel(
        starts_hbm, looked_hbm, bottom_hbm, table_ref, hot_ref, places_ref, near_ref, wide_ref,
        starts_ref, looked_ref, bottom_ref, held, sems, small,
    ):
        grp_pos = lax.axis_index("grp")
        shard_pos = lax.axis_index("shard")
        from_starts = pltpu.make_async_copy(starts_hbm, starts_ref, small.at[0])
        from_starts.start()
        from_looked = pltpu.make_async_copy(looked_hbm, looked_ref, small.at[1])
        from_looked.start()
        from_bottom = pltpu.make_async_copy(bottom_hbm, bottom_ref, small.at[2])
        from_bottom.start()
        tails = []
        for window in range(group_count):
            tail = pltpu.make_async_copy(
                table_ref.at[pl.ds(window * win_size, HOT)],
                held.at[window, pl.ds(head, HOT)],
                sems.at[window, 1],
            )
            tail.start()
            tails.append(tail)
        from_starts.wait()
        shifts = []
        copies = []
        for window in range(group_count):
            start = starts_ref[grp_pos, shard_pos * group_count + window]
            aligned = jnp.minimum(start // 8 * 8, win_size - head)
            shifts.append(start - aligned)
            base = window * win_size
            first = pltpu.make_async_copy(
                table_ref.at[pl.ds(pl.multiple_of(base + aligned, 8), head)],
                held.at[window, pl.ds(0, head)],
                sems.at[window, 0],
            )
            first.start()
            copies += [first, tails[window]]
        from_looked.wait()
        from_bottom.wait()
        found = looked_ref[...]
        window_of = jnp.floor((found.astype(jnp.float32) + 0.5) * (1.0 / win_size)).astype(jnp.int32)
        places = (found - window_of * (win_size - HOT)).astype(jnp.float32)
        places = jnp.concatenate([places, jnp.zeros((8 - bag, samples), jnp.float32)], axis=0)
        places_ref[...] = places
        near_ref[pl.ds(0, 8), :] = places
        wide = bottom_ref[...].astype(jnp.float32)
        near_ref[pl.ds(8, samples), :] = wide
        wide_ref[...] = wide
        for copy in copies:
            copy.wait()
        for window in range(group_count):
            hot_ref[pl.ds(window * HOT, HOT), :] = held[window, pl.ds(shifts[window], HOT), :]

    return pl.pallas_call(
        kernel,
        out_shape=(
            jax.ShapeDtypeStruct((group_count * HOT, width), jnp.float32),
            jax.ShapeDtypeStruct((8, samples), jnp.float32),
            jax.ShapeDtypeStruct((samples + 8, width), jnp.float32),
            jax.ShapeDtypeStruct((samples, width), jnp.float32),
        ),
        in_specs=[whole(pltpu.HBM)] * 4,
        out_specs=(whole(), whole(), whole(), whole()),
        scratch_shapes=[
            pltpu.SMEM(starts.shape, starts.dtype),
            pltpu.VMEM(looked.shape, looked.dtype),
            pltpu.VMEM(bottom_out.shape, bottom_out.dtype),
            pltpu.VMEM((group_count, head + HOT, width), jnp.float32),
            pltpu.SemaphoreType.DMA((group_count, 2)),
            pltpu.SemaphoreType.DMA((3,)),
        ],
        cost_estimate=cost(1e6, 1e6),
        compiler_params=pltpu.CompilerParams(vmem_limit_bytes=GRANT),
        name="load_first",
    )(stay(starts), stay(looked), stay(bottom_out), stay(table))


def linear_part(bottom_out, top_dense):
    def kernel(bottom_ref, dense_ref, linear_ref):
        linear_ref[...] = jnp.dot(bottom_ref[...], dense_ref[...], preferred_element_type=jnp.float32)

    return pl.pallas_call(
        kernel,
        out_shape=jax.ShapeDtypeStruct((bottom_out.shape[0], top_dense.shape[1]), jnp.float32),
        in_specs=[whole()] * 2,
        out_specs=whole(),
        cost_estimate=cost(3e7, 1e6),
        compiler_params=pltpu.CompilerParams(vmem_limit_bytes=GRANT),
        name="linear_part",
    )(bottom_out, top_dense)


def hot_terms(hot_own, hot_other):
    block_rows, width = hot_own.shape

    def kernel(own_ref, other_ref, terms_ref):
        for side, ref in enumerate((own_ref, other_ref)):
            high, low = two_terms(ref[...])
            chosen = pl.ds(side * block_rows, block_rows)
            terms_ref[chosen, pl.ds(0, width)] = high
            terms_ref[chosen, pl.ds(width, width)] = low

    return pl.pallas_call(
        kernel,
        out_shape=jax.ShapeDtypeStruct((2 * block_rows, 2 * width), jnp.bfloat16),
        in_specs=[whole()] * 2,
        out_specs=whole(),
        cost_estimate=cost(1e6, 1e6),
        compiler_params=pltpu.CompilerParams(vmem_limit_bytes=GRANT),
        name="hot_terms",
    )(hot_own, hot_other)


def pool_rows(places, terms, bag):
    block_rows = terms.shape[0] // 2
    width = terms.shape[1] // 2
    samples = places.shape[1]

    def kernel(places_ref, terms_ref, part_ref):
        shard_pos = lax.axis_index("shard")
        columns = jnp.concatenate(
            [places_ref[pl.ds(0, 8), :], jnp.zeros((samples - 8, samples), jnp.float32)], axis=0
        ).T
        spread = [
            jnp.broadcast_to(columns[:, slot : slot + 1], (samples, block_rows)) for slot in range(bag)
        ]
        both = []
        for side in range(2):
            first = jnp.bitwise_xor(shard_pos, side) * block_rows
            rows = lax.broadcasted_iota(jnp.int32, (samples, block_rows), 1) + first
            rows = rows.astype(jnp.float32)
            times = jnp.where(spread[0] == rows, 1.0, 0.0)
            for column in spread[1:]:
                times = jnp.where(column == rows, times + 1.0, times)
            both.append(times.astype(jnp.bfloat16))
        total = jnp.dot(
            jnp.concatenate(both, axis=1), terms_ref[...], preferred_element_type=jnp.float32
        )
        part_ref[...] = total[:, :width] + total[:, width:]

    return pl.pallas_call(
        kernel,
        out_shape=jax.ShapeDtypeStruct((samples, width), jnp.float32),
        in_specs=[whole()] * 2,
        out_specs=whole(),
        cost_estimate=cost(5e7, 1e6),
        compiler_params=pltpu.CompilerParams(vmem_limit_bytes=GRANT),
        name="pool_rows",
    )(places, terms)


def head_terms(pooled, bottom_ref, linear_ref, pairs_ref, cot_ref):
    dots = jnp.sum(bottom_ref[...].astype(jnp.float32) * pooled, axis=1, keepdims=True)
    preact = linear_ref[...] + dots * pairs_ref[...]
    sig = 1.0 / (1.0 + jnp.exp(-preact))
    pre_grad = cot_ref[...] * sig * (1.0 + preact * (1.0 - sig))
    pair_grad = jnp.sum(pre_grad * pairs_ref[...], axis=1, keepdims=True)
    return preact, sig, pre_grad, pair_grad


def score(parts, bottom_out, linear, top_pairs, cotangent):
    samples, width = bottom_out.shape
    count = len(parts)

    def kernel(*refs):
        bottom_ref, linear_ref, pairs_ref, cot_ref, row_ref, pooled_ref = refs[count:]
        pooled = refs[0][...]
        for ref in refs[1:count]:
            pooled = pooled + ref[...]
        pooled_ref[...] = pooled
        pair_grad = head_terms(pooled, bottom_ref, linear_ref, pairs_ref, cot_ref)[3]
        down = lax.broadcasted_iota(jnp.int32, (samples, samples), 0)
        across = lax.broadcasted_iota(jnp.int32, (samples, samples), 1)
        row_ref[...] = jnp.sum(jnp.where(down == across, pair_grad, 0.0), axis=0, keepdims=True)

    return pl.pallas_call(
        kernel,
        out_shape=(
            jax.ShapeDtypeStruct((1, samples), jnp.float32),
            jax.ShapeDtypeStruct((samples, width), jnp.float32),
        ),
        in_specs=[whole()] * (count + 4),
        out_specs=(whole(), whole()),
        cost_estimate=cost(1e7, 1e6),
        compiler_params=pltpu.CompilerParams(vmem_limit_bytes=GRANT),
        name="score",
    )(*parts, bottom_out, linear, top_pairs, cotangent)


def finish_dense(pooled, bottom_out, linear, top_pairs, cotangent, top_dense, win_size):
    samples, width = bottom_out.shape
    hidden = top_dense.shape[1]

    def kernel(
        pooled_ref, bottom_ref, linear_ref, pairs_ref, cot_ref, dense_ref, act_ref, grad_ref,
        blank_ref, zeros, sem,
    ):
        zeros[...] = jnp.zeros_like(zeros)
        copy = pltpu.make_async_copy(zeros, blank_ref, sem)
        copy.start()
        pooled = pooled_ref[...]
        preact, sig, pre_grad, pair_grad = head_terms(pooled, bottom_ref, linear_ref, pairs_ref, cot_ref)
        act_ref[...] = (preact * sig).astype(jnp.bfloat16)
        grad_ref[...] = (
            lax.dot_general(
                pre_grad.astype(jnp.bfloat16),
                dense_ref[...],
                (((1,), (1,)), ((), ())),
                preferred_element_type=jnp.float32,
            )
            + pair_grad * pooled
        )
        copy.wait()

    return pl.pallas_call(
        kernel,
        out_shape=(
            jax.ShapeDtypeStruct((samples, hidden), jnp.bfloat16),
            jax.ShapeDtypeStruct((samples, width), jnp.float32),
            jax.ShapeDtypeStruct((win_size, width), jnp.float32),
        ),
        in_specs=[whole()] * 6,
        out_specs=(whole(), whole(), whole(pltpu.HBM)),
        scratch_shapes=[pltpu.VMEM((win_size, width), jnp.float32), pltpu.SemaphoreType.DMA],
        cost_estimate=cost(5e7, 1e6),
        compiler_params=pltpu.CompilerParams(vmem_limit_bytes=GRANT),
        name="finish_dense",
    )(pooled, bottom_out, linear, top_pairs, cotangent, top_dense)


def count_grads(places, bag, group_count):
    samples = places[0].shape[1]
    count = len(places)
    held_rows = group_count * HOT

    def kernel(*refs):
        place_refs, out_refs = refs[:count], refs[count:]
        grp_pos = lax.axis_index("grp")
        shard_pos = lax.axis_index("shard")
        for kept, out_ref in enumerate(out_refs):
            ids = []
            for step in range(group_count):
                holder = shard_pos if (kept == 1) == (step == 0) else jnp.bitwise_xor(shard_pos, 1)
                first = (holder * group_count + jnp.bitwise_xor(grp_pos, step)) * HOT
                ids.append(lax.broadcasted_iota(jnp.int32, (HOT, samples), 0) + first)
            rows = jnp.concatenate(ids, axis=0).astype(jnp.float32)
            for place, ref in enumerate(place_refs):
                times = jnp.zeros(rows.shape, jnp.float32)
                for slot in range(bag):
                    times += jnp.where(ref[pl.ds(slot, 1), :] == rows, 1.0, 0.0)
                out_ref[:, pl.ds(place * samples, samples)] = times

    part = jax.ShapeDtypeStruct((held_rows, count * samples), jnp.float32)
    return pl.pallas_call(
        kernel,
        out_shape=(part, part),
        in_specs=[whole()] * count,
        out_specs=(whole(),) * 2,
        cost_estimate=cost(1e7, 1e6),
        compiler_params=pltpu.CompilerParams(vmem_limit_bytes=GRANT),
        name="count_grads",
    )(*places)


def row_grads(times, scores, wides):
    samples = scores[0].shape[1]
    width = wides[0].shape[1]
    count = len(scores)

    def kernel(times_ref, *refs):
        score_refs, wide_refs = refs[:count], refs[count:-1]
        total = jnp.zeros((times_ref.shape[0], width), jnp.float32)
        for place, (score_ref, wide_ref) in enumerate(zip(score_refs, wide_refs)):
            weights = times_ref[:, pl.ds(place * samples, samples)] * score_ref[...]
            high, low = two_terms(weights)
            bottom = wide_ref[pl.ds(wide_ref.shape[0] - samples, samples), :].astype(jnp.bfloat16)
            total += jnp.dot(high, bottom, preferred_element_type=jnp.float32)
            total += jnp.dot(low, bottom, preferred_element_type=jnp.float32)
        refs[-1][...] = total

    return pl.pallas_call(
        kernel,
        out_shape=jax.ShapeDtypeStruct((times.shape[0], width), jnp.float32),
        in_specs=[whole()] * (1 + 2 * count),
        out_specs=whole(),
        cost_estimate=cost(1e8, 1e6),
        compiler_params=pltpu.CompilerParams(vmem_limit_bytes=GRANT),
        name="row_grads",
    )(times, *scores, *wides)


def split_owners(kept, received, group_count):
    width = kept.shape[1]

    def kernel(kept_ref, received_ref, *out_refs):
        for step, out_ref in enumerate(out_refs):
            chosen = pl.ds(step * HOT, HOT)
            out_ref[...] = kept_ref[chosen, :] + received_ref[chosen, :]

    part = jax.ShapeDtypeStruct((HOT, width), jnp.float32)
    return pl.pallas_call(
        kernel,
        out_shape=(part,) * group_count,
        in_specs=[whole()] * 2,
        out_specs=(whole(),) * group_count,
        cost_estimate=cost(1e6, 1e6),
        compiler_params=pltpu.CompilerParams(vmem_limit_bytes=GRANT),
        name="split_owners",
    )(kept, received)


def place_rows(starts, blocks, blank):
    win_size, width = blank.shape
    count = len(blocks)
    head = min(HOT + 8, win_size)

    def kernel(starts_ref, *refs):
        block_refs = refs[:count]
        out_ref, held, sems = refs[count + 1 :]
        grp_pos = lax.axis_index("grp")
        column = lax.axis_index("shard") * count + grp_pos
        known = starts_ref[...]
        lines = lax.broadcasted_iota(jnp.int32, known.shape, 0)
        windows = lax.broadcasted_iota(jnp.int32, known.shape, 1)
        held[...] = jnp.zeros_like(held)
        firsts = [jnp.int32(0)]
        for step, ref in enumerate(block_refs):
            asked = (lines == jnp.bitwise_xor(grp_pos, step)) & (windows == column)
            start = jnp.sum(jnp.where(asked, known, 0))
            firsts.append(jnp.minimum(start // 8 * 8, win_size - head))
            held[pl.ds(start, HOT), :] += ref[...]
        held[pl.ds(0, HOT), :] += held[pl.ds(win_size, HOT), :]
        copies = []
        for place, first in enumerate(firsts):
            chosen = pl.ds(pl.multiple_of(first, 8), head)
            copy = pltpu.make_async_copy(held.at[chosen], out_ref.at[chosen], sems.at[place])
            copy.start()
            copies.append(copy)
        for copy in copies:
            copy.wait()

    return pl.pallas_call(
        kernel,
        out_shape=jax.ShapeDtypeStruct((win_size, width), jnp.float32),
        in_specs=[whole()] * (1 + count) + [whole(pltpu.HBM)],
        out_specs=whole(pltpu.HBM),
        input_output_aliases={1 + count: 0},
        scratch_shapes=[
            pltpu.VMEM((win_size + HOT, width), jnp.float32),
            pltpu.SemaphoreType.DMA((count + 1,)),
        ],
        cost_estimate=cost(1e6, 2e6),
        compiler_params=pltpu.CompilerParams(vmem_limit_bytes=GRANT),
        name="place_rows",
    )(starts, *blocks, blank)


def far_steps(shard_count):
    return [2 * chips + chips % 2 for chips in range(shard_count // 2 - 1, 1, -1)]


def by_hot_rows(bottom_out, lookups, starts, tables, top_dense, top_pairs, cotangent):
    group_count = lax.axis_size("grp")
    shard_count = lax.axis_size("shard")
    bag = lookups.shape[2]
    win_size = tables.shape[1] // group_count

    def across(values, grp_step, shard_step):
        pairs = [
            (grp * shard_count + shard, (grp ^ grp_step) * shard_count + (shard ^ shard_step))
            for grp in range(group_count)
            for shard in range(shard_count)
        ]
        return lax.ppermute(values, ("grp", "shard"), pairs)

    near, steps = 3, far_steps(shard_count)
    looked = lookups[:, 0, :].T
    hot_own, places_own, near_own, wide_own = load_first(
        starts, looked, bottom_out, tables[0], group_count
    )
    hot_other = across(hot_own, 0, 1)
    places = [across(places_own, 0, step) for step in steps]
    near_back = across(near_own, 0, near)
    terms = hot_terms(hot_own, hot_other)
    linear = linear_part(bottom_out, top_dense)
    own_sums = pool_rows(places_own, terms, bag)
    parts = [own_sums]
    for step, block in zip(steps + [near], places + [near_back]):
        part = pool_rows(block, terms, bag)
        parts.append(across(part, 0, step))
    wides = [across(wide_own, 0, step) for step in steps]
    score_row, pooled = score(parts, bottom_out, linear, top_pairs, cotangent)
    scores = [score_row] + [across(score_row, 0, step) for step in steps + [near]]
    activation, bottom_grad, blank = finish_dense(
        pooled, bottom_out, linear, top_pairs, cotangent, top_dense, win_size
    )
    places = [places_own] + places + [near_back]
    wides = [near_own] + wides + [near_back]
    times_given, times_kept = count_grads(places, bag, group_count)
    given = row_grads(times_given, scores, wides)
    received = across(given, 0, 1)
    kept = row_grads(times_kept, scores, wides)
    owned = split_owners(kept, received, group_count)
    blocks = [owned[0]] + [across(owned[step], step, 1) for step in range(1, group_count)]
    table_grad = place_rows(starts, blocks, blank)
    return activation, bottom_grad, table_grad[None, None]


def is_power(number):
    return number & (number - 1) == 0


def on_device(bottom_out, lookups, starts, tables, top_dense, top_pairs, cotangent):
    group_count = lax.axis_size("grp")
    shard_count = lax.axis_size("shard")
    group_lookups = lookups.shape[0] * lookups.shape[2] * shard_count
    hot_rows = group_count * HOT * shard_count
    fits = (
        tables.shape[0] == 1
        and lookups.shape[2] <= 8
        and bottom_out.shape[0] == tables.shape[2]
        and is_power(group_count)
        and is_power(shard_count)
        and tables.shape[1] // group_count % 8 == 0
        and hot_rows <= group_lookups
        and shard_count >= 8
    )
    plan = by_hot_rows if fits else by_row_sums
    return plan(bottom_out, lookups, starts, tables, top_dense, top_pairs, cotangent)


def solution(mesh):
    in_specs = (
        P(("grp", "shard"), None),
        P(("grp", "shard"), None, None),
        P(),
        P(None, "shard", None),
        P(),
        P(),
        P(("grp", "shard"), None),
    )
    out_specs = (
        P(("grp", "shard"), None),
        P(("grp", "shard"), None),
        P(None, "shard", "grp", None),
    )
    return jax.shard_map(
        on_device, mesh=mesh, in_specs=in_specs, out_specs=out_specs, check_vma=False
    )
```
